32 devices in a mesh: seq: 8 (over z, x), head: 4 (over y, core).
Axes of the slice: x: 2, y: 2, z: 4, core: 2. Of those that a mesh axis runs over, the one named last changes fastest.
Arguments:
- queries: bfloat16 [8192, 4096], P('seq', 'head'), may hold values from -120 to 120
- keys: bfloat16 [8192, 512], P('seq', 'head'), may hold values from -6 to 6
- values: bfloat16 [8192, 512], P('seq', 'head'), may hold values from -6 to 6
- mid_pool: bfloat16 [4, 8], P('head'), may hold values from -3 to 3
- coarse_pool: bfloat16 [4, 256], P('head'), may hold values from -0.375 to 0.375
Outputs:
- attended: bfloat16 [8192, 4096], P(('seq', 'head'))
The draws below stay inside these ranges and needn't reach their ends.
All inputs are finite; a program needn't handle non-finite values.
Results may differ from the reference program's by a relative error of at most 0.0092.
Values may be sent and summed in bfloat16 or wider, within the bound.
No kernel may reach another device: no remote copies, remote signals or barrier semaphores. Data moves between devices by JAX's collectives and lax.ppermute only.
A program may use at most 128 MiB of HBM per device.

```python
import math
import jax
import jax.numpy as jnp
from jax import lax

HEADS = 32
KV_GROUP = 8
HEAD_DIM = 128
BLK = 256
GROUP = 8
MIDS = 256
KV_HEADS = 4
MIDB = 8
SEQ = 8192


def joint_draw(key):
    base = jax.random.fold_in(key, 7)
    subkeys = jax.random.split(base, 2)
    query = jax.random.truncated_normal(subkeys[0], -6.0, 6.0, (SEQ, HEADS, HEAD_DIM), jnp.float32)
    keyset = jax.random.truncated_normal(subkeys[1], -6.0, 6.0, (SEQ, KV_HEADS, HEAD_DIM), jnp.float32)
    return (query.reshape(SEQ, HEADS * HEAD_DIM), keyset.reshape(SEQ, KV_HEADS * HEAD_DIM))


def draw_queries(key, part):
    return joint_draw(key)[0].astype(jnp.bfloat16)


def draw_keys(key, part):
    return joint_draw(key)[1].astype(jnp.bfloat16)


def levels(rng, shape, cuts, smallest, largest):
    def one(dim, parts):
        heights = jax.random.uniform(jax.random.fold_in(jax.random.fold_in(rng, 6), dim), (parts,), jnp.float32, smallest / len(cuts), largest / len(cuts))
        return jnp.repeat(jnp.exp(heights), shape[dim] // parts).reshape((-1,) + (1,) * (len(shape) - dim - 1))

    level = one(*cuts[0])
    for cut in cuts[1:]:
        level = level * one(*cut)
    return level


def noise(stream_key, extent, deviation, limit, cuts=(), kind=jnp.bfloat16):
    result = jax.random.normal(stream_key, extent, jnp.float32) * deviation
    if len(cuts) > 0:
        result = levels(stream_key, extent, cuts, -0.22, 0.18) * result
    return jnp.clip(result, min=-limit, max=limit).astype(kind)


def setup_inputs(seed: int = 0) -> dict:
    key_of = jax.random.split(jax.random.key(seed), 6)
    return {
        "queries": draw_queries(jax.random.fold_in(key_of[5], 71), 0),
        "keys": draw_keys(jax.random.fold_in(key_of[5], 71), 0),
        "values": noise(key_of[2], (SEQ, KV_HEADS * HEAD_DIM), 1.0, 6.0, ((0, 8), (1, 4))),
        "mid_pool": noise(key_of[3], (KV_HEADS, GROUP), 0.5, 3.0, ((0, 4),)),
        "coarse_pool": noise(key_of[4], (KV_HEADS, BLK), (BLK ** -0.5), 0.375, ((0, 4),)),
    }


def reference(queries, keys, values, mid_pool, coarse_pool):
    seq_len = queries.shape[0]
    blocks = seq_len // BLK
    per_group = BLK // GROUP
    logit_scale = 1.0 / math.sqrt(HEAD_DIM)

    def one_head(head_index):
        kv_index = head_index // KV_GROUP
        column = head_index * HEAD_DIM
        kv_column = kv_index * HEAD_DIM
        head_query = lax.dynamic_slice_in_dim(queries, column, HEAD_DIM, 1)
        head_key = lax.dynamic_slice_in_dim(keys, kv_column, HEAD_DIM, 1)
        head_value = lax.dynamic_slice_in_dim(values, kv_column, HEAD_DIM, 1)
        mid_weights = lax.dynamic_slice_in_dim(mid_pool, kv_index, 1, 0)[0].astype(jnp.float32)
        coarse_weights = lax.dynamic_slice_in_dim(coarse_pool, kv_index, 1, 0)[0].astype(jnp.float32)

        def pooled(source, weights, group_size):
            grouped = source.astype(jnp.float32).reshape(seq_len // group_size, group_size, HEAD_DIM)
            return jnp.einsum('gtd,t->gd', grouped, weights).astype(jnp.bfloat16)
        mid_keys = pooled(head_key, mid_weights, GROUP)
        mid_values = pooled(head_value, mid_weights, GROUP)
        summary_key_rows = pooled(head_key, coarse_weights, BLK)
        coarse_values = pooled(head_value, coarse_weights, BLK)
        zero_rows = jnp.zeros((BLK, HEAD_DIM), jnp.bfloat16)
        key_blocks = jnp.concatenate([zero_rows, head_key]).reshape(blocks + 1, BLK, HEAD_DIM)
        value_blocks = jnp.concatenate([zero_rows, head_value]).reshape(blocks + 1, BLK, HEAD_DIM)
        local_keys = jnp.concatenate([key_blocks[:-1], key_blocks[1:]], axis=1)
        near_values = jnp.concatenate([value_blocks[:-1], value_blocks[1:]], axis=1)
        zero_groups = jnp.zeros(((MIDB + 1) * per_group, HEAD_DIM), jnp.bfloat16)
        mid_padded_k = jnp.concatenate([zero_groups, mid_keys]).reshape(blocks + MIDB + 1, per_group, HEAD_DIM)
        mid_padded_v = jnp.concatenate([zero_groups, mid_values]).reshape(blocks + MIDB + 1, per_group, HEAD_DIM)
        distant_keys = jnp.concatenate([mid_padded_k[offset:offset + blocks] for offset in range(MIDB)], axis=1)
        far_v = jnp.concatenate([mid_padded_v[offset:offset + blocks] for offset in range(MIDB)], axis=1)
        blocked_queries = head_query.astype(jnp.float32).reshape(blocks, BLK, HEAD_DIM)
        local_scores = jnp.einsum('hwu,hau->hwa', blocked_queries, local_keys.astype(jnp.float32)) * logit_scale
        middle_level_scores = jnp.einsum('hwu,hau->hwa', blocked_queries, distant_keys.astype(jnp.float32)) * logit_scale
        summary_score_rows = jnp.einsum('ipj,xj->ipx', blocked_queries, summary_key_rows.astype(jnp.float32)) * logit_scale
        block_ids = jnp.arange(blocks, dtype=jnp.int32)[:, None, None]
        query_pos = block_ids * BLK + jnp.arange(BLK, dtype=jnp.int32)[None, :, None]
        key_pos = block_ids * BLK - BLK + jnp.arange(2 * BLK, dtype=jnp.int32)[None, None, :]
        near_ok = (key_pos >= 0) & (key_pos <= query_pos)
        mid_ok = (block_ids - 1 - MIDB) * per_group + jnp.arange(MIDS, dtype=jnp.int32)[None, None, :] >= 0
        coarse_ok = jnp.arange(blocks, dtype=jnp.int32)[None, None, :] <= block_ids - MIDB - 2
        scores = jnp.concatenate([jnp.where(near_ok, local_scores, -jnp.inf), jnp.where(mid_ok, middle_level_scores, -jnp.inf), jnp.where(coarse_ok, summary_score_rows, -jnp.inf)], axis=-1)
        row_max = lax.optimization_barrier(jnp.max(scores, axis=-1, keepdims=True))
        exponent = jnp.exp(scores - row_max)
        row_total = lax.optimization_barrier(jnp.sum(exponent, axis=-1, keepdims=True))
        softmax_weights = (exponent / row_total).astype(jnp.bfloat16)
        coarse_all = jnp.broadcast_to(coarse_values[None], (blocks, blocks, HEAD_DIM))
        collected_rows = jnp.concatenate([near_values, far_v, coarse_all], axis=1)
        output_rows = jnp.einsum('sja,sah->sjh', softmax_weights.astype(jnp.float32), collected_rows.astype(jnp.float32))
        return output_rows.astype(jnp.bfloat16).reshape(seq_len, HEAD_DIM)
    every_head = lax.map(one_head, jnp.arange(HEADS, dtype=jnp.int32))
    return jnp.transpose(every_head, (1, 0, 2)).reshape(seq_len, HEADS * HEAD_DIM)
```

```python
import functools
import math

import jax
import jax.numpy as jnp
from jax import lax
from jax.experimental import pallas as pl
from jax.experimental.pallas import tpu as pltpu
from jax.sharding import PartitionSpec as P

HEAD_DIM = 128
BLK = 256
GROUP = 8
MIDS = 256
MIDB = 8
PER_GROUP = BLK // GROUP
LANES = 128
NEG = -1e30
EXP_SCALE = math.log2(math.e) / math.sqrt(HEAD_DIM)
BF16 = jnp.bfloat16
F32 = jnp.float32


def round_up(value, multiple):
    return -(-value // multiple) * multiple


def cyclic(array, axis, by):
    size = lax.axis_size(axis)
    return lax.ppermute(array, axis, [(i, (i + by) % size) for i in range(size)])


def exchange(array, axis, flip):
    size = lax.axis_size(axis)
    return lax.ppermute(array, axis, [(i, i ^ flip) for i in range(size)])


def pool_kernel(block_count, last_blocks, slot, keys_ref, values_ref, mid_ref, coarse_ref,
                coarse_out, mids_out, last_out, first_out):
    rows = block_count * PER_GROUP
    repeat = (
        lax.broadcasted_iota(jnp.int32, (GROUP, BLK), 1) % GROUP
        == lax.broadcasted_iota(jnp.int32, (GROUP, BLK), 0)
    ).astype(BF16)
    tiled = jnp.dot(mid_ref[...], repeat, preferred_element_type=F32)
    owner = lax.broadcasted_iota(jnp.int32, (PER_GROUP, BLK), 1) // GROUP
    mine = owner == lax.broadcasted_iota(jnp.int32, (PER_GROUP, BLK), 0)
    mid_weights = jnp.where(mine, jnp.broadcast_to(tiled, (PER_GROUP, BLK)), 0.0)
    coarse_weights = coarse_ref[...].astype(F32)
    row = lax.broadcasted_iota(jnp.int32, (slot, BLK), 0)
    for source, mid_base, coarse_base in ((keys_ref, 0, 0), (values_ref, rows, slot)):
        total = jnp.zeros((slot, HEAD_DIM), F32)
        for block in range(block_count):
            here = source[block * BLK : (block + 1) * BLK, :]
            weights = jnp.concatenate(
                [mid_weights, jnp.where(row == block, jnp.broadcast_to(coarse_weights, (slot, BLK)), 0.0)]
            ).astype(BF16)
            pooled = jnp.dot(weights, here, preferred_element_type=F32)
            mids = pooled[:PER_GROUP].astype(BF16)
            total = total + pooled[PER_GROUP:]
            start = mid_base + block * PER_GROUP
            mids_out[start : start + PER_GROUP, :] = mids
            first_out[2 * BLK + start : 2 * BLK + start + PER_GROUP, :] = mids
            late = block - (block_count - last_blocks)
            if late >= 0:
                start = (mid_base // rows) * last_blocks * PER_GROUP + late * PER_GROUP
                last_out[start : start + PER_GROUP, :] = mids
        coarse_out[coarse_base : coarse_base + slot, :] = total.astype(BF16)
    edge = (block_count - 1) * BLK
    first_out[:BLK, :] = keys_ref[edge : edge + BLK, :]
    first_out[BLK : 2 * BLK, :] = values_ref[edge : edge + BLK, :]


def pool(keys, values, mid_pool, coarse_pool, block_count, last_blocks, slot):
    rows = block_count * PER_GROUP
    shapes = (
        (2 * slot, HEAD_DIM),
        (2 * rows, HEAD_DIM),
        (2 * last_blocks * PER_GROUP, HEAD_DIM),
        (2 * BLK + 2 * rows, HEAD_DIM),
    )
    return pl.pallas_call(
        functools.partial(pool_kernel, block_count, last_blocks, slot),
        out_shape=[jax.ShapeDtypeStruct(shape, BF16) for shape in shapes],
        cost_estimate=pl.CostEstimate(
            flops=4 * keys.size * (PER_GROUP + slot), bytes_accessed=6 * keys.size, transcendentals=0
        ),
        name="pool",
    )(keys, values, mid_pool, coarse_pool)


def attend_kernel(geometry, info_ref, q_ref, keys_ref, values_ref, first_ref, *rest):
    block_count, hops, last_blocks, slot, reach, width, step_heads = geometry
    further = rest[: hops - 1]
    mids_ref, coarse_ref, _, out_ref, mid_scratch, all_keys, all_values, bias = rest[hops - 1 :]
    rows = block_count * PER_GROUP
    target = info_ref[0]
    device = info_ref[1]
    block = device * block_count + target
    coarse_at = MIDS
    prev_at = MIDS + width
    own_at = prev_at + BLK

    @pl.when(pl.program_id(0) == 0)
    def _():
        for which, everything in ((0, all_keys), (1, all_values)):
            at = 0
            for index in range(hops - 2, -1, -1):
                ref = further[index]
                size = ref.shape[0] // 2
                mid_scratch[at : at + size, :] = ref[which * size : (which + 1) * size, :]
                at += size
            start = 2 * BLK + which * rows
            mid_scratch[at : at + rows, :] = first_ref[start : start + rows, :]
            at += rows
            mid_scratch[at : at + rows, :] = mids_ref[which * rows : (which + 1) * rows, :]
            window = pl.ds(pl.multiple_of(target * PER_GROUP, PER_GROUP), MIDS)
            everything[:MIDS, :HEAD_DIM] = mid_scratch[window, :]
            wide = coarse_ref[...].astype(F32).reshape(reach, 2, slot, HEAD_DIM)[:, which]
            wide = wide.reshape(reach * slot, HEAD_DIM)
            if width > reach * slot:
                wide = jnp.concatenate([wide, jnp.zeros((width - reach * slot, HEAD_DIM), F32)])
            everything[coarse_at : coarse_at + width, :HEAD_DIM] = wide.astype(BF16)
            source = (keys_ref, values_ref)[which]
            before = pl.ds(pl.multiple_of(jnp.maximum(target - 1, 0) * BLK, BLK), BLK)
            own = pl.ds(pl.multiple_of(target * BLK, BLK), BLK)
            everything[prev_at : prev_at + BLK, :HEAD_DIM] = source[before, :]
            everything[own_at : own_at + BLK, :HEAD_DIM] = source[own, :]

            @pl.when(target == 0)
            def _():
                everything[prev_at : prev_at + BLK, :HEAD_DIM] = first_ref[
                    which * BLK : (which + 1) * BLK, :
                ]

        all_values[:, HEAD_DIM:] = jnp.ones((own_at + BLK, HEAD_DIM), BF16)
        lane = lax.broadcasted_iota(jnp.int32, (8, own_at), 1)
        mid_ok = lane >= (MIDB + 1 - block) * PER_GROUP
        far = (lane - coarse_at) // slot
        nth = (lane - coarse_at) % slot
        coarse_ok = (
            (nth < block_count)
            & (far < reach)
            & (far <= device)
            & (far * block_count - nth + target >= MIDB + 2)
        )
        mid_bias = jnp.where(mid_ok, 0.0, NEG)
        coarse_bias = jnp.where(coarse_ok, 0.0, NEG)
        prev_bias = jnp.where(block * (lane + 1) >= 1, 0.0, NEG)
        bias[...] = jnp.where(
            lane < coarse_at, mid_bias, jnp.where(lane < prev_at, coarse_bias, prev_bias)
        )

    causal = lax.broadcasted_iota(jnp.int32, (BLK, BLK), 0) >= lax.broadcasted_iota(
        jnp.int32, (BLK, BLK), 1
    )
    for head in range(step_heads):
        columns = slice(head * HEAD_DIM, (head + 1) * HEAD_DIM)
        scores = lax.dot_general(
            q_ref[:, columns], all_keys[...], (((1,), (1,)), ((), ())), preferred_element_type=F32
        )
        left = scores[:, :own_at] + bias[0:1, :]
        own = jnp.where(causal, scores[:, own_at:], NEG)
        top = jnp.maximum(
            jnp.max(left, axis=-1, keepdims=True), jnp.max(own, axis=-1, keepdims=True)
        )
        left = jnp.exp2((left - top) * EXP_SCALE).astype(BF16)
        own = jnp.exp2((own - top) * EXP_SCALE).astype(BF16)
        mixed = jnp.dot(left, all_values[:own_at, :], preferred_element_type=F32) + jnp.dot(
            own, all_values[own_at:, :], preferred_element_type=F32
        )
        out_ref[:, columns] = (mixed[:, :HEAD_DIM] / mixed[:, HEAD_DIM:]).astype(BF16)


def attend(info, queries, shared, after, head_start, heads, geometry, full_columns=None):
    block_count, hops, last_blocks, slot, reach, width, step_heads = geometry
    step = step_heads * HEAD_DIM
    first = head_start // step_heads
    total = MIDS + width + 2 * BLK
    out_columns = heads * HEAD_DIM if full_columns is None else full_columns
    own_steps = queries.shape[1] // step
    if full_columns is None:
        out_map = lambda i, info: (0, i)
    else:
        out_map = lambda i, info: (0, info[2] * own_steps + i)
    whole = [pl.BlockSpec(a.shape, lambda i, info: (0, 0)) for a in shared]
    mid_rows = (hops + 1) * block_count * PER_GROUP
    return pl.pallas_call(
        functools.partial(attend_kernel, geometry),
        grid_spec=pltpu.PrefetchScalarGridSpec(
            num_scalar_prefetch=1,
            grid=(heads // step_heads,),
            in_specs=[pl.BlockSpec((BLK, step), lambda i, info: (info[0], first + i))]
            + whole
            + [pl.BlockSpec(memory_space=pl.ANY)],
            out_specs=pl.BlockSpec((BLK, step), out_map),
            scratch_shapes=[
                pltpu.VMEM((mid_rows, HEAD_DIM), BF16),
                pltpu.VMEM((total, HEAD_DIM), BF16),
                pltpu.VMEM((total, 2 * HEAD_DIM), BF16),
                pltpu.VMEM((8, MIDS + width + BLK), F32),
            ],
        ),
        out_shape=jax.ShapeDtypeStruct((BLK, out_columns), BF16),
        compiler_params=pltpu.CompilerParams(vmem_limit_bytes=32 * 1024 * 1024),
        cost_estimate=pl.CostEstimate(
            flops=6 * BLK * heads * total * HEAD_DIM,
            bytes_accessed=4 * BLK * heads * HEAD_DIM + 1024 * 1024,
            transcendentals=BLK * heads * total,
        ),
        name="attend",
    )(info, queries, *shared, after)


def place_kernel(info_ref, piece_ref, _, out_ref):
    out_ref[...] = piece_ref[...]


def place(info, output, piece, at, flip, columns):
    step = math.gcd(piece.shape[1], at) if at else piece.shape[1]
    per_device = columns // step
    return pl.pallas_call(
        place_kernel,
        grid_spec=pltpu.PrefetchScalarGridSpec(
            num_scalar_prefetch=1,
            grid=(piece.shape[1] // step,),
            in_specs=[
                pl.BlockSpec((BLK, step), lambda i, info: (0, i)),
                pl.BlockSpec(memory_space=pl.ANY),
            ],
            out_specs=pl.BlockSpec(
                (BLK, step), lambda i, info: (0, (info[2] ^ flip) * per_device + at // step + i)
            ),
        ),
        out_shape=jax.ShapeDtypeStruct(output.shape, output.dtype),
        input_output_aliases={2: 0},
        cost_estimate=pl.CostEstimate(
            flops=piece.size, bytes_accessed=4 * piece.size, transcendentals=0
        ),
        name="place",
    )(info, piece, output)


def body(queries, keys, values, mid_pool, coarse_pool):
    tokens_here, columns = queries.shape
    heads_here = columns // HEAD_DIM
    block_count = tokens_here // BLK
    members = lax.axis_size("head")
    length = lax.axis_size("seq")
    assert keys.shape[1] == HEAD_DIM and block_count == members
    assert block_count <= MIDB and members & (members - 1) == 0
    device = lax.axis_index("seq")
    member = lax.axis_index("head")
    hops = -(-(MIDB + 1) // block_count)
    last_blocks = MIDB + 1 - (hops - 1) * block_count
    slot = round_up(block_count, 8)

    coarse, mids, last, first = pool(
        keys, values, mid_pool, coarse_pool, block_count, last_blocks, slot
    )
    near = cyclic(first, "seq", 1)
    further = [cyclic(mids, "seq", by) for by in range(2, hops)] + [cyclic(last, "seq", hops)]
    reach = 1
    while reach < length:
        coarse = jnp.concatenate([coarse, cyclic(coarse, "seq", reach)])
        reach *= 2
    width = round_up(reach * slot, LANES)
    geometry = (block_count, hops, last_blocks, slot, reach, width, 2)
    shared = (keys, values, near, *further, mids, coarse)

    def info(flip):
        return jnp.stack([member ^ flip, device, member]).astype(jnp.int32)

    plan = []
    for flip in range(members // 2, members):
        half = heads_here // 2 if flip > members // 2 else heads_here // 4
        plan += [(flip, 0, half), (flip, half, heads_here - half)]
    plan += [(flip, 0, heads_here) for flip in range(1, members // 2)]
    after = coarse
    arrived = []
    for flip, start, heads in plan:
        after = attend(info(flip), queries, shared, after, start, heads, geometry)
        arrived.append((flip, start, exchange(after, "head", flip)))
    output = attend(
        info(0), queries, shared, after, 0, heads_here, geometry, full_columns=members * columns
    )
    order = [p for p in arrived if p[0] < members // 2] + [p for p in arrived if p[0] >= members // 2]
    for flip, start, piece in order:
        output = place(info(0), output, piece, start * HEAD_DIM, flip, columns)
    return output


def solution(mesh):
    return jax.shard_map(
        body,
        mesh=mesh,
        in_specs=(
            P("seq", "head"),
            P("seq", "head"),
            P("seq", "head"),
            P("head", None),
            P("head", None),
        ),
        out_specs=P(("seq", "head"), None),
        check_vma=False,
    )
```

```python
import functools
import math

import jax
import jax.numpy as jnp
from jax import lax
from jax.experimental import pallas as pl
from jax.experimental.pallas import tpu as pltpu
from jax.sharding import PartitionSpec as P


HEAD_DIM = 128
BLK = 256
GROUP = 8
MIDS = 256
MIDB = 8
PER_GROUP = BLK // GROUP
LANES = 128
NEG = -1e30
VMEM_LIMIT = 16 * 1024 * 1024
EXP_SCALE = math.log2(math.e) / math.sqrt(HEAD_DIM)
BF16 = jnp.bfloat16
F32 = jnp.float32


def round_up(value, multiple):
    return -(-value // multiple) * multiple


def cyclic(array, axis, by):
    size = lax.axis_size(axis)
    return lax.ppermute(array, axis, [(i, (i + by) % size) for i in range(size)])


def off_chip(*arrays):
    return [pltpu.with_memory_space_constraint(a, pltpu.HBM) for a in arrays]


def exchange(array, axis, flip):
    size = lax.axis_size(axis)
    return lax.ppermute(array, axis, [(i, i ^ flip) for i in range(size)])


def pool_kernel(block_count, last_blocks, slot, keys_hbm, values_hbm, mid_hbm, coarse_hbm,
                keys_ref, values_ref, coarse_out, mids_out, last_out, first_out,
                mid_ref, coarse_ref, arrived):
    copies = [
        pltpu.make_async_copy(source, target, arrived.at[i])
        for i, (source, target) in enumerate(
            (
                (mid_hbm, mid_ref),
                (coarse_hbm, coarse_ref),
                (keys_hbm, keys_ref),
                (values_hbm, values_ref),
            )
        )
    ]
    for copy in copies:
        copy.start()
    for copy in copies:
        copy.wait()
    rows = block_count * PER_GROUP
    repeat = (
        lax.broadcasted_iota(jnp.int32, (GROUP, BLK), 1) % GROUP
        == lax.broadcasted_iota(jnp.int32, (GROUP, BLK), 0)
    ).astype(BF16)
    tiled = jnp.dot(mid_ref[...], repeat, preferred_element_type=F32)
    owner = lax.broadcasted_iota(jnp.int32, (PER_GROUP, BLK), 1) // GROUP
    mine = owner == lax.broadcasted_iota(jnp.int32, (PER_GROUP, BLK), 0)
    mid_weights = jnp.where(mine, jnp.broadcast_to(tiled, (PER_GROUP, BLK)), 0.0)
    coarse_weights = coarse_ref[...].astype(F32)
    row = lax.broadcasted_iota(jnp.int32, (slot, BLK), 0)
    for source, mid_base, coarse_base in ((keys_ref, 0, 0), (values_ref, rows, slot)):
        total = jnp.zeros((slot, HEAD_DIM), F32)
        for block in range(block_count):
            here = source[block * BLK : (block + 1) * BLK, :]
            weights = jnp.concatenate(
                [mid_weights, jnp.where(row == block, jnp.broadcast_to(coarse_weights, (slot, BLK)), 0.0)]
            ).astype(BF16)
            pooled = jnp.dot(weights, here, preferred_element_type=F32)
            mids = pooled[:PER_GROUP].astype(BF16)
            total = total + pooled[PER_GROUP:]
            start = mid_base + block * PER_GROUP
            mids_out[start : start + PER_GROUP, :] = mids
            first_out[2 * BLK + start : 2 * BLK + start + PER_GROUP, :] = mids
            late = block - (block_count - last_blocks)
            if late >= 0:
                start = (mid_base // rows) * last_blocks * PER_GROUP + late * PER_GROUP
                last_out[start : start + PER_GROUP, :] = mids
        coarse_out[coarse_base : coarse_base + slot, :] = total.astype(BF16)
    edge = (block_count - 1) * BLK
    first_out[:BLK, :] = keys_ref[edge : edge + BLK, :]
    first_out[BLK : 2 * BLK, :] = values_ref[edge : edge + BLK, :]


def pool(keys, values, mid_pool, coarse_pool, block_count, last_blocks, slot):
    rows = block_count * PER_GROUP
    shapes = (
        keys.shape,
        values.shape,
        (2 * slot, HEAD_DIM),
        (2 * rows, HEAD_DIM),
        (2 * last_blocks * PER_GROUP, HEAD_DIM),
        (2 * BLK + 2 * rows, HEAD_DIM),
    )
    return pl.pallas_call(
        functools.partial(pool_kernel, block_count, last_blocks, slot),
        in_specs=[pl.BlockSpec(memory_space=pltpu.HBM)] * 4,
        out_specs=[pl.BlockSpec(memory_space=pltpu.VMEM) for _ in shapes],
        out_shape=[jax.ShapeDtypeStruct(shape, BF16) for shape in shapes],
        scratch_shapes=[
            pltpu.VMEM(mid_pool.shape, BF16),
            pltpu.VMEM(coarse_pool.shape, BF16),
            pltpu.SemaphoreType.DMA((4,)),
        ],
        cost_estimate=pl.CostEstimate(
            flops=4 * keys.size * (PER_GROUP + slot), bytes_accessed=6 * keys.size, transcendentals=0
        ),
        compiler_params=pltpu.CompilerParams(vmem_limit_bytes=VMEM_LIMIT),
        name="pool",
    )(*off_chip(keys, values, mid_pool, coarse_pool))


def join_kernel(one_ref, two_ref, out_ref):
    size = one_ref.shape[0]
    out_ref[:size, :] = one_ref[...]
    out_ref[size:, :] = two_ref[...]


def join(one, two):
    return pl.pallas_call(
        join_kernel,
        out_shape=jax.ShapeDtypeStruct((one.shape[0] + two.shape[0], one.shape[1]), one.dtype),
        compiler_params=pltpu.CompilerParams(vmem_limit_bytes=VMEM_LIMIT),
        name="join",
    )(one, two)


def load_kernel(*refs):
    count = len(refs) // 2
    copies = [
        pltpu.make_async_copy(refs[i], refs[count + i], refs[-1].at[i]) for i in range(count)
    ]
    for copy in copies:
        copy.start()
    for copy in copies:
        copy.wait()


def load(*arrays):
    return pl.pallas_call(
        load_kernel,
        in_specs=[pl.BlockSpec(memory_space=pltpu.HBM) for _ in arrays],
        out_specs=[pl.BlockSpec(memory_space=pltpu.VMEM) for _ in arrays],
        out_shape=[jax.ShapeDtypeStruct(a.shape, a.dtype) for a in arrays],
        scratch_shapes=[pltpu.SemaphoreType.DMA((len(arrays),))],
        compiler_params=pltpu.CompilerParams(vmem_limit_bytes=VMEM_LIMIT),
        cost_estimate=pl.CostEstimate(
            flops=2 * sum(a.size for a in arrays),
            bytes_accessed=4 * sum(a.size for a in arrays),
            transcendentals=0,
        ),
        name="load",
    )(*off_chip(*arrays))


def attend_kernel(geometry, info_ref, q_ref, keys_ref, values_ref, first_ref, *rest):
    block_count, hops, _, slot, reach, width, step_heads = geometry
    further = rest[: hops - 1]
    mids_ref, coarse_ref, _, out_ref, mid_scratch, all_keys, all_values, bias = rest[hops - 1 :]
    rows = block_count * PER_GROUP
    target = info_ref[0]
    device = info_ref[1]
    block = device * block_count + target
    coarse_at = MIDS
    prev_at = MIDS + width
    own_at = prev_at + BLK

    @pl.when(pl.program_id(0) == 0)
    def _():
        for which, everything in ((0, all_keys), (1, all_values)):
            at = 0
            for index in range(hops - 2, -1, -1):
                ref = further[index]
                size = ref.shape[0] // 2
                mid_scratch[at : at + size, :] = ref[which * size : (which + 1) * size, :]
                at += size
            start = 2 * BLK + which * rows
            mid_scratch[at : at + rows, :] = first_ref[start : start + rows, :]
            at += rows
            mid_scratch[at : at + rows, :] = mids_ref[which * rows : (which + 1) * rows, :]
            window = pl.ds(pl.multiple_of(target * PER_GROUP, PER_GROUP), MIDS)
            everything[:MIDS, :HEAD_DIM] = mid_scratch[window, :]
            wide = coarse_ref[...].astype(F32).reshape(reach, 2, slot, HEAD_DIM)[:, which]
            wide = wide.reshape(reach * slot, HEAD_DIM)
            if width > reach * slot:
                wide = jnp.concatenate([wide, jnp.zeros((width - reach * slot, HEAD_DIM), F32)])
            everything[coarse_at : coarse_at + width, :HEAD_DIM] = wide.astype(BF16)
            source = (keys_ref, values_ref)[which]
            before = pl.ds(pl.multiple_of(jnp.maximum(target - 1, 0) * BLK, BLK), BLK)
            own = pl.ds(pl.multiple_of(target * BLK, BLK), BLK)
            everything[prev_at : prev_at + BLK, :HEAD_DIM] = source[before, :]
            everything[own_at : own_at + BLK, :HEAD_DIM] = source[own, :]

            @pl.when(target == 0)
            def _():
                everything[prev_at : prev_at + BLK, :HEAD_DIM] = first_ref[
                    which * BLK : (which + 1) * BLK, :
                ]

        all_values[:, HEAD_DIM:] = jnp.ones((own_at + BLK, HEAD_DIM), BF16)
        lane = lax.broadcasted_iota(jnp.int32, (8, own_at), 1)
        mid_ok = lane >= (MIDB + 1 - block) * PER_GROUP
        far = (lane - coarse_at) // slot
        nth = (lane - coarse_at) % slot
        coarse_ok = (
            (nth < block_count)
            & (far < reach)
            & (far <= device)
            & (far * block_count - nth + target >= MIDB + 2)
        )
        mid_bias = jnp.where(mid_ok, 0.0, NEG)
        coarse_bias = jnp.where(coarse_ok, 0.0, NEG)
        prev_bias = jnp.where(block * (lane + 1) >= 1, 0.0, NEG)
        bias[...] = jnp.where(
            lane < coarse_at, mid_bias, jnp.where(lane < prev_at, coarse_bias, prev_bias)
        )

    causal = lax.broadcasted_iota(jnp.int32, (BLK, BLK), 0) >= lax.broadcasted_iota(
        jnp.int32, (BLK, BLK), 1
    )
    for head in range(step_heads):
        columns = slice(head * HEAD_DIM, (head + 1) * HEAD_DIM)
        scores = lax.dot_general(
            q_ref[:, columns], all_keys[...], (((1,), (1,)), ((), ())), preferred_element_type=F32
        )
        left = scores[:, :own_at] + bias[0:1, :]
        own = jnp.where(causal, scores[:, own_at:], NEG)
        top = jnp.maximum(
            jnp.max(left, axis=-1, keepdims=True), jnp.max(own, axis=-1, keepdims=True)
        )
        left = jnp.exp2((left - top) * EXP_SCALE).astype(BF16)
        own = jnp.exp2((own - top) * EXP_SCALE).astype(BF16)
        mixed = jnp.dot(left, all_values[:own_at, :], preferred_element_type=F32) + jnp.dot(
            own, all_values[own_at:, :], preferred_element_type=F32
        )
        out_ref[:, columns] = (mixed[:, :HEAD_DIM] / mixed[:, HEAD_DIM:]).astype(BF16)


def attend(info, queries, shared, after, head_start, heads, geometry, full_columns=None):
    block_count, hops, _, _, _, width, step_heads = geometry
    step = step_heads * HEAD_DIM
    first = head_start // step_heads
    total = MIDS + width + 2 * BLK
    out_columns = heads * HEAD_DIM if full_columns is None else full_columns
    own_steps = queries.shape[1] // step
    if full_columns is None:
        out_map = lambda i, info: (0, i)
    else:
        out_map = lambda i, info: (0, info[2] * own_steps + i)
    whole = [pl.BlockSpec(a.shape, lambda i, info: (0, 0)) for a in shared]
    mid_rows = (hops + 1) * block_count * PER_GROUP
    return pl.pallas_call(
        functools.partial(attend_kernel, geometry),
        grid_spec=pltpu.PrefetchScalarGridSpec(
            num_scalar_prefetch=1,
            grid=(heads // step_heads,),
            in_specs=[pl.BlockSpec((BLK, step), lambda i, info: (info[0], first + i))]
            + whole
            + [pl.BlockSpec(memory_space=pl.ANY)],
            out_specs=pl.BlockSpec((BLK, step), out_map),
            scratch_shapes=[
                pltpu.VMEM((mid_rows, HEAD_DIM), BF16),
                pltpu.VMEM((total, HEAD_DIM), BF16),
                pltpu.VMEM((total, 2 * HEAD_DIM), BF16),
                pltpu.VMEM((8, MIDS + width + BLK), F32),
            ],
        ),
        out_shape=jax.ShapeDtypeStruct((BLK, out_columns), BF16),
        compiler_params=pltpu.CompilerParams(vmem_limit_bytes=VMEM_LIMIT),
        cost_estimate=pl.CostEstimate(
            flops=6 * BLK * heads * total * HEAD_DIM,
            bytes_accessed=4 * BLK * heads * HEAD_DIM + 1024 * 1024,
            transcendentals=BLK * heads * total,
        ),
        name="attend",
    )(info, queries, *shared, after)


def place_kernel(flip, at, columns, info_ref, piece_ref, _, out_ref, done):
    start = pl.multiple_of((info_ref[2] ^ flip) * columns + at, HEAD_DIM)
    copy = pltpu.make_async_copy(
        piece_ref, out_ref.at[:, pl.ds(start, piece_ref.shape[1])], done
    )
    copy.start()
    copy.wait()


def place(info, output, piece, at, flip, columns):
    return pl.pallas_call(
        functools.partial(place_kernel, flip, at, columns),
        in_specs=[
            pl.BlockSpec(memory_space=pltpu.SMEM),
            pl.BlockSpec(memory_space=pltpu.VMEM),
            pl.BlockSpec(memory_space=pl.ANY),
        ],
        out_specs=pl.BlockSpec(memory_space=pl.ANY),
        scratch_shapes=[pltpu.SemaphoreType.DMA(())],
        out_shape=jax.ShapeDtypeStruct(output.shape, output.dtype),
        input_output_aliases={2: 0},
        compiler_params=pltpu.CompilerParams(vmem_limit_bytes=VMEM_LIMIT),
        cost_estimate=pl.CostEstimate(
            flops=piece.size, bytes_accessed=4 * piece.size, transcendentals=0
        ),
        name="place",
    )(info, piece, output)


def body(queries, keys, values, mid_pool, coarse_pool):
    tokens_here, columns = queries.shape
    heads_here = columns // HEAD_DIM
    block_count = tokens_here // BLK
    members = lax.axis_size("head")
    length = lax.axis_size("seq")
    assert keys.shape[1] == HEAD_DIM and block_count == members
    assert block_count <= MIDB and members & (members - 1) == 0
    device = lax.axis_index("seq")
    member = lax.axis_index("head")
    hops = -(-(MIDB + 1) // block_count)
    last_blocks = MIDB + 1 - (hops - 1) * block_count
    slot = round_up(block_count, 8)

    keys, values, coarse, mids, last, first = pool(
        keys, values, mid_pool, coarse_pool, block_count, last_blocks, slot
    )
    reach, step = 1, 0
    while reach < length:
        arriving = cyclic(coarse, "seq", reach)
        if step == 0:
            near = cyclic(first, "seq", 1)
            (queries,) = load(queries)
        coarse = join(coarse, arriving)
        reach, step = 2 * reach, step + 1
    further = [cyclic(mids, "seq", by) for by in range(2, hops)]
    further += [cyclic(last, "seq", hops)]
    width = round_up(reach * slot, LANES)
    geometry = (block_count, hops, last_blocks, slot, reach, width, 2)
    shared = (keys, values, near, *further, mids, coarse)

    def info(flip):
        return jnp.stack([member ^ flip, device, member]).astype(jnp.int32)

    after = coarse
    arrived = []
    for flip, start, heads in send_plan(members, heads_here):
        after = attend(info(flip), queries, shared, after, start, heads, geometry)
        arrived.append((flip, start, exchange(after, "head", flip)))
    output = attend(
        info(0), queries, shared, after, 0, heads_here, geometry, members * columns
    )
    order = [p for p in arrived if p[0] < members // 2] + [p for p in arrived if p[0] >= members // 2]
    for flip, start, piece in order:
        output = place(info(0), output, piece, start * HEAD_DIM, flip, columns)
    return output


def send_plan(members, heads):
    plan = []
    for flip in range(members // 2, members):
        half = heads // 2 if flip > members // 2 else heads // 4
        plan += [(flip, 0, half), (flip, half, heads - half)]
    return plan + [(flip, 0, heads) for flip in range(1, members // 2)]


def solution(mesh):
    return jax.shard_map(
        body,
        mesh=mesh,
        in_specs=(
            P("seq", "head"),
            P("seq", "head"),
            P("seq", "head"),
            P("head", None),
            P("head", None),
        ),
        out_specs=P(("seq", "head"), None),
        check_vma=False,
    )
```

```python
import functools
import math

import jax
import jax.numpy as jnp
from jax import lax
from jax.experimental import pallas as pl
from jax.experimental.pallas import tpu as pltpu
from jax.sharding import PartitionSpec as P


HEAD_DIM = 128
BLK = 256
GROUP = 8
MIDS = 256
MIDB = 8
PER_GROUP = BLK // GROUP
LANES = 128
NEG = -1e30
HALF = BLK // 2
CHUNK = 32
VMEM_LIMIT = 16 * 1024 * 1024
ATTEND_LIMIT = 28 * 1024 * 1024
EXP_SCALE = math.log2(math.e) / math.sqrt(HEAD_DIM)
BF16 = jnp.bfloat16
F32 = jnp.float32


def round_up(value, multiple):
    return -(-value // multiple) * multiple


def cyclic(array, axis, by):
    size = lax.axis_size(axis)
    return lax.ppermute(array, axis, [(i, (i + by) % size) for i in range(size)])


def off_chip(*arrays):
    return [pltpu.with_memory_space_constraint(a, pltpu.HBM) for a in arrays]


def exchange(array, axis, flip):
    size = lax.axis_size(axis)
    return lax.ppermute(array, axis, [(i, i ^ flip) for i in range(size)])


def pool_kernel(block_count, last_blocks, slot, keys_hbm, values_hbm, mid_hbm, coarse_hbm,
                keys_ref, values_ref, coarse_out, mids_out, last_out, first_out,
                mid_ref, coarse_ref, arrived):
    copies = [
        pltpu.make_async_copy(source, target, arrived.at[i])
        for i, (source, target) in enumerate(
            (
                (mid_hbm, mid_ref),
                (coarse_hbm, coarse_ref),
                (keys_hbm, keys_ref),
                (values_hbm, values_ref),
            )
        )
    ]
    for copy in copies:
        copy.start()
    for copy in copies:
        copy.wait()
    rows = block_count * PER_GROUP
    repeat = (
        lax.broadcasted_iota(jnp.int32, (GROUP, BLK), 1) % GROUP
        == lax.broadcasted_iota(jnp.int32, (GROUP, BLK), 0)
    ).astype(BF16)
    tiled = jnp.dot(mid_ref[...], repeat, preferred_element_type=F32)
    owner = lax.broadcasted_iota(jnp.int32, (PER_GROUP, BLK), 1) // GROUP
    mine = owner == lax.broadcasted_iota(jnp.int32, (PER_GROUP, BLK), 0)
    mid_weights = jnp.where(mine, jnp.broadcast_to(tiled, (PER_GROUP, BLK)), 0.0)
    coarse_weights = coarse_ref[...].astype(F32)
    row = lax.broadcasted_iota(jnp.int32, (slot, BLK), 0)
    for source, mid_base, coarse_base in ((keys_ref, 0, 0), (values_ref, rows, slot)):
        total = jnp.zeros((slot, HEAD_DIM), F32)
        for block in range(block_count):
            here = source[block * BLK : (block + 1) * BLK, :]
            weights = jnp.concatenate(
                [mid_weights, jnp.where(row == block, jnp.broadcast_to(coarse_weights, (slot, BLK)), 0.0)]
            ).astype(BF16)
            pooled = jnp.dot(weights, here, preferred_element_type=F32)
            mids = pooled[:PER_GROUP].astype(BF16)
            total = total + pooled[PER_GROUP:]
            start = mid_base + block * PER_GROUP
            mids_out[start : start + PER_GROUP, :] = mids
            first_out[2 * BLK + start : 2 * BLK + start + PER_GROUP, :] = mids
            late = block - (block_count - last_blocks)
            if late >= 0:
                start = (mid_base // rows) * last_blocks * PER_GROUP + late * PER_GROUP
                last_out[start : start + PER_GROUP, :] = mids
        coarse_out[coarse_base : coarse_base + slot, :] = total.astype(BF16)
    edge = (block_count - 1) * BLK
    first_out[:BLK, :] = keys_ref[edge : edge + BLK, :]
    first_out[BLK : 2 * BLK, :] = values_ref[edge : edge + BLK, :]


def pool(keys, values, mid_pool, coarse_pool, block_count, last_blocks, slot):
    rows = block_count * PER_GROUP
    shapes = (
        keys.shape,
        values.shape,
        (2 * slot, HEAD_DIM),
        (2 * rows, HEAD_DIM),
        (2 * last_blocks * PER_GROUP, HEAD_DIM),
        (2 * BLK + 2 * rows, HEAD_DIM),
    )
    return pl.pallas_call(
        functools.partial(pool_kernel, block_count, last_blocks, slot),
        in_specs=[pl.BlockSpec(memory_space=pltpu.HBM)] * 4,
        out_specs=[pl.BlockSpec(memory_space=pltpu.VMEM) for _ in shapes],
        out_shape=[jax.ShapeDtypeStruct(shape, BF16) for shape in shapes],
        scratch_shapes=[
            pltpu.VMEM(mid_pool.shape, BF16),
            pltpu.VMEM(coarse_pool.shape, BF16),
            pltpu.SemaphoreType.DMA((4,)),
        ],
        cost_estimate=pl.CostEstimate(
            flops=4 * keys.size * (PER_GROUP + slot), bytes_accessed=6 * keys.size, transcendentals=0
        ),
        compiler_params=pltpu.CompilerParams(vmem_limit_bytes=VMEM_LIMIT),
        name="pool",
    )(*off_chip(keys, values, mid_pool, coarse_pool))


def join_kernel(one_ref, two_ref, out_ref):
    size = one_ref.shape[0]
    out_ref[:size, :] = one_ref[...]
    out_ref[size:, :] = two_ref[...]


def join(one, two):
    return pl.pallas_call(
        join_kernel,
        out_shape=jax.ShapeDtypeStruct((one.shape[0] + two.shape[0], one.shape[1]), one.dtype),
        compiler_params=pltpu.CompilerParams(vmem_limit_bytes=VMEM_LIMIT),
        name="join",
    )(one, two)


def load_kernel(*refs):
    count = len(refs) // 2
    copies = [
        pltpu.make_async_copy(refs[i], refs[count + i], refs[-1].at[i]) for i in range(count)
    ]
    for copy in copies:
        copy.start()
    for copy in copies:
        copy.wait()


def load(*arrays):
    return pl.pallas_call(
        load_kernel,
        in_specs=[pl.BlockSpec(memory_space=pltpu.HBM) for _ in arrays],
        out_specs=[pl.BlockSpec(memory_space=pltpu.VMEM) for _ in arrays],
        out_shape=[jax.ShapeDtypeStruct(a.shape, a.dtype) for a in arrays],
        scratch_shapes=[pltpu.SemaphoreType.DMA((len(arrays),))],
        compiler_params=pltpu.CompilerParams(vmem_limit_bytes=VMEM_LIMIT),
        cost_estimate=pl.CostEstimate(
            flops=2 * sum(a.size for a in arrays),
            bytes_accessed=4 * sum(a.size for a in arrays),
            transcendentals=0,
        ),
        name="load",
    )(*off_chip(*arrays))


def fill_summaries(geometry, target, width, sources, mid_scratch, which, write):
    block_count, hops, _, slot, reach = geometry
    source, first_ref = sources[which], sources[2]
    further, mids_ref, coarse_ref = sources[3 : 2 + hops], sources[-2], sources[-1]
    rows = block_count * PER_GROUP
    at = 0
    for index in range(hops - 2, -1, -1):
        size = further[index].shape[0] // 2
        mid_scratch[at : at + size, :] = further[index][which * size : (which + 1) * size, :]
        at += size
    start = 2 * BLK + which * rows
    mid_scratch[at : at + rows, :] = first_ref[start : start + rows, :]
    at += rows
    mid_scratch[at : at + rows, :] = mids_ref[which * rows : (which + 1) * rows, :]
    window = pl.ds(pl.multiple_of(target * PER_GROUP, PER_GROUP), MIDS)
    write(0, mid_scratch[window, :])
    wide = coarse_ref[...].astype(F32).reshape(reach, 2, slot, HEAD_DIM)[:, which]
    wide = wide.reshape(reach * slot, HEAD_DIM)
    if width > reach * slot:
        wide = jnp.concatenate([wide, jnp.zeros((width - reach * slot, HEAD_DIM), F32)])
    write(MIDS, wide.astype(BF16))
    before = pl.ds(pl.multiple_of(jnp.maximum(target - 1, 0) * BLK, BLK), BLK)
    write(MIDS + width, source[before, :])

    @pl.when(target == 0)
    def _():
        write(MIDS + width, first_ref[which * BLK : (which + 1) * BLK, :])


def pack_kernel(geometry, info_ref, *refs):
    sources, (_, out_ref, mid_scratch) = refs[:-3], refs[-3:]
    _, _, _, slot, reach = geometry
    for which in range(2):
        columns = slice(which * HEAD_DIM, (which + 1) * HEAD_DIM)

        def write(at, value):
            out_ref[at : at + value.shape[0], columns] = value

        fill_summaries(geometry, info_ref[0], reach * slot, sources, mid_scratch, which, write)


def whole_in_vmem(count):
    return [pl.BlockSpec(memory_space=pltpu.VMEM)] * count


def mid_rows(geometry):
    block_count, hops = geometry[:2]
    return (hops + 1) * block_count * PER_GROUP


def pack(info, shared, after, geometry):
    _, _, _, slot, reach = geometry
    rows = MIDS + reach * slot + BLK
    return pl.pallas_call(
        functools.partial(pack_kernel, geometry),
        in_specs=[pl.BlockSpec(memory_space=pltpu.SMEM)]
        + whole_in_vmem(len(shared))
        + [pl.BlockSpec(memory_space=pl.ANY)],
        out_specs=pl.BlockSpec(memory_space=pltpu.VMEM),
        out_shape=jax.ShapeDtypeStruct((rows, 2 * HEAD_DIM), BF16),
        scratch_shapes=[pltpu.VMEM((mid_rows(geometry), HEAD_DIM), BF16)],
        compiler_params=pltpu.CompilerParams(vmem_limit_bytes=VMEM_LIMIT),
        cost_estimate=pl.CostEstimate(
            flops=rows * HEAD_DIM, bytes_accessed=8 * rows * HEAD_DIM, transcendentals=0
        ),
        name="pack",
    )(info, *shared, after)


def fill_bias(geometry, target, device, width, bias):
    block_count, _, _, slot, reach = geometry
    block = device * block_count + target
    coarse_at = MIDS
    prev_at = MIDS + width
    lane = lax.broadcasted_iota(jnp.int32, bias.shape, 1)
    mid_ok = lane >= (MIDB + 1 - block) * PER_GROUP
    far = (lane - coarse_at) // slot
    nth = (lane - coarse_at) % slot
    coarse_ok = (
        (nth < block_count)
        & (far < reach)
        & (far <= device)
        & (far * block_count - nth + target >= MIDB + 2)
    )
    mid_bias = jnp.where(mid_ok, 0.0, NEG)
    coarse_bias = jnp.where(coarse_ok, 0.0, NEG)
    prev_bias = jnp.where(block * (lane + 1) >= 1, 0.0, NEG)
    bias[...] = jnp.where(
        lane < coarse_at, mid_bias, jnp.where(lane < prev_at, coarse_bias, prev_bias)
    )


def attend_rows(q_ref, row_start, head_start, heads, out_ref, scratch):
    all_keys, all_values, bias, scores, weights = scratch
    own_at = bias.shape[1]
    all_values[:, HEAD_DIM:] = jnp.ones((own_at + BLK, HEAD_DIM), BF16)

    group = max(1, heads // 2)
    units = [(first, half) for first in range(0, heads, group) for half in range(2)]
    row = lax.broadcasted_iota(jnp.int32, (CHUNK, HALF), 0)
    column = lax.broadcasted_iota(jnp.int32, (CHUNK, HALF), 1)

    def columns(head):
        return slice(head * HEAD_DIM, (head + 1) * HEAD_DIM)

    def score(unit):
        first, half = units[unit]
        seen = own_at + (half + 1) * HALF
        rows_here = pl.ds(pl.multiple_of(row_start + half * HALF, HALF), HALF)
        stacked = jnp.concatenate(
            [q_ref[rows_here, columns(head_start + first + i)] for i in range(group)]
        )
        scores[unit % 2, :, :seen] = lax.dot_general(
            stacked, all_keys[:seen, :], (((1,), (1,)), ((), ())), preferred_element_type=F32
        )

    def weigh(unit):
        _, half = units[unit]
        seen = own_at + (half + 1) * HALF
        for at in range(0, group * HALF, CHUNK):
            here = slice(at, at + CHUNK)
            parts = [scores[unit % 2, here, :own_at] + bias[0:1, :]]
            if half:
                parts.append(scores[unit % 2, here, own_at : own_at + HALF])
            edge = scores[unit % 2, here, seen - HALF : seen]
            parts.append(jnp.where(row + at % HALF >= column, edge, NEG))
            chunk = jnp.concatenate(parts, axis=1)
            top = jnp.max(chunk, axis=-1, keepdims=True)
            weights[unit % 2, here, :seen] = jnp.exp2((chunk - top) * EXP_SCALE).astype(BF16)

    def mix(unit):
        first, half = units[unit]
        seen = own_at + (half + 1) * HALF
        mixed = jnp.dot(
            weights[unit % 2, :, :seen], all_values[:seen, :], preferred_element_type=F32
        )
        mixed = (mixed[:, :HEAD_DIM] / mixed[:, HEAD_DIM:]).astype(BF16)
        for i in range(group):
            out_ref[half * HALF : (half + 1) * HALF, columns(first + i)] = mixed[
                i * HALF : (i + 1) * HALF
            ]

    for unit in range(len(units) + 2):
        if unit < len(units):
            score(unit)
        if 1 <= unit <= len(units):
            weigh(unit - 1)
        if unit >= 2:
            mix(unit - 2)


def attend_kernel(geometry, width, head_start, heads, info_ref, q_ref, *rest):
    sources, rest = rest[: geometry[1] + 4], rest[geometry[1] + 4 :]
    _, out_ref, mid_scratch = rest[:3]
    scratch = rest[3:]
    target, device = info_ref[0], info_ref[1]
    own_at = MIDS + width + BLK
    for which in range(2):
        everything = scratch[which]

        def write(at, value):
            everything[at : at + value.shape[0], :HEAD_DIM] = value

        fill_summaries(geometry, target, width, sources, mid_scratch, which, write)
        own = pl.ds(pl.multiple_of(target * BLK, BLK), BLK)
        write(own_at, sources[which][own, :])
    fill_bias(geometry, target, device, width, scratch[2])
    attend_rows(q_ref, target * BLK, head_start, heads, out_ref, scratch)


def shipped_kernel(geometry, width, heads, info_ref, early_ref, late_ref, _, out_ref, *scratch):
    _, _, _, slot, reach = geometry
    used = MIDS + reach * slot
    own_at = MIDS + width + BLK
    for which in range(2):
        everything = scratch[which]
        columns = slice(which * HEAD_DIM, (which + 1) * HEAD_DIM)
        everything[:used, :HEAD_DIM] = late_ref[:used, columns]
        if width > reach * slot:
            everything[used : MIDS + width, :HEAD_DIM] = jnp.zeros(
                (MIDS + width - used, HEAD_DIM), BF16
            )
        everything[MIDS + width : own_at, :HEAD_DIM] = late_ref[used:, columns]
        at = (heads + which) * HEAD_DIM
        everything[own_at:, :HEAD_DIM] = early_ref[:, at : at + HEAD_DIM]
    fill_bias(geometry, info_ref[0], info_ref[1], width, scratch[2])
    attend_rows(early_ref, 0, 0, heads, out_ref, scratch)


def attend_call(kernel, operands, heads, width, out_columns, out_map, extra_scratch, alias):
    total = MIDS + width + 2 * BLK
    unit_rows = max(1, heads // 2) * HALF
    whole = [pl.BlockSpec(a.shape, lambda i, info: (0, 0)) for a in operands[1:-1]]
    return pl.pallas_call(
        kernel,
        grid_spec=pltpu.PrefetchScalarGridSpec(
            num_scalar_prefetch=1,
            grid=(1,),
            in_specs=whole + [pl.BlockSpec(memory_space=pl.ANY)],
            out_specs=pl.BlockSpec((BLK, heads * HEAD_DIM), out_map),
            scratch_shapes=extra_scratch
            + [
                pltpu.VMEM((total, HEAD_DIM), BF16),
                pltpu.VMEM((total, 2 * HEAD_DIM), BF16),
                pltpu.VMEM((8, total - BLK), F32),
                pltpu.VMEM((2, unit_rows, total), F32),
                pltpu.VMEM((2, unit_rows, total), BF16),
            ],
        ),
        out_shape=jax.ShapeDtypeStruct((BLK, out_columns), BF16),
        input_output_aliases={len(operands) - 1: 0} if alias else {},
        compiler_params=pltpu.CompilerParams(vmem_limit_bytes=ATTEND_LIMIT),
        cost_estimate=pl.CostEstimate(
            flops=6 * BLK * heads * total * HEAD_DIM,
            bytes_accessed=4 * BLK * heads * HEAD_DIM + 1024 * 1024,
            transcendentals=BLK * heads * total,
        ),
        name="attend",
    )(*operands)


def attend(info, queries, shared, after, head_start, heads, geometry, full_columns=None):
    width = round_up(geometry[4] * geometry[3], LANES)
    if full_columns is None:
        out_columns, out_map = heads * HEAD_DIM, lambda i, info: (0, 0)
    else:
        out_columns, out_map = full_columns, lambda i, info: (0, info[2])
    return attend_call(
        functools.partial(attend_kernel, geometry, width, head_start, heads),
        (info, queries, *shared, after),
        heads,
        width,
        out_columns,
        out_map,
        [pltpu.VMEM((mid_rows(geometry), HEAD_DIM), BF16)],
        False,
    )


def attend_shipped(info, early, late, output, flip, heads, geometry):
    width = round_up(geometry[4] * geometry[3], LANES)
    return attend_call(
        functools.partial(shipped_kernel, geometry, width, heads),
        (info, early, late, output),
        heads,
        width,
        output.shape[1],
        lambda i, info: (0, info[2] ^ flip),
        [],
        True,
    )


def prepare_kernel(info_ref, queries_hbm, keys_hbm, values_hbm, out_ref, done):
    rows = pl.ds(pl.multiple_of(info_ref[0] * BLK, BLK), BLK)
    copies, at = [], 0
    for i, source in enumerate((queries_hbm, keys_hbm, values_hbm)):
        columns = slice(at, at + source.shape[1])
        copies.append(
            pltpu.make_async_copy(source.at[rows, :], out_ref.at[:, columns], done.at[i])
        )
        at += source.shape[1]
    for copy in copies:
        copy.start()
    for copy in copies:
        copy.wait()


def prepare(info, queries, keys, values):
    columns = queries.shape[1] + 2 * HEAD_DIM
    return pl.pallas_call(
        prepare_kernel,
        in_specs=[pl.BlockSpec(memory_space=pltpu.SMEM)]
        + [pl.BlockSpec(memory_space=pltpu.HBM)] * 3,
        out_specs=pl.BlockSpec(memory_space=pltpu.VMEM),
        out_shape=jax.ShapeDtypeStruct((BLK, columns), BF16),
        scratch_shapes=[pltpu.SemaphoreType.DMA((3,))],
        compiler_params=pltpu.CompilerParams(vmem_limit_bytes=VMEM_LIMIT),
        cost_estimate=pl.CostEstimate(
            flops=BLK * columns, bytes_accessed=4 * BLK * columns, transcendentals=0
        ),
        name="prepare",
    )(info, *off_chip(queries, keys, values))


def place_kernel(spots, columns, info_ref, *refs):
    pieces, out_ref, done = refs[: len(spots)], refs[-2], refs[-1]
    copies = []
    for i, (flip, at) in enumerate(spots):
        start = pl.multiple_of((info_ref[2] ^ flip) * columns + at, HEAD_DIM)
        target = out_ref.at[:, pl.ds(start, pieces[i].shape[1])]
        copies.append(pltpu.make_async_copy(pieces[i], target, done.at[i]))
    for copy in copies:
        copy.start()
    for copy in copies:
        copy.wait()


def place(info, output, pieces, columns):
    spots = [(flip, start * HEAD_DIM) for flip, start, _ in pieces]
    size = sum(piece.size for _, _, piece in pieces)
    return pl.pallas_call(
        functools.partial(place_kernel, spots, columns),
        in_specs=[pl.BlockSpec(memory_space=pltpu.SMEM)]
        + [pl.BlockSpec(memory_space=pltpu.VMEM)] * len(pieces)
        + [pl.BlockSpec(memory_space=pl.ANY)],
        out_specs=pl.BlockSpec(memory_space=pl.ANY),
        scratch_shapes=[pltpu.SemaphoreType.DMA((len(pieces),))],
        out_shape=jax.ShapeDtypeStruct(output.shape, output.dtype),
        input_output_aliases={len(pieces) + 1: 0},
        compiler_params=pltpu.CompilerParams(vmem_limit_bytes=VMEM_LIMIT),
        cost_estimate=pl.CostEstimate(flops=size, bytes_accessed=4 * size, transcendentals=0),
        name="place",
    )(info, *[piece for _, _, piece in pieces], output)


def body(queries, keys, values, mid_pool, coarse_pool):
    tokens_here, columns = queries.shape
    heads_here = columns // HEAD_DIM
    block_count = tokens_here // BLK
    members = lax.axis_size("head")
    length = lax.axis_size("seq")
    assert keys.shape[1] == HEAD_DIM and block_count == members
    assert block_count <= MIDB and members & (members - 1) == 0
    device = lax.axis_index("seq")
    member = lax.axis_index("head")
    hops = -(-(MIDB + 1) // block_count)
    last_blocks = MIDB + 1 - (hops - 1) * block_count
    slot = round_up(block_count, 8)

    away = members // 2

    def info(flip):
        return jnp.stack([member ^ flip, device, member]).astype(jnp.int32)

    early = prepare(info(away), queries, keys, values)
    early = exchange(early, "head", away)
    keys, values, coarse, mids, last, first = pool(
        keys, values, mid_pool, coarse_pool, block_count, last_blocks, slot
    )
    reach, step = 1, 0
    while reach < length:
        arriving = cyclic(coarse, "seq", reach)
        if step == 0:
            near = cyclic(first, "seq", 1)
        if 2 * reach >= length:
            (queries,) = load(queries)
        coarse = join(coarse, arriving)
        reach, step = 2 * reach, step + 1
    further = [cyclic(mids, "seq", by) for by in range(2, hops)]
    further += [cyclic(last, "seq", hops)]
    geometry = (block_count, hops, last_blocks, slot, reach)
    shared = (keys, values, near, *further, mids, coarse)

    late = pack(info(away), shared, coarse, geometry)
    after = late
    late = exchange(late, "head", away)
    arrived = []
    for flip in sent_flips(members):
        after = attend(info(flip), queries, shared, after, 0, heads_here, geometry)
        arrived.append((flip, 0, exchange(after, "head", flip)))
    output = attend(
        info(0), queries, shared, after, 0, heads_here, geometry, members * columns
    )
    output = attend_shipped(info(0), early, late, output, away, heads_here, geometry)
    output = place(info(0), output, [p for p in arrived if p[0] < away], columns)
    return place(info(0), output, [p for p in arrived if p[0] > away], columns)


def sent_flips(members):
    return [*range(members // 2 + 1, members), *range(1, members // 2)]


def solution(mesh):
    return jax.shard_map(
        body,
        mesh=mesh,
        in_specs=(
            P("seq", "head"),
            P("seq", "head"),
            P("seq", "head"),
            P("head", None),
            P("head", None),
        ),
        out_specs=P(("seq", "head"), None),
        check_vma=False,
    )
```

```python
import functools
import math

import jax
import jax.numpy as jnp
from jax import lax
from jax.experimental import pallas as pl
from jax.experimental.pallas import tpu as pltpu
from jax.sharding import PartitionSpec as P


HEAD_DIM = 128
BLK = 256
GROUP = 8
MIDS = 256
MIDB = 8
PER_GROUP = BLK // GROUP
LANES = 128
NEG = -1e30
HALF = BLK // 2
CHUNK = 32
SHARED = 7
VMEM_LIMIT = 16 * 1024 * 1024
ATTEND_LIMIT = 28 * 1024 * 1024
EXP_SCALE = math.log2(math.e) / math.sqrt(HEAD_DIM)
BF16 = jnp.bfloat16
F32 = jnp.float32


def round_up(value, multiple):
    return -(-value // multiple) * multiple


def cyclic(array, axis, by):
    size = lax.axis_size(axis)
    return lax.ppermute(array, axis, [(i, (i + by) % size) for i in range(size)])


def off_chip(*arrays):
    return [pltpu.with_memory_space_constraint(a, pltpu.HBM) for a in arrays]


def exchange(array, axis, flip):
    size = lax.axis_size(axis)
    return lax.ppermute(array, axis, [(i, i ^ flip) for i in range(size)])


def pool_kernel(block_count, slot, info_ref, queries_hbm, keys_hbm, values_hbm, mid_hbm, coarse_hbm,
                early_out, keys_ref, values_ref, near_out, tails_out, mid_ref, coarse_ref, arrived):
    wanted = pl.ds(pl.multiple_of(info_ref[0] * BLK, BLK), BLK)
    moves = [
        (mid_hbm, mid_ref),
        (coarse_hbm, coarse_ref),
        (keys_hbm, keys_ref),
        (values_hbm, values_ref),
    ]
    at = 0
    for source in (queries_hbm, keys_hbm, values_hbm):
        columns = slice(at, at + source.shape[1])
        moves.append((source.at[wanted, :], early_out.at[:, columns]))
        at += source.shape[1]
    copies = [
        pltpu.make_async_copy(source, target, arrived.at[i])
        for i, (source, target) in enumerate(moves)
    ]
    for copy in copies:
        copy.start()
    for copy in copies[:4]:
        copy.wait()
    rows = block_count * PER_GROUP
    repeat = (
        lax.broadcasted_iota(jnp.int32, (GROUP, BLK), 1) % GROUP
        == lax.broadcasted_iota(jnp.int32, (GROUP, BLK), 0)
    ).astype(BF16)
    tiled = jnp.dot(mid_ref[...], repeat, preferred_element_type=F32)
    owner = lax.broadcasted_iota(jnp.int32, (PER_GROUP, BLK), 1) // GROUP
    mine = owner == lax.broadcasted_iota(jnp.int32, (PER_GROUP, BLK), 0)
    mid_weights = jnp.where(mine, jnp.broadcast_to(tiled, (PER_GROUP, BLK)), 0.0)
    coarse_weights = coarse_ref[...].astype(F32)
    row = lax.broadcasted_iota(jnp.int32, (slot, BLK), 0)
    for which, source in enumerate((keys_ref, values_ref)):
        total = jnp.zeros((slot, HEAD_DIM), F32)
        for block in range(block_count):
            here = source[block * BLK : (block + 1) * BLK, :]
            weights = jnp.concatenate(
                [mid_weights, jnp.where(row == block, jnp.broadcast_to(coarse_weights, (slot, BLK)), 0.0)]
            ).astype(BF16)
            pooled = jnp.dot(weights, here, preferred_element_type=F32)
            total = total + pooled[PER_GROUP:]
            start = 2 * slot + which * rows + block * PER_GROUP
            near_out[start : start + PER_GROUP, :] = pooled[:PER_GROUP].astype(BF16)
        near_out[which * slot : (which + 1) * slot, :] = total.astype(BF16)
        edge = (block_count - 1) * BLK
        tails_out[which * BLK : (which + 1) * BLK, :] = source[edge : edge + BLK, :]
    for copy in copies[4:]:
        copy.wait()


def pool(info, queries, keys, values, mid_pool, coarse_pool, block_count, slot):
    shapes = (
        (BLK, queries.shape[1] + 2 * HEAD_DIM),
        keys.shape,
        values.shape,
        (2 * slot + 2 * block_count * PER_GROUP, HEAD_DIM),
        (2 * BLK, HEAD_DIM),
    )
    return pl.pallas_call(
        functools.partial(pool_kernel, block_count, slot),
        in_specs=[pl.BlockSpec(memory_space=pltpu.SMEM)]
        + [pl.BlockSpec(memory_space=pltpu.HBM)] * 5,
        out_specs=[pl.BlockSpec(memory_space=pltpu.VMEM) for _ in shapes],
        out_shape=[jax.ShapeDtypeStruct(shape, BF16) for shape in shapes],
        scratch_shapes=[
            pltpu.VMEM(mid_pool.shape, BF16),
            pltpu.VMEM(coarse_pool.shape, BF16),
            pltpu.SemaphoreType.DMA((7,)),
        ],
        cost_estimate=pl.CostEstimate(
            flops=4 * keys.size * (PER_GROUP + slot), bytes_accessed=6 * keys.size, transcendentals=0
        ),
        compiler_params=pltpu.CompilerParams(vmem_limit_bytes=VMEM_LIMIT),
        name="pool",
    )(info, *off_chip(queries, keys, values, mid_pool, coarse_pool))


def select_kernel(parts, *refs):
    out_ref, at = refs[-1], 0
    for index, start, size in parts:
        out_ref[at : at + size, :] = refs[index][start : start + size, :]
        at += size


def select(parts, *arrays):
    rows = sum(size for _, _, size in parts)
    return pl.pallas_call(
        functools.partial(select_kernel, parts),
        in_specs=[pl.BlockSpec(memory_space=pltpu.VMEM)] * len(arrays),
        out_specs=pl.BlockSpec(memory_space=pltpu.VMEM),
        out_shape=jax.ShapeDtypeStruct((rows, arrays[0].shape[1]), arrays[0].dtype),
        compiler_params=pltpu.CompilerParams(vmem_limit_bytes=VMEM_LIMIT),
        name="select",
    )(*arrays)


def load_kernel(*refs):
    count = len(refs) // 2
    copies = [
        pltpu.make_async_copy(refs[i], refs[count + i], refs[-1].at[i]) for i in range(count)
    ]
    for copy in copies:
        copy.start()
    for copy in copies:
        copy.wait()


def load(*arrays):
    return pl.pallas_call(
        load_kernel,
        in_specs=[pl.BlockSpec(memory_space=pltpu.HBM) for _ in arrays],
        out_specs=[pl.BlockSpec(memory_space=pltpu.VMEM) for _ in arrays],
        out_shape=[jax.ShapeDtypeStruct(a.shape, a.dtype) for a in arrays],
        scratch_shapes=[pltpu.SemaphoreType.DMA((len(arrays),))],
        compiler_params=pltpu.CompilerParams(vmem_limit_bytes=VMEM_LIMIT),
        cost_estimate=pl.CostEstimate(
            flops=2 * sum(a.size for a in arrays),
            bytes_accessed=4 * sum(a.size for a in arrays),
            transcendentals=0,
        ),
        name="load",
    )(*off_chip(*arrays))


def fill_summaries(geometry, target, width, sources, mid_scratch, which, write):
    block_count, last_blocks, slot, reach = geometry
    source = sources[which]
    tails_ref, near_ref, far_ref, mine_ref, coarse_ref = sources[2:]
    rows = block_count * PER_GROUP
    late = last_blocks * PER_GROUP
    at = 0
    for ref, start, size in (
        (far_ref, 2 * rows + which * late, late),
        (far_ref, which * rows, rows),
        (near_ref, 2 * slot + which * rows, rows),
        (mine_ref, 2 * slot + which * rows, rows),
    ):
        mid_scratch[at : at + size, :] = ref[start : start + size, :]
        at += size
    window = pl.ds(pl.multiple_of(target * PER_GROUP, PER_GROUP), MIDS)
    write(0, mid_scratch[window, :])
    wide = coarse_ref[...].astype(F32).reshape(reach, 2, slot, HEAD_DIM)[:, which]
    wide = wide.reshape(reach * slot, HEAD_DIM)
    if width > reach * slot:
        wide = jnp.concatenate([wide, jnp.zeros((width - reach * slot, HEAD_DIM), F32)])
    write(MIDS, wide.astype(BF16))
    before = pl.ds(pl.multiple_of(jnp.maximum(target - 1, 0) * BLK, BLK), BLK)
    write(MIDS + width, source[before, :])

    @pl.when(target == 0)
    def _():
        write(MIDS + width, tails_ref[which * BLK : (which + 1) * BLK, :])


def pack_kernel(geometry, info_ref, *refs):
    sources, (_, out_ref, mid_scratch) = refs[:-3], refs[-3:]
    _, _, slot, reach = geometry
    for which in range(2):
        columns = slice(which * HEAD_DIM, (which + 1) * HEAD_DIM)

        def write(at, value):
            out_ref[at : at + value.shape[0], columns] = value

        fill_summaries(geometry, info_ref[0], reach * slot, sources, mid_scratch, which, write)


def whole_in_vmem(count):
    return [pl.BlockSpec(memory_space=pltpu.VMEM)] * count


def mid_rows(geometry):
    block_count, last_blocks = geometry[:2]
    return (3 * block_count + last_blocks) * PER_GROUP


def pack(info, shared, after, geometry):
    _, _, slot, reach = geometry
    rows = MIDS + reach * slot + BLK
    return pl.pallas_call(
        functools.partial(pack_kernel, geometry),
        in_specs=[pl.BlockSpec(memory_space=pltpu.SMEM)]
        + whole_in_vmem(len(shared))
        + [pl.BlockSpec(memory_space=pl.ANY)],
        out_specs=pl.BlockSpec(memory_space=pltpu.VMEM),
        out_shape=jax.ShapeDtypeStruct((rows, 2 * HEAD_DIM), BF16),
        scratch_shapes=[pltpu.VMEM((mid_rows(geometry), HEAD_DIM), BF16)],
        compiler_params=pltpu.CompilerParams(vmem_limit_bytes=VMEM_LIMIT),
        cost_estimate=pl.CostEstimate(
            flops=rows * HEAD_DIM, bytes_accessed=8 * rows * HEAD_DIM, transcendentals=0
        ),
        name="pack",
    )(info, *shared, after)


def fill_bias(geometry, target, device, width, bias):
    block_count, _, slot, reach = geometry
    block = device * block_count + target
    coarse_at = MIDS
    prev_at = MIDS + width
    lane = lax.broadcasted_iota(jnp.int32, bias.shape, 1)
    mid_ok = lane >= (MIDB + 1 - block) * PER_GROUP
    far = (lane - coarse_at) // slot
    nth = (lane - coarse_at) % slot
    coarse_ok = (
        (nth < block_count)
        & (far < reach)
        & (far <= device)
        & (far * block_count - nth + target >= MIDB + 2)
    )
    mid_bias = jnp.where(mid_ok, 0.0, NEG)
    coarse_bias = jnp.where(coarse_ok, 0.0, NEG)
    prev_bias = jnp.where(block * (lane + 1) >= 1, 0.0, NEG)
    bias[...] = jnp.where(
        lane < coarse_at, mid_bias, jnp.where(lane < prev_at, coarse_bias, prev_bias)
    )


def attend_jobs(jobs, heads, scores, weights):
    group = max(1, heads // 2)
    units = [
        (job, first, half) for job in jobs for first in range(0, heads, group) for half in range(2)
    ]
    row = lax.broadcasted_iota(jnp.int32, (CHUNK, HALF), 0)
    column = lax.broadcasted_iota(jnp.int32, (CHUNK, HALF), 1)

    def score(unit):
        (q_ref, row_start, keys, _, bias, _), first, half = units[unit]
        seen = bias.shape[1] + (half + 1) * HALF
        rows_here = pl.ds(pl.multiple_of(row_start + half * HALF, HALF), HALF)
        stacked = jnp.concatenate([q_ref[rows_here, head_columns(first + i)] for i in range(group)])
        scores[unit % 2, :, :seen] = lax.dot_general(
            stacked, keys[:seen, :], (((1,), (1,)), ((), ())), preferred_element_type=F32
        )

    def weigh(unit):
        (_, _, _, _, bias, _), first, half = units[unit]
        own_at = bias.shape[1]
        seen = own_at + (half + 1) * HALF
        for at in range(0, group * HALF, CHUNK):
            here = slice(at, at + CHUNK)
            parts = [scores[unit % 2, here, :own_at] + bias[0:1, :]]
            if half:
                parts.append(scores[unit % 2, here, own_at : own_at + HALF])
            edge = scores[unit % 2, here, seen - HALF : seen]
            parts.append(jnp.where(row + at % HALF >= column, edge, NEG))
            chunk = jnp.concatenate(parts, axis=1)
            top = jnp.max(chunk, axis=-1, keepdims=True)
            weights[unit % 2, here, :seen] = jnp.exp2((chunk - top) * EXP_SCALE).astype(BF16)

    def mix(unit):
        (_, _, _, values, bias, emit), first, half = units[unit]
        seen = bias.shape[1] + (half + 1) * HALF
        mixed = jnp.dot(weights[unit % 2, :, :seen], values[:seen, :], preferred_element_type=F32)
        emit(first, group, half, (mixed[:, :HEAD_DIM] / mixed[:, HEAD_DIM:]).astype(BF16))

    for unit in range(len(units) + 2):
        if unit < len(units):
            score(unit)
        if 1 <= unit <= len(units):
            weigh(unit - 1)
        if unit >= 2:
            mix(unit - 2)


def head_columns(head):
    return slice(head * HEAD_DIM, (head + 1) * HEAD_DIM)


def store(ref, first_head, first, group, half, mixed):
    for i in range(group):
        ref[half * HALF : (half + 1) * HALF, head_columns(first_head + first + i)] = mixed[
            i * HALF : (i + 1) * HALF
        ]


def fill_local(geometry, width, info_ref, target, sources, mid_scratch, scratch):
    own_at = MIDS + width + BLK
    for which in range(2):
        everything = scratch[which]

        def write(at, value):
            everything[at : at + value.shape[0], :HEAD_DIM] = value

        fill_summaries(geometry, target, width, sources, mid_scratch, which, write)
        own = pl.ds(pl.multiple_of(target * BLK, BLK), BLK)
        write(own_at, sources[which][own, :])
    scratch[1][:, HEAD_DIM:] = jnp.ones((own_at + BLK, HEAD_DIM), BF16)
    fill_bias(geometry, target, info_ref[1], width, scratch[2])


def fill_shipped(geometry, width, info_ref, target, early_ref, late_ref, scratch):
    _, _, slot, reach = geometry
    used = MIDS + reach * slot
    own_at = MIDS + width + BLK
    for which in range(2):
        everything = scratch[which]
        columns = head_columns(which)
        everything[:used, :HEAD_DIM] = late_ref[:used, columns]
        if width > reach * slot:
            everything[used : MIDS + width, :HEAD_DIM] = jnp.zeros(
                (MIDS + width - used, HEAD_DIM), BF16
            )
        everything[MIDS + width : own_at, :HEAD_DIM] = late_ref[used:, columns]
        at = early_ref.shape[1] - (2 - which) * HEAD_DIM
        everything[own_at:, :HEAD_DIM] = early_ref[:, at : at + HEAD_DIM]
    scratch[1][:, HEAD_DIM:] = jnp.ones((own_at + BLK, HEAD_DIM), BF16)
    fill_bias(geometry, target, info_ref[1], width, scratch[2])


def attend_kernel(geometry, width, heads, info_ref, q_ref, *rest):
    sources, (_, out_ref, mid_scratch) = rest[:SHARED], rest[SHARED : SHARED + 3]
    scratch, (scores, weights) = rest[SHARED + 3 : SHARED + 6], rest[SHARED + 6 :]
    target = info_ref[0]
    fill_local(geometry, width, info_ref, target, sources, mid_scratch, scratch)
    emit = functools.partial(store, out_ref, 0)
    attend_jobs([(q_ref, target * BLK, *scratch, emit)], heads, scores, weights)


def finish_kernel(flip, geometry, width, heads, info_ref, q_ref, *rest):
    sources, rest = rest[:SHARED], rest[SHARED:]
    early_ref, late_ref, _, output, mid_scratch = rest[:5]
    rest = rest[2:]
    ours, theirs = rest[3:6], rest[6:9]
    scores, weights, results, sent = rest[9:]
    member = info_ref[2]
    copies = []

    fill_local(geometry, width, info_ref, info_ref[0], sources, mid_scratch, ours)
    fill_shipped(geometry, width, info_ref, info_ref[0], early_ref, late_ref, theirs)

    def emit(job, owner):
        def put(first, group, half, mixed):
            store(results, job * heads, first, group, half, mixed)
            if half:
                start = (job * heads + first) * HEAD_DIM
                size = group * HEAD_DIM
                at = pl.multiple_of((owner * heads + first) * HEAD_DIM, HEAD_DIM)
                copy = pltpu.make_async_copy(
                    results.at[:, start : start + size],
                    output.at[:, pl.ds(at, size)],
                    sent.at[len(copies)],
                )
                copies.append(copy)
                copy.start()

        return put

    attend_jobs(
        [
            (q_ref, info_ref[0] * BLK, *ours, emit(0, member)),
            (early_ref, 0, *theirs, emit(1, member ^ flip)),
        ],
        heads,
        scores,
        weights,
    )
    for copy in copies:
        copy.wait()


def context_scratch(total):
    return [
        pltpu.VMEM((total, HEAD_DIM), BF16),
        pltpu.VMEM((total, 2 * HEAD_DIM), BF16),
        pltpu.VMEM((8, total - BLK), F32),
    ]


def attend_call(kernel, operands, jobs, heads, geometry, out_columns, out_spec, extra):
    width = coarse_width(geometry)
    total = MIDS + width + 2 * BLK
    unit_rows = max(1, heads // 2) * HALF
    return pl.pallas_call(
        functools.partial(kernel, geometry, width, heads),
        in_specs=[pl.BlockSpec(memory_space=pltpu.SMEM)]
        + whole_in_vmem(len(operands) - 2)
        + [pl.BlockSpec(memory_space=pl.ANY)],
        out_specs=out_spec,
        scratch_shapes=[pltpu.VMEM((mid_rows(geometry), HEAD_DIM), BF16)]
        + context_scratch(total) * jobs
        + [
            pltpu.VMEM((2, unit_rows, total), F32),
            pltpu.VMEM((2, unit_rows, total), BF16),
        ]
        + extra,
        out_shape=jax.ShapeDtypeStruct((BLK, out_columns), BF16),
        compiler_params=pltpu.CompilerParams(vmem_limit_bytes=ATTEND_LIMIT),
        cost_estimate=pl.CostEstimate(
            flops=6 * jobs * BLK * heads * total * HEAD_DIM,
            bytes_accessed=4 * BLK * heads * HEAD_DIM + 1024 * 1024,
            transcendentals=jobs * BLK * heads * total,
        ),
        name="attend",
    )(*operands)


def coarse_width(geometry):
    return round_up(geometry[3] * geometry[2], LANES)


def attend(info, queries, shared, after, heads, geometry):
    return attend_call(
        attend_kernel,
        (info, queries, *shared, after),
        1,
        heads,
        geometry,
        heads * HEAD_DIM,
        pl.BlockSpec(memory_space=pltpu.VMEM),
        [],
    )


def finish(info, queries, shared, early, late, after, flip, heads, geometry, out_columns):
    kernel = functools.partial(finish_kernel, flip)
    groups = heads // max(1, heads // 2)
    return attend_call(
        kernel,
        (info, queries, *shared, early, late, after),
        2,
        heads,
        geometry,
        out_columns,
        pl.BlockSpec(memory_space=pl.ANY),
        [
            pltpu.VMEM((BLK, 2 * heads * HEAD_DIM), BF16),
            pltpu.SemaphoreType.DMA((2 * groups,)),
        ],
    )


def place_kernel(spots, columns, info_ref, *refs):
    pieces, out_ref, done = refs[: len(spots)], refs[-2], refs[-1]
    copies = []
    for i, (flip, at) in enumerate(spots):
        start = pl.multiple_of((info_ref[2] ^ flip) * columns + at, HEAD_DIM)
        target = out_ref.at[:, pl.ds(start, pieces[i].shape[1])]
        copies.append(pltpu.make_async_copy(pieces[i], target, done.at[i]))
    for copy in copies:
        copy.start()
    for copy in copies:
        copy.wait()


def place(info, output, pieces, columns):
    spots = [(flip, start * HEAD_DIM) for flip, start, _ in pieces]
    size = sum(piece.size for _, _, piece in pieces)
    return pl.pallas_call(
        functools.partial(place_kernel, spots, columns),
        in_specs=[pl.BlockSpec(memory_space=pltpu.SMEM)]
        + [pl.BlockSpec(memory_space=pltpu.VMEM)] * len(pieces)
        + [pl.BlockSpec(memory_space=pl.ANY)],
        out_specs=pl.BlockSpec(memory_space=pl.ANY),
        scratch_shapes=[pltpu.SemaphoreType.DMA((len(pieces),))],
        out_shape=jax.ShapeDtypeStruct(output.shape, output.dtype),
        input_output_aliases={len(pieces) + 1: 0},
        compiler_params=pltpu.CompilerParams(vmem_limit_bytes=VMEM_LIMIT),
        cost_estimate=pl.CostEstimate(flops=size, bytes_accessed=4 * size, transcendentals=0),
        name="place",
    )(info, *[piece for _, _, piece in pieces], output)


def body(queries, keys, values, mid_pool, coarse_pool):
    tokens_here, columns = queries.shape
    heads_here = columns // HEAD_DIM
    block_count = tokens_here // BLK
    members = lax.axis_size("head")
    length = lax.axis_size("seq")
    assert keys.shape[1] == HEAD_DIM and block_count == members
    assert block_count <= MIDB and members & (members - 1) == 0
    assert 2 * block_count <= MIDB < 3 * block_count
    device = lax.axis_index("seq")
    member = lax.axis_index("head")
    last_blocks = MIDB + 1 - 2 * block_count
    slot = round_up(block_count, 8)
    rows = block_count * PER_GROUP
    late_rows = last_blocks * PER_GROUP
    away = members // 2

    def info(flip):
        return jnp.stack([member ^ flip, device, member]).astype(jnp.int32)

    early, keys, values, mine, tails = pool(
        info(away), queries, keys, values, mid_pool, coarse_pool, block_count, slot
    )
    near = cyclic(mine, "seq", 1)
    early = exchange(early, "head", away)
    ends = [2 * slot + (i + 1) * rows - late_rows for i in range(2)]
    passing = select(
        [
            (0, 2 * slot, 2 * rows),
            *[(1, end, late_rows) for end in ends],
            (0, 0, 2 * slot),
            (1, 0, 2 * slot),
        ],
        mine,
        near,
    )
    far = cyclic(passing, "seq", 2)
    tails = cyclic(tails, "seq", 1)
    (queries,) = load(queries)
    summaries = 2 * rows + 2 * late_rows
    coarse = select([(0, summaries, 4 * slot), (1, summaries, 4 * slot)], passing, far)
    reach = 4
    while reach < length:
        arriving = cyclic(coarse, "seq", reach)
        size = coarse.shape[0]
        coarse = select([(0, 0, size), (1, 0, size)], coarse, arriving)
        reach *= 2
    geometry = (block_count, last_blocks, slot, reach)
    shared = (keys, values, tails, near, far, mine, coarse)

    late = pack(info(away), shared, coarse, geometry)
    after = late
    late = exchange(late, "head", away)
    arrived = []
    for flip in sent_flips(members):
        after = attend(info(flip), queries, shared, after, heads_here, geometry)
        arrived.append((flip, 0, exchange(after, "head", flip)))
    output = finish(
        info(0),
        queries,
        shared,
        early,
        late,
        after,
        away,
        heads_here,
        geometry,
        members * columns,
    )
    return place(info(0), output, arrived, columns)


def sent_flips(members):
    return [*range(members // 2 + 1, members), *range(1, members // 2)]


def solution(mesh):
    return jax.shard_map(
        body,
        mesh=mesh,
        in_specs=(
            P("seq", "head"),
            P("seq", "head"),
            P("seq", "head"),
            P("head", None),
            P("head", None),
        ),
        out_specs=P(("seq", "head"), None),
        check_vma=False,
    )
```

```python
import functools
import math

import jax
import jax.numpy as jnp
from jax import lax
from jax.experimental import pallas as pl
from jax.experimental.pallas import tpu as pltpu
from jax.sharding import PartitionSpec as P


HEAD_DIM = 128
BLK = 256
GROUP = 8
MIDS = 256
MIDB = 8
PER_GROUP = BLK // GROUP
LANES = 128
NEG = -1e30
HALF = BLK // 2
CHUNK = 32
SHARED = 8
VMEM_LIMIT = 16 * 1024 * 1024
ATTEND_LIMIT = 28 * 1024 * 1024
EXP_SCALE = math.log2(math.e) / math.sqrt(HEAD_DIM)
BF16 = jnp.bfloat16
F32 = jnp.float32


def round_up(value, multiple):
    return -(-value // multiple) * multiple


def cyclic(array, axis, by):
    size = lax.axis_size(axis)
    return lax.ppermute(array, axis, [(i, (i + by) % size) for i in range(size)])


def off_chip(*arrays):
    return [pltpu.with_memory_space_constraint(a, pltpu.HBM) for a in arrays]


def exchange(array, axis, flip):
    size = lax.axis_size(axis)
    return lax.ppermute(array, axis, [(i, i ^ flip) for i in range(size)])


def pool_kernel(block_count, last_blocks, slot, info_ref, queries_hbm, keys_hbm, values_hbm, mid_hbm, coarse_hbm,
                early_out, keys_ref, values_ref, near_out, third_out, tails_out, mid_ref, coarse_ref,
                arrived):
    wanted = pl.ds(pl.multiple_of(info_ref[0] * BLK, BLK), BLK)
    moves = [
        (mid_hbm, mid_ref),
        (coarse_hbm, coarse_ref),
        (keys_hbm, keys_ref),
        (values_hbm, values_ref),
    ]
    at = 0
    for source in (queries_hbm, keys_hbm, values_hbm):
        columns = slice(at, at + source.shape[1])
        moves.append((source.at[wanted, :], early_out.at[:, columns]))
        at += source.shape[1]
    copies = [
        pltpu.make_async_copy(source, target, arrived.at[i])
        for i, (source, target) in enumerate(moves)
    ]
    for copy in copies:
        copy.start()
    for copy in copies[:4]:
        copy.wait()
    rows = block_count * PER_GROUP
    repeat = (
        lax.broadcasted_iota(jnp.int32, (GROUP, BLK), 1) % GROUP
        == lax.broadcasted_iota(jnp.int32, (GROUP, BLK), 0)
    ).astype(BF16)
    tiled = jnp.dot(mid_ref[...], repeat, preferred_element_type=F32)
    owner = lax.broadcasted_iota(jnp.int32, (PER_GROUP, BLK), 1) // GROUP
    mine = owner == lax.broadcasted_iota(jnp.int32, (PER_GROUP, BLK), 0)
    mid_weights = jnp.where(mine, jnp.broadcast_to(tiled, (PER_GROUP, BLK)), 0.0)
    coarse_weights = coarse_ref[...].astype(F32)
    row = lax.broadcasted_iota(jnp.int32, (slot, BLK), 0)
    for which, source in enumerate((keys_ref, values_ref)):
        total = jnp.zeros((slot, HEAD_DIM), F32)
        for block in range(block_count):
            here = source[block * BLK : (block + 1) * BLK, :]
            weights = jnp.concatenate(
                [mid_weights, jnp.where(row == block, jnp.broadcast_to(coarse_weights, (slot, BLK)), 0.0)]
            ).astype(BF16)
            pooled = jnp.dot(weights, here, preferred_element_type=F32)
            total = total + pooled[PER_GROUP:]
            start = 2 * slot + which * rows + block * PER_GROUP
            mids = pooled[:PER_GROUP].astype(BF16)
            near_out[start : start + PER_GROUP, :] = mids
            nth = block - (block_count - last_blocks)
            if nth >= 0:
                start = 2 * slot + (which * last_blocks + nth) * PER_GROUP
                third_out[start : start + PER_GROUP, :] = mids
        near_out[which * slot : (which + 1) * slot, :] = total.astype(BF16)
        third_out[which * slot : (which + 1) * slot, :] = total.astype(BF16)
        edge = (block_count - 1) * BLK
        tails_out[which * BLK : (which + 1) * BLK, :] = source[edge : edge + BLK, :]
    for copy in copies[4:]:
        copy.wait()


def pool(info, queries, keys, values, mid_pool, coarse_pool, block_count, last_blocks, slot):
    shapes = (
        (BLK, queries.shape[1] + 2 * HEAD_DIM),
        keys.shape,
        values.shape,
        (2 * slot + 2 * block_count * PER_GROUP, HEAD_DIM),
        (2 * slot + 2 * last_blocks * PER_GROUP, HEAD_DIM),
        (2 * BLK, HEAD_DIM),
    )
    return pl.pallas_call(
        functools.partial(pool_kernel, block_count, last_blocks, slot),
        in_specs=[pl.BlockSpec(memory_space=pltpu.SMEM)]
        + [pl.BlockSpec(memory_space=pltpu.HBM)] * 5,
        out_specs=[pl.BlockSpec(memory_space=pltpu.VMEM) for _ in shapes],
        out_shape=[jax.ShapeDtypeStruct(shape, BF16) for shape in shapes],
        scratch_shapes=[
            pltpu.VMEM(mid_pool.shape, BF16),
            pltpu.VMEM(coarse_pool.shape, BF16),
            pltpu.SemaphoreType.DMA((7,)),
        ],
        cost_estimate=pl.CostEstimate(
            flops=4 * keys.size * (PER_GROUP + slot), bytes_accessed=6 * keys.size, transcendentals=0
        ),
        compiler_params=pltpu.CompilerParams(vmem_limit_bytes=VMEM_LIMIT),
        name="pool",
    )(info, *off_chip(queries, keys, values, mid_pool, coarse_pool))


def select_kernel(parts, *refs):
    out_ref, at = refs[-1], 0
    for index, start, size in parts:
        out_ref[at : at + size, :] = refs[index][start : start + size, :]
        at += size


def select(parts, *arrays):
    rows = sum(size for _, _, size in parts)
    return pl.pallas_call(
        functools.partial(select_kernel, parts),
        in_specs=[pl.BlockSpec(memory_space=pltpu.VMEM)] * len(arrays),
        out_specs=pl.BlockSpec(memory_space=pltpu.VMEM),
        out_shape=jax.ShapeDtypeStruct((rows, arrays[0].shape[1]), arrays[0].dtype),
        compiler_params=pltpu.CompilerParams(vmem_limit_bytes=VMEM_LIMIT),
        name="select",
    )(*arrays)


def load_kernel(*refs):
    count = len(refs) // 2
    copies = [
        pltpu.make_async_copy(refs[i], refs[count + i], refs[-1].at[i]) for i in range(count)
    ]
    for copy in copies:
        copy.start()
    for copy in copies:
        copy.wait()


def load(*arrays):
    return pl.pallas_call(
        load_kernel,
        in_specs=[pl.BlockSpec(memory_space=pltpu.HBM) for _ in arrays],
        out_specs=[pl.BlockSpec(memory_space=pltpu.VMEM) for _ in arrays],
        out_shape=[jax.ShapeDtypeStruct(a.shape, a.dtype) for a in arrays],
        scratch_shapes=[pltpu.SemaphoreType.DMA((len(arrays),))],
        compiler_params=pltpu.CompilerParams(vmem_limit_bytes=VMEM_LIMIT),
        cost_estimate=pl.CostEstimate(
            flops=2 * sum(a.size for a in arrays),
            bytes_accessed=4 * sum(a.size for a in arrays),
            transcendentals=0,
        ),
        name="load",
    )(*off_chip(*arrays))


def fill_late(geometry, target, prev_at, sources, mid_scratch, which, write):
    block_count, last_blocks, slot, _ = geometry
    source = sources[which]
    tails_ref, near_ref, far_ref, third_ref, mine_ref = sources[2:7]
    rows = block_count * PER_GROUP
    late = last_blocks * PER_GROUP
    at = 0
    for ref, start, size in (
        (third_ref, 2 * slot + which * late, late),
        (far_ref, 2 * slot + which * rows, rows),
        (near_ref, 2 * slot + which * rows, rows),
        (mine_ref, 2 * slot + which * rows, rows),
    ):
        mid_scratch[at : at + size, :] = ref[start : start + size, :]
        at += size
    window = pl.ds(pl.multiple_of(target * PER_GROUP, PER_GROUP), MIDS)
    write(0, mid_scratch[window, :])
    before = pl.ds(pl.multiple_of(jnp.maximum(target - 1, 0) * BLK, BLK), BLK)
    tail = tails_ref[which * BLK : (which + 1) * BLK, :]
    write(prev_at, jnp.where(target == 0, tail, source[before, :]))


def fill_coarse(geometry, width, coarse_ref, which, write):
    _, _, slot, reach = geometry
    wide = coarse_ref[...].astype(F32).reshape(reach, 2, slot, HEAD_DIM)[:, which]
    wide = wide.reshape(reach * slot, HEAD_DIM)
    if width > reach * slot:
        wide = jnp.concatenate([wide, jnp.zeros((width - reach * slot, HEAD_DIM), F32)])
    write(MIDS, wide.astype(BF16))


def pack_kernel(geometry, info_ref, *refs):
    sources, (_, out_ref, mid_scratch) = refs[:-3], refs[-3:]
    for which in range(2):
        columns = head_columns(which)

        def write(at, value):
            out_ref[at : at + value.shape[0], columns] = value

        fill_late(geometry, info_ref[0], MIDS, sources, mid_scratch, which, write)


def whole_in_vmem(count):
    return [pl.BlockSpec(memory_space=pltpu.VMEM)] * count


def mid_rows(geometry):
    block_count, last_blocks = geometry[:2]
    return (3 * block_count + last_blocks) * PER_GROUP


def pack(info, shared, after, geometry):
    rows = MIDS + BLK
    return pl.pallas_call(
        functools.partial(pack_kernel, geometry),
        in_specs=[pl.BlockSpec(memory_space=pltpu.SMEM)]
        + whole_in_vmem(len(shared))
        + [pl.BlockSpec(memory_space=pl.ANY)],
        out_specs=pl.BlockSpec(memory_space=pltpu.VMEM),
        out_shape=jax.ShapeDtypeStruct((rows, 2 * HEAD_DIM), BF16),
        scratch_shapes=[pltpu.VMEM((mid_rows(geometry), HEAD_DIM), BF16)],
        compiler_params=pltpu.CompilerParams(vmem_limit_bytes=VMEM_LIMIT),
        cost_estimate=pl.CostEstimate(
            flops=rows * HEAD_DIM, bytes_accessed=8 * rows * HEAD_DIM, transcendentals=0
        ),
        name="pack",
    )(info, *shared, after)


def fill_bias(geometry, target, device, width, bias):
    block_count, _, slot, reach = geometry
    block = device * block_count + target
    coarse_at = MIDS
    prev_at = MIDS + width
    lane = lax.broadcasted_iota(jnp.int32, bias.shape, 1)
    mid_ok = lane >= (MIDB + 1 - block) * PER_GROUP
    far = (lane - coarse_at) // slot
    nth = (lane - coarse_at) % slot
    coarse_ok = (
        (nth < block_count)
        & (far < reach)
        & (far <= device)
        & (far * block_count - nth + target >= MIDB + 2)
    )
    mid_bias = jnp.where(mid_ok, 0.0, NEG)
    coarse_bias = jnp.where(coarse_ok, 0.0, NEG)
    prev_bias = jnp.where(block * (lane + 1) >= 1, 0.0, NEG)
    bias[...] = jnp.where(
        lane < coarse_at, mid_bias, jnp.where(lane < prev_at, coarse_bias, prev_bias)
    )


def attend_jobs(jobs, heads, scores, weights):
    group = max(1, heads // 2)
    units = [
        (job, first, half) for job in jobs for first in range(0, heads, group) for half in range(2)
    ]
    row = lax.broadcasted_iota(jnp.int32, (CHUNK, HALF), 0)
    column = lax.broadcasted_iota(jnp.int32, (CHUNK, HALF), 1)

    def score(unit):
        (q_ref, row_start, keys, _, bias, _), first, half = units[unit]
        seen = bias.shape[1] + (half + 1) * HALF
        rows_here = pl.ds(pl.multiple_of(row_start + half * HALF, HALF), HALF)
        stacked = jnp.concatenate([q_ref[rows_here, head_columns(first + i)] for i in range(group)])
        scores[unit % 2, :, :seen] = lax.dot_general(
            stacked, keys[:seen, :], (((1,), (1,)), ((), ())), preferred_element_type=F32
        )

    def weigh(unit):
        (_, _, _, _, bias, _), first, half = units[unit]
        own_at = bias.shape[1]
        seen = own_at + (half + 1) * HALF
        for at in range(0, group * HALF, CHUNK):
            here = slice(at, at + CHUNK)
            parts = [scores[unit % 2, here, :own_at] + bias[0:1, :]]
            if half:
                parts.append(scores[unit % 2, here, own_at : own_at + HALF])
            edge = scores[unit % 2, here, seen - HALF : seen]
            parts.append(jnp.where(row + at % HALF >= column, edge, NEG))
            chunk = jnp.concatenate(parts, axis=1)
            top = jnp.max(chunk, axis=-1, keepdims=True)
            weights[unit % 2, here, :seen] = jnp.exp2((chunk - top) * EXP_SCALE).astype(BF16)

    def mix(unit):
        (_, _, _, values, bias, emit), first, half = units[unit]
        seen = bias.shape[1] + (half + 1) * HALF
        mixed = jnp.dot(weights[unit % 2, :, :seen], values[:seen, :], preferred_element_type=F32)
        emit(first, group, half, (mixed[:, :HEAD_DIM] / mixed[:, HEAD_DIM:]).astype(BF16))

    for unit in range(len(units) + 2):
        if unit < len(units):
            score(unit)
        if 1 <= unit <= len(units):
            weigh(unit - 1)
        if unit >= 2:
            mix(unit - 2)


def head_columns(head):
    return slice(head * HEAD_DIM, (head + 1) * HEAD_DIM)


def store(ref, first_head, first, group, half, mixed):
    for i in range(group):
        ref[half * HALF : (half + 1) * HALF, head_columns(first_head + first + i)] = mixed[
            i * HALF : (i + 1) * HALF
        ]


def fill_local(geometry, width, info_ref, target, sources, mid_scratch, scratch):
    own_at = MIDS + width + BLK
    for which in range(2):
        everything = scratch[which]

        def write(at, value):
            everything[at : at + value.shape[0], :HEAD_DIM] = value

        fill_late(geometry, target, MIDS + width, sources, mid_scratch, which, write)
        fill_coarse(geometry, width, sources[-1], which, write)
        own = pl.ds(pl.multiple_of(target * BLK, BLK), BLK)
        write(own_at, sources[which][own, :])
    scratch[1][:, HEAD_DIM:] = jnp.ones((own_at + BLK, HEAD_DIM), BF16)
    fill_bias(geometry, target, info_ref[1], width, scratch[2])


def fill_shipped(geometry, width, info_ref, target, early_ref, late_ref, coarse_ref, scratch):
    own_at = MIDS + width + BLK
    for which in range(2):
        everything = scratch[which]
        columns = head_columns(which)

        def write(at, value):
            everything[at : at + value.shape[0], :HEAD_DIM] = value

        write(0, late_ref[:MIDS, columns])
        fill_coarse(geometry, width, coarse_ref, which, write)
        write(MIDS + width, late_ref[MIDS:, columns])
        at = early_ref.shape[1] - (2 - which) * HEAD_DIM
        write(own_at, early_ref[:, at : at + HEAD_DIM])
    scratch[1][:, HEAD_DIM:] = jnp.ones((own_at + BLK, HEAD_DIM), BF16)
    fill_bias(geometry, target, info_ref[1], width, scratch[2])


def attend_kernel(geometry, width, heads, info_ref, q_ref, *rest):
    sources, (_, out_ref, mid_scratch) = rest[:SHARED], rest[SHARED : SHARED + 3]
    scratch, (scores, weights) = rest[SHARED + 3 : SHARED + 6], rest[SHARED + 6 :]
    target = info_ref[0]
    fill_local(geometry, width, info_ref, target, sources, mid_scratch, scratch)
    emit = functools.partial(store, out_ref, 0)
    attend_jobs([(q_ref, target * BLK, *scratch, emit)], heads, scores, weights)


def finish_kernel(flip, geometry, width, heads, info_ref, q_ref, *rest):
    sources, rest = rest[:SHARED], rest[SHARED:]
    early_ref, late_ref, coarse_ref, _, output, mid_scratch = rest[:6]
    rest = rest[3:]
    ours, theirs = rest[3:6], rest[6:9]
    scores, weights, results, sent = rest[9:]
    member = info_ref[2]
    copies = []

    fill_local(geometry, width, info_ref, info_ref[0], sources, mid_scratch, ours)
    fill_shipped(geometry, width, info_ref, info_ref[0], early_ref, late_ref, coarse_ref, theirs)

    def emit(job, owner):
        def put(first, group, half, mixed):
            store(results, job * heads, first, group, half, mixed)
            if half:
                start = (job * heads + first) * HEAD_DIM
                size = group * HEAD_DIM
                at = pl.multiple_of((owner * heads + first) * HEAD_DIM, HEAD_DIM)
                copy = pltpu.make_async_copy(
                    results.at[:, start : start + size],
                    output.at[:, pl.ds(at, size)],
                    sent.at[len(copies)],
                )
                copies.append(copy)
                copy.start()

        return put

    attend_jobs(
        [
            (q_ref, info_ref[0] * BLK, *ours, emit(0, member)),
            (early_ref, 0, *theirs, emit(1, member ^ flip)),
        ],
        heads,
        scores,
        weights,
    )
    for copy in copies:
        copy.wait()


def context_scratch(total):
    return [
        pltpu.VMEM((total, HEAD_DIM), BF16),
        pltpu.VMEM((total, 2 * HEAD_DIM), BF16),
        pltpu.VMEM((8, total - BLK), F32),
    ]


def attend_call(kernel, operands, jobs, heads, geometry, out_columns, out_spec, extra):
    width = coarse_width(geometry)
    total = MIDS + width + 2 * BLK
    unit_rows = max(1, heads // 2) * HALF
    return pl.pallas_call(
        functools.partial(kernel, geometry, width, heads),
        in_specs=[pl.BlockSpec(memory_space=pltpu.SMEM)]
        + whole_in_vmem(len(operands) - 2)
        + [pl.BlockSpec(memory_space=pl.ANY)],
        out_specs=out_spec,
        scratch_shapes=[pltpu.VMEM((mid_rows(geometry), HEAD_DIM), BF16)]
        + context_scratch(total) * jobs
        + [
            pltpu.VMEM((2, unit_rows, total), F32),
            pltpu.VMEM((2, unit_rows, total), BF16),
        ]
        + extra,
        out_shape=jax.ShapeDtypeStruct((BLK, out_columns), BF16),
        compiler_params=pltpu.CompilerParams(vmem_limit_bytes=ATTEND_LIMIT),
        cost_estimate=pl.CostEstimate(
            flops=6 * jobs * BLK * heads * total * HEAD_DIM,
            bytes_accessed=4 * BLK * heads * HEAD_DIM + 1024 * 1024,
            transcendentals=jobs * BLK * heads * total,
        ),
        name="attend",
    )(*operands)


def coarse_width(geometry):
    return round_up(geometry[3] * geometry[2], LANES)


def attend(info, queries, shared, after, heads, geometry):
    return attend_call(
        attend_kernel,
        (info, queries, *shared, after),
        1,
        heads,
        geometry,
        heads * HEAD_DIM,
        pl.BlockSpec(memory_space=pltpu.VMEM),
        [],
    )


def finish(info, queries, shared, shipped, after, flip, heads, geometry, out_columns):
    kernel = functools.partial(finish_kernel, flip)
    groups = heads // max(1, heads // 2)
    return attend_call(
        kernel,
        (info, queries, *shared, *shipped, after),
        2,
        heads,
        geometry,
        out_columns,
        pl.BlockSpec(memory_space=pl.ANY),
        [
            pltpu.VMEM((BLK, 2 * heads * HEAD_DIM), BF16),
            pltpu.SemaphoreType.DMA((2 * groups,)),
        ],
    )


def place_kernel(spots, columns, info_ref, *refs):
    pieces, out_ref, done = refs[: len(spots)], refs[-2], refs[-1]
    copies = []
    for i, (flip, at) in enumerate(spots):
        start = pl.multiple_of((info_ref[2] ^ flip) * columns + at, HEAD_DIM)
        target = out_ref.at[:, pl.ds(start, pieces[i].shape[1])]
        copies.append(pltpu.make_async_copy(pieces[i], target, done.at[i]))
    for copy in copies:
        copy.start()
    for copy in copies:
        copy.wait()


def place(info, output, pieces, columns):
    spots = [(flip, start * HEAD_DIM) for flip, start, _ in pieces]
    size = sum(piece.size for _, _, piece in pieces)
    return pl.pallas_call(
        functools.partial(place_kernel, spots, columns),
        in_specs=[pl.BlockSpec(memory_space=pltpu.SMEM)]
        + [pl.BlockSpec(memory_space=pltpu.VMEM)] * len(pieces)
        + [pl.BlockSpec(memory_space=pl.ANY)],
        out_specs=pl.BlockSpec(memory_space=pl.ANY),
        scratch_shapes=[pltpu.SemaphoreType.DMA((len(pieces),))],
        out_shape=jax.ShapeDtypeStruct(output.shape, output.dtype),
        input_output_aliases={len(pieces) + 1: 0},
        compiler_params=pltpu.CompilerParams(vmem_limit_bytes=VMEM_LIMIT),
        cost_estimate=pl.CostEstimate(flops=size, bytes_accessed=4 * size, transcendentals=0),
        name="place",
    )(info, *[piece for _, _, piece in pieces], output)


def body(queries, keys, values, mid_pool, coarse_pool):
    tokens_here, columns = queries.shape
    heads_here = columns // HEAD_DIM
    block_count = tokens_here // BLK
    members = lax.axis_size("head")
    length = lax.axis_size("seq")
    assert keys.shape[1] == HEAD_DIM and block_count == members
    assert block_count <= MIDB and members & (members - 1) == 0
    assert 2 * block_count <= MIDB < 3 * block_count
    device = lax.axis_index("seq")
    member = lax.axis_index("head")
    last_blocks = MIDB + 1 - 2 * block_count
    slot = round_up(block_count, 8)
    away = members // 2

    def info(flip):
        return jnp.stack([member ^ flip, device, member]).astype(jnp.int32)

    early, keys, values, mine, third, tails = pool(
        info(away), queries, keys, values, mid_pool, coarse_pool, block_count, last_blocks, slot
    )
    near = cyclic(mine, "seq", 1)
    early = exchange(early, "head", away)
    far = cyclic(mine, "seq", 2)
    third = cyclic(third, "seq", 3)
    tails = cyclic(tails, "seq", 1)
    (queries,) = load(queries)
    coarse = select([(i, 0, 2 * slot) for i in range(4)], mine, near, far, third)
    reach = 4
    while reach < length:
        arriving = cyclic(coarse, "seq", reach)
        size = coarse.shape[0]
        coarse = select([(0, 0, size), (1, 0, size)], coarse, arriving)
        reach *= 2
    geometry = (block_count, last_blocks, slot, reach)
    late = pack(info(away), (keys, values, tails, near, far, third, mine), far, geometry)
    late = exchange(late, "head", away)
    shipped = (early, late, exchange(coarse, "head", away))

    shared = (keys, values, tails, near, far, third, mine, coarse)
    after = coarse
    arrived = []
    for flip in sent_flips(members):
        after = attend(info(flip), queries, shared, after, heads_here, geometry)
        arrived.append((flip, 0, exchange(after, "head", flip)))
    output = finish(
        info(0),
        queries,
        shared,
        shipped,
        after,
        away,
        heads_here,
        geometry,
        members * columns,
    )
    return place(info(0), output, arrived, columns)


def sent_flips(members):
    return [*range(members // 2 + 1, members), *range(1, members // 2)]


def solution(mesh):
    return jax.shard_map(
        body,
        mesh=mesh,
        in_specs=(
            P("seq", "head"),
            P("seq", "head"),
            P("seq", "head"),
            P("head", None),
            P("head", None),
        ),
        out_specs=P(("seq", "head"), None),
        check_vma=False,
    )
```

```python
import functools
import math

import jax
import jax.numpy as jnp
from jax import lax
from jax.experimental import pallas as pl
from jax.experimental.pallas import tpu as pltpu
from jax.sharding import PartitionSpec as P


HEAD_DIM = 128
BLK = 256
GROUP = 8
MIDS = 256
MIDB = 8
PER_GROUP = BLK // GROUP
LANES = 128
NEG = -1e30
HALF = BLK // 2
CHUNK = 32
SHARED = 8
VMEM_LIMIT = 16 * 1024 * 1024
ATTEND_LIMIT = 28 * 1024 * 1024
EXP_SCALE = math.log2(math.e) / math.sqrt(HEAD_DIM)
BF16 = jnp.bfloat16
F32 = jnp.float32


def round_up(value, multiple):
    return -(-value // multiple) * multiple


def cyclic(array, axis, by):
    size = lax.axis_size(axis)
    return lax.ppermute(array, axis, [(i, (i + by) % size) for i in range(size)])


def off_chip(*arrays):
    return [pltpu.with_memory_space_constraint(a, pltpu.HBM) for a in arrays]


def exchange(array, axis, flip):
    size = lax.axis_size(axis)
    return lax.ppermute(array, axis, [(i, i ^ flip) for i in range(size)])


def block_of(flip):
    return lax.axis_index("head") ^ flip


def pool_kernel(block_count, last_blocks, slot, flip, queries_hbm, keys_hbm, values_hbm, mid_hbm, coarse_hbm,
                early_out, keys_ref, values_ref, near_out, third_out, tails_out, mid_ref, coarse_ref,
                arrived):
    wanted = pl.ds(pl.multiple_of(block_of(flip) * BLK, BLK), BLK)
    moves = [
        (mid_hbm, mid_ref),
        (coarse_hbm, coarse_ref),
        (keys_hbm, keys_ref),
        (values_hbm, values_ref),
    ]
    at = 0
    for source in (queries_hbm, keys_hbm, values_hbm):
        columns = slice(at, at + source.shape[1])
        moves.append((source.at[wanted, :], early_out.at[:, columns]))
        at += source.shape[1]
    copies = [
        pltpu.make_async_copy(source, target, arrived.at[i])
        for i, (source, target) in enumerate(moves)
    ]
    for copy in copies:
        copy.start()
    for copy in copies[:4]:
        copy.wait()
    rows = block_count * PER_GROUP
    repeat = (
        lax.broadcasted_iota(jnp.int32, (GROUP, BLK), 1) % GROUP
        == lax.broadcasted_iota(jnp.int32, (GROUP, BLK), 0)
    ).astype(BF16)
    tiled = jnp.dot(mid_ref[...], repeat, preferred_element_type=F32)
    owner = lax.broadcasted_iota(jnp.int32, (PER_GROUP, BLK), 1) // GROUP
    mine = owner == lax.broadcasted_iota(jnp.int32, (PER_GROUP, BLK), 0)
    mid_weights = jnp.where(mine, jnp.broadcast_to(tiled, (PER_GROUP, BLK)), 0.0)
    coarse_weights = coarse_ref[...].astype(F32)
    row = lax.broadcasted_iota(jnp.int32, (slot, BLK), 0)
    for which, source in enumerate((keys_ref, values_ref)):
        total = jnp.zeros((slot, HEAD_DIM), F32)
        for block in range(block_count):
            here = source[block * BLK : (block + 1) * BLK, :]
            weights = jnp.concatenate(
                [mid_weights, jnp.where(row == block, jnp.broadcast_to(coarse_weights, (slot, BLK)), 0.0)]
            ).astype(BF16)
            pooled = jnp.dot(weights, here, preferred_element_type=F32)
            total = total + pooled[PER_GROUP:]
            start = 2 * slot + which * rows + block * PER_GROUP
            mids = pooled[:PER_GROUP].astype(BF16)
            near_out[start : start + PER_GROUP, :] = mids
            nth = block - (block_count - last_blocks)
            if nth >= 0:
                start = 2 * slot + (which * last_blocks + nth) * PER_GROUP
                third_out[start : start + PER_GROUP, :] = mids
        near_out[which * slot : (which + 1) * slot, :] = total.astype(BF16)
        third_out[which * slot : (which + 1) * slot, :] = total.astype(BF16)
        edge = (block_count - 1) * BLK
        tails_out[which * BLK : (which + 1) * BLK, :] = source[edge : edge + BLK, :]
    for copy in copies[4:]:
        copy.wait()


def pool(flip, queries, keys, values, mid_pool, coarse_pool, block_count, last_blocks, slot):
    shapes = (
        (BLK, queries.shape[1] + 2 * HEAD_DIM),
        keys.shape,
        values.shape,
        (2 * slot + 2 * block_count * PER_GROUP, HEAD_DIM),
        (2 * slot + 2 * last_blocks * PER_GROUP, HEAD_DIM),
        (2 * BLK, HEAD_DIM),
    )
    return pl.pallas_call(
        functools.partial(pool_kernel, block_count, last_blocks, slot, flip),
        in_specs=[pl.BlockSpec(memory_space=pltpu.HBM)] * 5,
        out_specs=[pl.BlockSpec(memory_space=pltpu.VMEM) for _ in shapes],
        out_shape=[jax.ShapeDtypeStruct(shape, BF16) for shape in shapes],
        scratch_shapes=[
            pltpu.VMEM(mid_pool.shape, BF16),
            pltpu.VMEM(coarse_pool.shape, BF16),
            pltpu.SemaphoreType.DMA((7,)),
        ],
        cost_estimate=pl.CostEstimate(
            flops=4 * keys.size * (PER_GROUP + slot), bytes_accessed=6 * keys.size, transcendentals=0
        ),
        compiler_params=pltpu.CompilerParams(vmem_limit_bytes=VMEM_LIMIT),
        name="pool",
    )(*off_chip(queries, keys, values, mid_pool, coarse_pool))


def select_kernel(parts, *refs):
    out_ref, at = refs[-1], 0
    for index, start, size in parts:
        out_ref[at : at + size, :] = refs[index][start : start + size, :]
        at += size


def select(parts, *arrays):
    rows = sum(size for _, _, size in parts)
    return pl.pallas_call(
        functools.partial(select_kernel, parts),
        in_specs=[pl.BlockSpec(memory_space=pltpu.VMEM)] * len(arrays),
        out_specs=pl.BlockSpec(memory_space=pltpu.VMEM),
        out_shape=jax.ShapeDtypeStruct((rows, arrays[0].shape[1]), arrays[0].dtype),
        compiler_params=pltpu.CompilerParams(vmem_limit_bytes=VMEM_LIMIT),
        name="select",
    )(*arrays)


def load_kernel(*refs):
    count = len(refs) // 2
    copies = [
        pltpu.make_async_copy(refs[i], refs[count + i], refs[-1].at[i]) for i in range(count)
    ]
    for copy in copies:
        copy.start()
    for copy in copies:
        copy.wait()


def load(*arrays):
    return pl.pallas_call(
        load_kernel,
        in_specs=[pl.BlockSpec(memory_space=pltpu.HBM) for _ in arrays],
        out_specs=[pl.BlockSpec(memory_space=pltpu.VMEM) for _ in arrays],
        out_shape=[jax.ShapeDtypeStruct(a.shape, a.dtype) for a in arrays],
        scratch_shapes=[pltpu.SemaphoreType.DMA((len(arrays),))],
        compiler_params=pltpu.CompilerParams(vmem_limit_bytes=VMEM_LIMIT),
        cost_estimate=pl.CostEstimate(
            flops=2 * sum(a.size for a in arrays),
            bytes_accessed=4 * sum(a.size for a in arrays),
            transcendentals=0,
        ),
        name="load",
    )(*off_chip(*arrays))


def fill_late(geometry, target, prev_at, sources, mid_scratch, which, write):
    block_count, last_blocks, slot, _ = geometry
    source = sources[which]
    tails_ref, near_ref, far_ref, third_ref, mine_ref = sources[2:7]
    rows = block_count * PER_GROUP
    late = last_blocks * PER_GROUP
    at = 0
    for ref, start, size in (
        (third_ref, 2 * slot + which * late, late),
        (far_ref, 2 * slot + which * rows, rows),
        (near_ref, 2 * slot + which * rows, rows),
        (mine_ref, 2 * slot + which * rows, rows),
    ):
        mid_scratch[at : at + size, :] = ref[start : start + size, :]
        at += size
    window = pl.ds(pl.multiple_of(target * PER_GROUP, PER_GROUP), MIDS)
    write(0, mid_scratch[window, :])
    before = pl.ds(pl.multiple_of(jnp.maximum(target - 1, 0) * BLK, BLK), BLK)
    tail = tails_ref[which * BLK : (which + 1) * BLK, :]
    write(prev_at, jnp.where(target == 0, tail, source[before, :]))


def fill_coarse(geometry, width, coarse_ref, which, write):
    _, _, slot, reach = geometry
    wide = coarse_ref[...].astype(F32).reshape(reach, 2, slot, HEAD_DIM)[:, which]
    wide = wide.reshape(reach * slot, HEAD_DIM)
    if width > reach * slot:
        wide = jnp.concatenate([wide, jnp.zeros((width - reach * slot, HEAD_DIM), F32)])
    write(MIDS, wide.astype(BF16))


def pack_kernel(geometry, flip, *refs):
    sources, (_, out_ref, mid_scratch) = refs[:-3], refs[-3:]
    for which in range(2):
        columns = head_columns(which)

        def write(at, value):
            out_ref[at : at + value.shape[0], columns] = value

        fill_late(geometry, block_of(flip), MIDS, sources, mid_scratch, which, write)


def whole_in_vmem(count):
    return [pl.BlockSpec(memory_space=pltpu.VMEM)] * count


def mid_rows(geometry):
    block_count, last_blocks = geometry[:2]
    return (3 * block_count + last_blocks) * PER_GROUP


def pack(flip, shared, after, geometry):
    rows = MIDS + BLK
    return pl.pallas_call(
        functools.partial(pack_kernel, geometry, flip),
        in_specs=whole_in_vmem(len(shared))
        + [pl.BlockSpec(memory_space=pl.ANY)],
        out_specs=pl.BlockSpec(memory_space=pltpu.VMEM),
        out_shape=jax.ShapeDtypeStruct((rows, 2 * HEAD_DIM), BF16),
        scratch_shapes=[pltpu.VMEM((mid_rows(geometry), HEAD_DIM), BF16)],
        compiler_params=pltpu.CompilerParams(vmem_limit_bytes=VMEM_LIMIT),
        cost_estimate=pl.CostEstimate(
            flops=rows * HEAD_DIM, bytes_accessed=8 * rows * HEAD_DIM, transcendentals=0
        ),
        name="pack",
    )(*shared, after)


def fill_bias(geometry, target, device, width, bias):
    block_count, _, slot, reach = geometry
    block = device * block_count + target
    coarse_at = MIDS
    prev_at = MIDS + width
    lane = lax.broadcasted_iota(jnp.int32, bias.shape, 1)
    mid_ok = lane >= (MIDB + 1 - block) * PER_GROUP
    far = (lane - coarse_at) // slot
    nth = (lane - coarse_at) % slot
    coarse_ok = (
        (nth < block_count)
        & (far < reach)
        & (far <= device)
        & (far * block_count - nth + target >= MIDB + 2)
    )
    mid_bias = jnp.where(mid_ok, 0.0, NEG)
    coarse_bias = jnp.where(coarse_ok, 0.0, NEG)
    prev_bias = jnp.where(block * (lane + 1) >= 1, 0.0, NEG)
    bias[...] = jnp.where(
        lane < coarse_at, mid_bias, jnp.where(lane < prev_at, coarse_bias, prev_bias)
    )


def attend_jobs(jobs, heads, scores, weights):
    group = max(1, heads // 2)
    units = [
        (job, first, half) for job in jobs for first in range(0, heads, group) for half in range(2)
    ]
    row = lax.broadcasted_iota(jnp.int32, (CHUNK, HALF), 0)
    column = lax.broadcasted_iota(jnp.int32, (CHUNK, HALF), 1)

    def score(unit):
        (q_ref, row_start, keys, _, bias, _), first, half = units[unit]
        seen = bias.shape[1] + (half + 1) * HALF
        rows_here = pl.ds(pl.multiple_of(row_start + half * HALF, HALF), HALF)
        stacked = jnp.concatenate([q_ref[rows_here, head_columns(first + i)] for i in range(group)])
        scores[unit % 2, :, :seen] = lax.dot_general(
            stacked, keys[:seen, :], (((1,), (1,)), ((), ())), preferred_element_type=F32
        )

    def weigh(unit):
        (_, _, _, _, bias, _), first, half = units[unit]
        own_at = bias.shape[1]
        seen = own_at + (half + 1) * HALF
        for at in range(0, group * HALF, CHUNK):
            here = slice(at, at + CHUNK)
            parts = [scores[unit % 2, here, :own_at] + bias[0:1, :]]
            if half:
                parts.append(scores[unit % 2, here, own_at : own_at + HALF])
            edge = scores[unit % 2, here, seen - HALF : seen]
            parts.append(jnp.where(row + at % HALF >= column, edge, NEG))
            chunk = jnp.concatenate(parts, axis=1)
            top = jnp.max(chunk, axis=-1, keepdims=True)
            weights[unit % 2, here, :seen] = jnp.exp2((chunk - top) * EXP_SCALE).astype(BF16)

    def mix(unit):
        (_, _, _, values, bias, emit), first, half = units[unit]
        seen = bias.shape[1] + (half + 1) * HALF
        mixed = jnp.dot(weights[unit % 2, :, :seen], values[:seen, :], preferred_element_type=F32)
        emit(first, group, half, (mixed[:, :HEAD_DIM] / mixed[:, HEAD_DIM:]).astype(BF16))

    for unit in range(len(units) + 2):
        if unit < len(units):
            score(unit)
        if 1 <= unit <= len(units):
            weigh(unit - 1)
        if unit >= 2:
            mix(unit - 2)


def head_columns(head):
    return slice(head * HEAD_DIM, (head + 1) * HEAD_DIM)


def store(ref, first_head, first, group, half, mixed):
    for i in range(group):
        ref[half * HALF : (half + 1) * HALF, head_columns(first_head + first + i)] = mixed[
            i * HALF : (i + 1) * HALF
        ]


def fill_local(geometry, width, target, sources, mid_scratch, scratch):
    own_at = MIDS + width + BLK
    for which in range(2):
        everything = scratch[which]

        def write(at, value):
            everything[at : at + value.shape[0], :HEAD_DIM] = value

        fill_late(geometry, target, MIDS + width, sources, mid_scratch, which, write)
        fill_coarse(geometry, width, sources[-1], which, write)
        own = pl.ds(pl.multiple_of(target * BLK, BLK), BLK)
        write(own_at, sources[which][own, :])
    scratch[1][:, HEAD_DIM:] = jnp.ones((own_at + BLK, HEAD_DIM), BF16)
    fill_bias(geometry, target, lax.axis_index("seq"), width, scratch[2])


def fill_shipped(geometry, width, target, early_ref, late_ref, coarse_ref, scratch):
    own_at = MIDS + width + BLK
    for which in range(2):
        everything = scratch[which]
        columns = head_columns(which)

        def write(at, value):
            everything[at : at + value.shape[0], :HEAD_DIM] = value

        write(0, late_ref[:MIDS, columns])
        fill_coarse(geometry, width, coarse_ref, which, write)
        write(MIDS + width, late_ref[MIDS:, columns])
        at = early_ref.shape[1] - (2 - which) * HEAD_DIM
        write(own_at, early_ref[:, at : at + HEAD_DIM])
    scratch[1][:, HEAD_DIM:] = jnp.ones((own_at + BLK, HEAD_DIM), BF16)
    fill_bias(geometry, target, lax.axis_index("seq"), width, scratch[2])


def attend_kernel(flip, geometry, width, heads, q_ref, *rest):
    sources, (_, out_ref, mid_scratch) = rest[:SHARED], rest[SHARED : SHARED + 3]
    scratch, (scores, weights) = rest[SHARED + 3 : SHARED + 6], rest[SHARED + 6 :]
    target = block_of(flip)
    fill_local(geometry, width, target, sources, mid_scratch, scratch)
    emit = functools.partial(store, out_ref, 0)
    attend_jobs([(q_ref, target * BLK, *scratch, emit)], heads, scores, weights)


def finish_kernel(flip, geometry, width, heads, q_ref, *rest):
    sources, rest = rest[:SHARED], rest[SHARED:]
    early_ref, late_ref, coarse_ref, _, output, mid_scratch = rest[:6]
    rest = rest[3:]
    ours, theirs = rest[3:6], rest[6:9]
    scores, weights, results, sent = rest[9:]
    member = block_of(0)
    copies = []

    fill_local(geometry, width, member, sources, mid_scratch, ours)
    fill_shipped(geometry, width, member, early_ref, late_ref, coarse_ref, theirs)

    def emit(job, owner):
        def put(first, group, half, mixed):
            store(results, job * heads, first, group, half, mixed)
            if half:
                start = (job * heads + first) * HEAD_DIM
                size = group * HEAD_DIM
                at = pl.multiple_of((owner * heads + first) * HEAD_DIM, HEAD_DIM)
                copy = pltpu.make_async_copy(
                    results.at[:, start : start + size],
                    output.at[:, pl.ds(at, size)],
                    sent.at[len(copies)],
                )
                copies.append(copy)
                copy.start()

        return put

    attend_jobs(
        [
            (q_ref, member * BLK, *ours, emit(0, member)),
            (early_ref, 0, *theirs, emit(1, member ^ flip)),
        ],
        heads,
        scores,
        weights,
    )
    for copy in copies:
        copy.wait()


def context_scratch(total):
    return [
        pltpu.VMEM((total, HEAD_DIM), BF16),
        pltpu.VMEM((total, 2 * HEAD_DIM), BF16),
        pltpu.VMEM((8, total - BLK), F32),
    ]


def attend_call(kernel, operands, jobs, heads, geometry, out_columns, out_spec, extra):
    width = coarse_width(geometry)
    total = MIDS + width + 2 * BLK
    unit_rows = max(1, heads // 2) * HALF
    return pl.pallas_call(
        functools.partial(kernel, geometry, width, heads),
        in_specs=whole_in_vmem(len(operands) - 1)
        + [pl.BlockSpec(memory_space=pl.ANY)],
        out_specs=out_spec,
        scratch_shapes=[pltpu.VMEM((mid_rows(geometry), HEAD_DIM), BF16)]
        + context_scratch(total) * jobs
        + [
            pltpu.VMEM((2, unit_rows, total), F32),
            pltpu.VMEM((2, unit_rows, total), BF16),
        ]
        + extra,
        out_shape=jax.ShapeDtypeStruct((BLK, out_columns), BF16),
        compiler_params=pltpu.CompilerParams(vmem_limit_bytes=ATTEND_LIMIT),
        cost_estimate=pl.CostEstimate(
            flops=6 * jobs * BLK * heads * total * HEAD_DIM,
            bytes_accessed=4 * BLK * heads * HEAD_DIM + 1024 * 1024,
            transcendentals=jobs * BLK * heads * total,
        ),
        name="attend",
    )(*operands)


def coarse_width(geometry):
    return round_up(geometry[3] * geometry[2], LANES)


def attend(flip, queries, shared, after, heads, geometry):
    return attend_call(
        functools.partial(attend_kernel, flip),
        (queries, *shared, after),
        1,
        heads,
        geometry,
        heads * HEAD_DIM,
        pl.BlockSpec(memory_space=pltpu.VMEM),
        [],
    )


def finish(queries, shared, shipped, after, flip, heads, geometry, out_columns):
    kernel = functools.partial(finish_kernel, flip)
    groups = heads // max(1, heads // 2)
    return attend_call(
        kernel,
        (queries, *shared, *shipped, after),
        2,
        heads,
        geometry,
        out_columns,
        pl.BlockSpec(memory_space=pl.ANY),
        [
            pltpu.VMEM((BLK, 2 * heads * HEAD_DIM), BF16),
            pltpu.SemaphoreType.DMA((2 * groups,)),
        ],
    )


def place_kernel(spots, columns, *refs):
    pieces, out_ref, done = refs[: len(spots)], refs[-2], refs[-1]
    copies = []
    for i, (flip, at) in enumerate(spots):
        start = pl.multiple_of(block_of(flip) * columns + at, HEAD_DIM)
        target = out_ref.at[:, pl.ds(start, pieces[i].shape[1])]
        copies.append(pltpu.make_async_copy(pieces[i], target, done.at[i]))
    for copy in copies:
        copy.start()
    for copy in copies:
        copy.wait()


def place(output, pieces, columns):
    spots = [(flip, start * HEAD_DIM) for flip, start, _ in pieces]
    size = sum(piece.size for _, _, piece in pieces)
    return pl.pallas_call(
        functools.partial(place_kernel, spots, columns),
        in_specs=[pl.BlockSpec(memory_space=pltpu.VMEM)] * len(pieces)
        + [pl.BlockSpec(memory_space=pl.ANY)],
        out_specs=pl.BlockSpec(memory_space=pl.ANY),
        scratch_shapes=[pltpu.SemaphoreType.DMA((len(pieces),))],
        out_shape=jax.ShapeDtypeStruct(output.shape, output.dtype),
        input_output_aliases={len(pieces): 0},
        compiler_params=pltpu.CompilerParams(vmem_limit_bytes=VMEM_LIMIT),
        cost_estimate=pl.CostEstimate(flops=size, bytes_accessed=4 * size, transcendentals=0),
        name="place",
    )(*[piece for _, _, piece in pieces], output)


def body(queries, keys, values, mid_pool, coarse_pool):
    tokens_here, columns = queries.shape
    heads_here = columns // HEAD_DIM
    block_count = tokens_here // BLK
    members = lax.axis_size("head")
    length = lax.axis_size("seq")
    assert keys.shape[1] == HEAD_DIM and block_count == members
    assert block_count <= MIDB and members & (members - 1) == 0
    assert 2 * block_count <= MIDB < 3 * block_count
    last_blocks = MIDB + 1 - 2 * block_count
    slot = round_up(block_count, 8)
    away = members // 2

    early, keys, values, mine, third, tails = pool(
        away, queries, keys, values, mid_pool, coarse_pool, block_count, last_blocks, slot
    )
    near = cyclic(mine, "seq", 1)
    early = exchange(early, "head", away)
    far = cyclic(mine, "seq", 2)
    third = cyclic(third, "seq", 3)
    tails = cyclic(tails, "seq", 1)
    (queries,) = load(queries)
    coarse = select([(i, 0, 2 * slot) for i in range(4)], mine, near, far, third)
    reach = 4
    while reach < length:
        arriving = cyclic(coarse, "seq", reach)
        size = coarse.shape[0]
        coarse = select([(0, 0, size), (1, 0, size)], coarse, arriving)
        reach *= 2
    geometry = (block_count, last_blocks, slot, reach)
    late = pack(away, (keys, values, tails, near, far, third, mine), far, geometry)
    late = exchange(late, "head", away)
    shipped = (early, late, exchange(coarse, "head", away))

    shared = (keys, values, tails, near, far, third, mine, coarse)
    after = coarse
    arrived = []
    for flip in sent_flips(members):
        after = attend(flip, queries, shared, after, heads_here, geometry)
        arrived.append((flip, 0, exchange(after, "head", flip)))
    output = finish(queries, shared, shipped, after, away, heads_here, geometry, members * columns)
    return place(output, arrived, columns)


def sent_flips(members):
    return [*range(members // 2 + 1, members), *range(1, members // 2)]


def solution(mesh):
    return jax.shard_map(
        body,
        mesh=mesh,
        in_specs=(
            P("seq", "head"),
            P("seq", "head"),
            P("seq", "head"),
            P("head", None),
            P("head", None),
        ),
        out_specs=P(("seq", "head"), None),
        check_vma=False,
    )
```

```python
import functools
import math

import jax
import jax.numpy as jnp
from jax import lax
from jax.experimental import pallas as pl
from jax.experimental.pallas import tpu as pltpu
from jax.sharding import PartitionSpec as P


HEAD_DIM = 128
BLK = 256
GROUP = 8
MIDS = 256
MIDB = 8
PER_GROUP = BLK // GROUP
LANES = 128
NEG = -1e30
HALF = BLK // 2
CHUNK = 32
SHARED = 8
VMEM_LIMIT = 16 * 1024 * 1024
ATTEND_LIMIT = 28 * 1024 * 1024
EXP_SCALE = math.log2(math.e) / math.sqrt(HEAD_DIM)
BF16 = jnp.bfloat16
F32 = jnp.float32


def round_up(value, multiple):
    return -(-value // multiple) * multiple


def cyclic(array, axis, by):
    size = lax.axis_size(axis)
    return lax.ppermute(array, axis, [(i, (i + by) % size) for i in range(size)])


def off_chip(*arrays):
    return [pltpu.with_memory_space_constraint(a, pltpu.HBM) for a in arrays]


def exchange(array, axis, flip):
    size = lax.axis_size(axis)
    return lax.ppermute(array, axis, [(i, i ^ flip) for i in range(size)])


def block_of(flip):
    return lax.axis_index("head") ^ flip


def pool_kernel(block_count, last_blocks, slot, flip, queries_hbm, keys_hbm, values_hbm, mid_hbm, coarse_hbm,
                early_out, keys_ref, values_ref, near_out, third_out, tails_out, mid_ref, coarse_ref,
                arrived):
    wanted = pl.ds(pl.multiple_of(block_of(flip) * BLK, BLK), BLK)
    moves = [
        (mid_hbm, mid_ref),
        (coarse_hbm, coarse_ref),
        (keys_hbm, keys_ref),
        (values_hbm, values_ref),
    ]
    at = 0
    for source in (queries_hbm, keys_hbm, values_hbm):
        columns = slice(at, at + source.shape[1])
        moves.append((source.at[wanted, :], early_out.at[:, columns]))
        at += source.shape[1]
    copies = [
        pltpu.make_async_copy(source, target, arrived.at[i])
        for i, (source, target) in enumerate(moves)
    ]
    for copy in copies:
        copy.start()
    for copy in copies[:4]:
        copy.wait()
    rows = block_count * PER_GROUP
    repeat = (
        lax.broadcasted_iota(jnp.int32, (GROUP, BLK), 1) % GROUP
        == lax.broadcasted_iota(jnp.int32, (GROUP, BLK), 0)
    ).astype(BF16)
    tiled = jnp.dot(mid_ref[...], repeat, preferred_element_type=F32)
    owner = lax.broadcasted_iota(jnp.int32, (PER_GROUP, BLK), 1) // GROUP
    mine = owner == lax.broadcasted_iota(jnp.int32, (PER_GROUP, BLK), 0)
    mid_weights = jnp.where(mine, jnp.broadcast_to(tiled, (PER_GROUP, BLK)), 0.0)
    coarse_weights = jnp.broadcast_to(coarse_ref[...].astype(F32), (slot, BLK))
    row = lax.broadcasted_iota(jnp.int32, (slot, BLK), 0)
    total = jnp.zeros((slot, HEAD_DIM), F32)
    for which, source in enumerate((keys_ref, values_ref)):
        for block in range(block_count):
            here = source[block * BLK : (block + 1) * BLK, :]
            weights = jnp.concatenate(
                [
                    mid_weights,
                    jnp.where(row == which * block_count + block, coarse_weights, 0.0),
                ]
            ).astype(BF16)
            pooled = jnp.dot(weights, here, preferred_element_type=F32)
            total = total + pooled[PER_GROUP:]
            start = slot + which * rows + block * PER_GROUP
            mids = pooled[:PER_GROUP].astype(BF16)
            near_out[start : start + PER_GROUP, :] = mids
            nth = block - (block_count - last_blocks)
            if nth >= 0:
                start = slot + (which * last_blocks + nth) * PER_GROUP
                third_out[start : start + PER_GROUP, :] = mids
        edge = (block_count - 1) * BLK
        tails_out[which * BLK : (which + 1) * BLK, :] = source[edge : edge + BLK, :]
    near_out[:slot, :] = total.astype(BF16)
    third_out[:slot, :] = total.astype(BF16)
    for copy in copies[4:]:
        copy.wait()


def pool(flip, queries, keys, values, mid_pool, coarse_pool, block_count, last_blocks, slot):
    shapes = (
        (BLK, queries.shape[1] + 2 * HEAD_DIM),
        keys.shape,
        values.shape,
        (slot + 2 * block_count * PER_GROUP, HEAD_DIM),
        (slot + 2 * last_blocks * PER_GROUP, HEAD_DIM),
        (2 * BLK, HEAD_DIM),
    )
    return pl.pallas_call(
        functools.partial(pool_kernel, block_count, last_blocks, slot, flip),
        in_specs=[pl.BlockSpec(memory_space=pltpu.HBM)] * 5,
        out_specs=[pl.BlockSpec(memory_space=pltpu.VMEM) for _ in shapes],
        out_shape=[jax.ShapeDtypeStruct(shape, BF16) for shape in shapes],
        scratch_shapes=[
            pltpu.VMEM(mid_pool.shape, BF16),
            pltpu.VMEM(coarse_pool.shape, BF16),
            pltpu.SemaphoreType.DMA((7,)),
        ],
        cost_estimate=pl.CostEstimate(
            flops=4 * keys.size * (PER_GROUP + slot), bytes_accessed=6 * keys.size, transcendentals=0
        ),
        compiler_params=pltpu.CompilerParams(vmem_limit_bytes=VMEM_LIMIT),
        name="pool",
    )(*off_chip(queries, keys, values, mid_pool, coarse_pool))


def select_kernel(parts, *refs):
    out_ref, at = refs[-1], 0
    for index, start, size in parts:
        out_ref[at : at + size, :] = refs[index][start : start + size, :]
        at += size


def select(parts, *arrays):
    rows = sum(size for _, _, size in parts)
    return pl.pallas_call(
        functools.partial(select_kernel, parts),
        in_specs=[pl.BlockSpec(memory_space=pltpu.VMEM)] * len(arrays),
        out_specs=pl.BlockSpec(memory_space=pltpu.VMEM),
        out_shape=jax.ShapeDtypeStruct((rows, arrays[0].shape[1]), arrays[0].dtype),
        compiler_params=pltpu.CompilerParams(vmem_limit_bytes=VMEM_LIMIT),
        name="select",
    )(*arrays)


def load_kernel(*refs):
    count = len(refs) // 2
    copies = [
        pltpu.make_async_copy(refs[i], refs[count + i], refs[-1].at[i]) for i in range(count)
    ]
    for copy in copies:
        copy.start()
    for copy in copies:
        copy.wait()


def load(*arrays):
    return pl.pallas_call(
        load_kernel,
        in_specs=[pl.BlockSpec(memory_space=pltpu.HBM) for _ in arrays],
        out_specs=[pl.BlockSpec(memory_space=pltpu.VMEM) for _ in arrays],
        out_shape=[jax.ShapeDtypeStruct(a.shape, a.dtype) for a in arrays],
        scratch_shapes=[pltpu.SemaphoreType.DMA((len(arrays),))],
        compiler_params=pltpu.CompilerParams(vmem_limit_bytes=VMEM_LIMIT),
        cost_estimate=pl.CostEstimate(
            flops=2 * sum(a.size for a in arrays),
            bytes_accessed=4 * sum(a.size for a in arrays),
            transcendentals=0,
        ),
        name="load",
    )(*off_chip(*arrays))


def fill_late(geometry, target, prev_at, sources, mid_scratch, which, write):
    block_count, last_blocks, slot, _ = geometry
    source = sources[which]
    tails_ref, near_ref, far_ref, third_ref, mine_ref = sources[2:7]
    rows = block_count * PER_GROUP
    late = last_blocks * PER_GROUP
    at = 0
    for ref, start, size in (
        (third_ref, slot + which * late, late),
        (far_ref, slot + which * rows, rows),
        (near_ref, slot + which * rows, rows),
        (mine_ref, slot + which * rows, rows),
    ):
        mid_scratch[at : at + size, :] = ref[start : start + size, :]
        at += size
    window = pl.ds(pl.multiple_of(target * PER_GROUP, PER_GROUP), MIDS)
    write(0, mid_scratch[window, :])
    before = pl.ds(pl.multiple_of(jnp.maximum(target - 1, 0) * BLK, BLK), BLK)
    tail = tails_ref[which * BLK : (which + 1) * BLK, :]
    write(prev_at, jnp.where(target == 0, tail, source[before, :]))


def fill_coarse(geometry, width, coarse_ref, which, write):
    block_count, _, slot, reach = geometry
    wide = coarse_ref[...].astype(F32)
    if which:
        wide = pltpu.roll(wide, reach * slot - block_count, 0)
    if width > reach * slot:
        wide = jnp.concatenate([wide, jnp.zeros((width - reach * slot, HEAD_DIM), F32)])
    write(MIDS, wide.astype(BF16))


def pack_kernel(geometry, flip, *refs):
    sources, (_, out_ref, mid_scratch) = refs[:-3], refs[-3:]
    for which in range(2):
        columns = head_columns(which)

        def write(at, value):
            out_ref[at : at + value.shape[0], columns] = value

        fill_late(geometry, block_of(flip), MIDS, sources, mid_scratch, which, write)


def whole_in_vmem(count):
    return [pl.BlockSpec(memory_space=pltpu.VMEM)] * count


def mid_rows(geometry):
    block_count, last_blocks = geometry[:2]
    return (3 * block_count + last_blocks) * PER_GROUP


def pack(flip, shared, after, geometry):
    rows = MIDS + BLK
    return pl.pallas_call(
        functools.partial(pack_kernel, geometry, flip),
        in_specs=whole_in_vmem(len(shared))
        + [pl.BlockSpec(memory_space=pl.ANY)],
        out_specs=pl.BlockSpec(memory_space=pltpu.VMEM),
        out_shape=jax.ShapeDtypeStruct((rows, 2 * HEAD_DIM), BF16),
        scratch_shapes=[pltpu.VMEM((mid_rows(geometry), HEAD_DIM), BF16)],
        compiler_params=pltpu.CompilerParams(vmem_limit_bytes=VMEM_LIMIT),
        cost_estimate=pl.CostEstimate(
            flops=rows * HEAD_DIM, bytes_accessed=8 * rows * HEAD_DIM, transcendentals=0
        ),
        name="pack",
    )(*shared, after)


def fill_bias(geometry, target, device, width, bias):
    block_count, _, slot, reach = geometry
    block = device * block_count + target
    coarse_at = MIDS
    prev_at = MIDS + width
    lane = lax.broadcasted_iota(jnp.int32, bias.shape, 1)
    mid_ok = lane >= (MIDB + 1 - block) * PER_GROUP
    far = (lane - coarse_at) // slot
    nth = (lane - coarse_at) % slot
    coarse_ok = (
        (nth < block_count)
        & (far < reach)
        & (far <= device)
        & (far * block_count - nth + target >= MIDB + 2)
    )
    mid_bias = jnp.where(mid_ok, 0.0, NEG)
    coarse_bias = jnp.where(coarse_ok, 0.0, NEG)
    prev_bias = jnp.where(block * (lane + 1) >= 1, 0.0, NEG)
    bias[...] = jnp.where(
        lane < coarse_at, mid_bias, jnp.where(lane < prev_at, coarse_bias, prev_bias)
    )


def attend_jobs(jobs, heads, scores, weights):
    group = max(1, heads // 2)
    units = [
        (job, first, half) for job in jobs for first in range(0, heads, group) for half in range(2)
    ]
    row = lax.broadcasted_iota(jnp.int32, (CHUNK, HALF), 0)
    column = lax.broadcasted_iota(jnp.int32, (CHUNK, HALF), 1)

    def score(unit):
        (q_ref, row_start, keys, _, bias, _), first, half = units[unit]
        seen = bias.shape[1] + (half + 1) * HALF
        rows_here = pl.ds(pl.multiple_of(row_start + half * HALF, HALF), HALF)
        stacked = jnp.concatenate([q_ref[rows_here, head_columns(first + i)] for i in range(group)])
        scores[unit % 2, :, :seen] = lax.dot_general(
            stacked, keys[:seen, :], (((1,), (1,)), ((), ())), preferred_element_type=F32
        )

    def weigh(unit):
        (_, _, _, _, bias, _), first, half = units[unit]
        own_at = bias.shape[1]
        seen = own_at + (half + 1) * HALF
        for at in range(0, group * HALF, CHUNK):
            here = slice(at, at + CHUNK)
            parts = [scores[unit % 2, here, :own_at] + bias[0:1, :]]
            if half:
                parts.append(scores[unit % 2, here, own_at : own_at + HALF])
            edge = scores[unit % 2, here, seen - HALF : seen]
            parts.append(jnp.where(row + at % HALF >= column, edge, NEG))
            chunk = jnp.concatenate(parts, axis=1)
            top = jnp.max(chunk, axis=-1, keepdims=True)
            weights[unit % 2, here, :seen] = jnp.exp2((chunk - top) * EXP_SCALE).astype(BF16)

    def mix(unit):
        (_, _, _, values, bias, emit), first, half = units[unit]
        seen = bias.shape[1] + (half + 1) * HALF
        mixed = jnp.dot(weights[unit % 2, :, :seen], values[:seen, :], preferred_element_type=F32)
        emit(first, group, half, (mixed[:, :HEAD_DIM] / mixed[:, HEAD_DIM:]).astype(BF16))

    for unit in range(len(units) + 2):
        if unit < len(units):
            score(unit)
        if 1 <= unit <= len(units):
            weigh(unit - 1)
        if unit >= 2:
            mix(unit - 2)


def head_columns(head):
    return slice(head * HEAD_DIM, (head + 1) * HEAD_DIM)


def store(ref, first_head, first, group, half, mixed):
    for i in range(group):
        ref[half * HALF : (half + 1) * HALF, head_columns(first_head + first + i)] = mixed[
            i * HALF : (i + 1) * HALF
        ]


def fill_local(geometry, width, target, sources, mid_scratch, scratch):
    own_at = MIDS + width + BLK
    for which in range(2):
        everything = scratch[which]

        def write(at, value):
            everything[at : at + value.shape[0], :HEAD_DIM] = value

        fill_late(geometry, target, MIDS + width, sources, mid_scratch, which, write)
        fill_coarse(geometry, width, sources[-1], which, write)
        own = pl.ds(pl.multiple_of(target * BLK, BLK), BLK)
        write(own_at, sources[which][own, :])
    scratch[1][:, HEAD_DIM:] = jnp.ones((own_at + BLK, HEAD_DIM), BF16)
    fill_bias(geometry, target, lax.axis_index("seq"), width, scratch[2])


def fill_shipped(geometry, width, target, early_ref, late_ref, coarse_ref, scratch):
    own_at = MIDS + width + BLK
    for which in range(2):
        everything = scratch[which]
        columns = head_columns(which)

        def write(at, value):
            everything[at : at + value.shape[0], :HEAD_DIM] = value

        write(0, late_ref[:MIDS, columns])
        fill_coarse(geometry, width, coarse_ref, which, write)
        write(MIDS + width, late_ref[MIDS:, columns])
        at = early_ref.shape[1] - (2 - which) * HEAD_DIM
        write(own_at, early_ref[:, at : at + HEAD_DIM])
    scratch[1][:, HEAD_DIM:] = jnp.ones((own_at + BLK, HEAD_DIM), BF16)
    fill_bias(geometry, target, lax.axis_index("seq"), width, scratch[2])


def attend_kernel(flip, geometry, width, heads, q_ref, *rest):
    sources, (_, out_ref, mid_scratch) = rest[:SHARED], rest[SHARED : SHARED + 3]
    scratch, (scores, weights) = rest[SHARED + 3 : SHARED + 6], rest[SHARED + 6 :]
    target = block_of(flip)
    fill_local(geometry, width, target, sources, mid_scratch, scratch)
    emit = functools.partial(store, out_ref, 0)
    attend_jobs([(q_ref, target * BLK, *scratch, emit)], heads, scores, weights)


def finish_kernel(flip, geometry, width, heads, q_ref, *rest):
    sources, rest = rest[:SHARED], rest[SHARED:]
    early_ref, late_ref, coarse_ref, _, output, mid_scratch = rest[:6]
    rest = rest[3:]
    ours, theirs = rest[3:6], rest[6:9]
    scores, weights, results, sent = rest[9:]
    member = block_of(0)
    copies = []

    fill_local(geometry, width, member, sources, mid_scratch, ours)
    fill_shipped(geometry, width, member, early_ref, late_ref, coarse_ref, theirs)

    def emit(job, owner):
        def put(first, group, half, mixed):
            store(results, job * heads, first, group, half, mixed)
            if half:
                start = (job * heads + first) * HEAD_DIM
                size = group * HEAD_DIM
                at = pl.multiple_of((owner * heads + first) * HEAD_DIM, HEAD_DIM)
                copy = pltpu.make_async_copy(
                    results.at[:, start : start + size],
                    output.at[:, pl.ds(at, size)],
                    sent.at[len(copies)],
                )
                copies.append(copy)
                copy.start()

        return put

    attend_jobs(
        [
            (q_ref, member * BLK, *ours, emit(0, member)),
            (early_ref, 0, *theirs, emit(1, member ^ flip)),
        ],
        heads,
        scores,
        weights,
    )
    for copy in copies:
        copy.wait()


def context_scratch(total):
    return [
        pltpu.VMEM((total, HEAD_DIM), BF16),
        pltpu.VMEM((total, 2 * HEAD_DIM), BF16),
        pltpu.VMEM((8, total - BLK), F32),
    ]


def attend_call(kernel, operands, jobs, heads, geometry, out_columns, out_spec, extra):
    width = coarse_width(geometry)
    total = MIDS + width + 2 * BLK
    unit_rows = max(1, heads // 2) * HALF
    return pl.pallas_call(
        functools.partial(kernel, geometry, width, heads),
        in_specs=whole_in_vmem(len(operands) - 1)
        + [pl.BlockSpec(memory_space=pl.ANY)],
        out_specs=out_spec,
        scratch_shapes=[pltpu.VMEM((mid_rows(geometry), HEAD_DIM), BF16)]
        + context_scratch(total) * jobs
        + [
            pltpu.VMEM((2, unit_rows, total), F32),
            pltpu.VMEM((2, unit_rows, total), BF16),
        ]
        + extra,
        out_shape=jax.ShapeDtypeStruct((BLK, out_columns), BF16),
        compiler_params=pltpu.CompilerParams(vmem_limit_bytes=ATTEND_LIMIT),
        cost_estimate=pl.CostEstimate(
            flops=6 * jobs * BLK * heads * total * HEAD_DIM,
            bytes_accessed=4 * BLK * heads * HEAD_DIM + 1024 * 1024,
            transcendentals=jobs * BLK * heads * total,
        ),
        name="attend",
    )(*operands)


def coarse_width(geometry):
    return round_up(geometry[3] * geometry[2], LANES)


def attend(flip, queries, shared, after, heads, geometry):
    return attend_call(
        functools.partial(attend_kernel, flip),
        (queries, *shared, after),
        1,
        heads,
        geometry,
        heads * HEAD_DIM,
        pl.BlockSpec(memory_space=pltpu.VMEM),
        [],
    )


def finish(queries, shared, shipped, after, flip, heads, geometry, out_columns):
    kernel = functools.partial(finish_kernel, flip)
    groups = heads // max(1, heads // 2)
    return attend_call(
        kernel,
        (queries, *shared, *shipped, after),
        2,
        heads,
        geometry,
        out_columns,
        pl.BlockSpec(memory_space=pl.ANY),
        [
            pltpu.VMEM((BLK, 2 * heads * HEAD_DIM), BF16),
            pltpu.SemaphoreType.DMA((2 * groups,)),
        ],
    )


def place_kernel(spots, columns, *refs):
    pieces, out_ref, done = refs[: len(spots)], refs[-2], refs[-1]
    copies = []
    for i, (flip, at) in enumerate(spots):
        start = pl.multiple_of(block_of(flip) * columns + at, HEAD_DIM)
        target = out_ref.at[:, pl.ds(start, pieces[i].shape[1])]
        copies.append(pltpu.make_async_copy(pieces[i], target, done.at[i]))
    for copy in copies:
        copy.start()
    for copy in copies:
        copy.wait()


def place(output, pieces, columns):
    spots = [(flip, start * HEAD_DIM) for flip, start, _ in pieces]
    size = sum(piece.size for _, _, piece in pieces)
    return pl.pallas_call(
        functools.partial(place_kernel, spots, columns),
        in_specs=[pl.BlockSpec(memory_space=pltpu.VMEM)] * len(pieces)
        + [pl.BlockSpec(memory_space=pl.ANY)],
        out_specs=pl.BlockSpec(memory_space=pl.ANY),
        scratch_shapes=[pltpu.SemaphoreType.DMA((len(pieces),))],
        out_shape=jax.ShapeDtypeStruct(output.shape, output.dtype),
        input_output_aliases={len(pieces): 0},
        compiler_params=pltpu.CompilerParams(vmem_limit_bytes=VMEM_LIMIT),
        cost_estimate=pl.CostEstimate(flops=size, bytes_accessed=4 * size, transcendentals=0),
        name="place",
    )(*[piece for _, _, piece in pieces], output)


def body(queries, keys, values, mid_pool, coarse_pool):
    tokens_here, columns = queries.shape
    heads_here = columns // HEAD_DIM
    block_count = tokens_here // BLK
    members = lax.axis_size("head")
    length = lax.axis_size("seq")
    assert keys.shape[1] == HEAD_DIM and block_count == members
    assert block_count <= MIDB and members & (members - 1) == 0
    assert 2 * block_count <= MIDB < 3 * block_count
    last_blocks = MIDB + 1 - 2 * block_count
    slot = round_up(2 * block_count, 8)
    away = members // 2

    early, keys, values, mine, third, tails = pool(
        away, queries, keys, values, mid_pool, coarse_pool, block_count, last_blocks, slot
    )
    near = cyclic(mine, "seq", 1)
    early = exchange(early, "head", away)
    far = cyclic(mine, "seq", 2)
    third = cyclic(third, "seq", 3)
    tails = cyclic(tails, "seq", 1)
    (queries,) = load(queries)
    coarse = select([(i, 0, slot) for i in range(4)], mine, near, far, third)
    reach = 4
    while reach < length:
        arriving = cyclic(coarse, "seq", reach)
        size = coarse.shape[0]
        coarse = select([(0, 0, size), (1, 0, size)], coarse, arriving)
        reach *= 2
    geometry = (block_count, last_blocks, slot, reach)
    late = pack(away, (keys, values, tails, near, far, third, mine), far, geometry)
    late = exchange(late, "head", away)
    shipped = (early, late, exchange(coarse, "head", away))

    shared = (keys, values, tails, near, far, third, mine, coarse)
    after = coarse
    arrived = []
    for flip in sent_flips(members):
        after = attend(flip, queries, shared, after, heads_here, geometry)
        arrived.append((flip, 0, exchange(after, "head", flip)))
    output = finish(queries, shared, shipped, after, away, heads_here, geometry, members * columns)
    return place(output, arrived, columns)


def sent_flips(members):
    return [*range(members // 2 + 1, members), *range(1, members // 2)]


def solution(mesh):
    return jax.shard_map(
        body,
        mesh=mesh,
        in_specs=(
            P("seq", "head"),
            P("seq", "head"),
            P("seq", "head"),
            P("head", None),
            P("head", None),
        ),
        out_specs=P(("seq", "head"), None),
        check_vma=False,
    )
```

```python
import functools
import math

import jax
import jax.numpy as jnp
from jax import lax
from jax.experimental import pallas as pl
from jax.experimental.pallas import tpu as pltpu
from jax.sharding import PartitionSpec as P


HEAD_DIM = 128
BLK = 256
GROUP = 8
MIDS = 256
MIDB = 8
PER_GROUP = BLK // GROUP
LANES = 128
NEG = -1e30
HALF = BLK // 2
CHUNK = 32
SHARED = 8
VMEM_LIMIT = 16 * 1024 * 1024
ATTEND_LIMIT = 28 * 1024 * 1024
EXP_SCALE = math.log2(math.e) / math.sqrt(HEAD_DIM)
BF16 = jnp.bfloat16
F32 = jnp.float32


def round_up(value, multiple):
    return -(-value // multiple) * multiple


def cyclic(array, axis, by):
    size = lax.axis_size(axis)
    return lax.ppermute(array, axis, [(i, (i + by) % size) for i in range(size)])


def off_chip(*arrays):
    return [pltpu.with_memory_space_constraint(a, pltpu.HBM) for a in arrays]


def exchange(array, axis, flip):
    size = lax.axis_size(axis)
    return lax.ppermute(array, axis, [(i, i ^ flip) for i in range(size)])


def block_of(flip):
    return lax.axis_index("head") ^ flip


def pool_kernel(block_count, last_blocks, slot, flip, queries_hbm, keys_hbm, values_hbm, mid_hbm, coarse_hbm,
                early_out, keys_ref, values_ref, near_out, third_out, tails_out, mid_ref, coarse_ref,
                arrived):
    wanted = pl.ds(pl.multiple_of(block_of(flip) * BLK, BLK), BLK)
    moves = [
        (mid_hbm, mid_ref),
        (coarse_hbm, coarse_ref),
        (keys_hbm, keys_ref),
        (values_hbm, values_ref),
    ]
    at = 0
    for source in (queries_hbm, keys_hbm, values_hbm):
        columns = slice(at, at + source.shape[1])
        moves.append((source.at[wanted, :], early_out.at[:, columns]))
        at += source.shape[1]
    copies = [
        pltpu.make_async_copy(source, target, arrived.at[i])
        for i, (source, target) in enumerate(moves)
    ]
    for copy in copies:
        copy.start()
    for copy in copies[:4]:
        copy.wait()
    rows = block_count * PER_GROUP
    repeat = (
        lax.broadcasted_iota(jnp.int32, (GROUP, BLK), 1) % GROUP
        == lax.broadcasted_iota(jnp.int32, (GROUP, BLK), 0)
    ).astype(BF16)
    tiled = jnp.dot(mid_ref[...], repeat, preferred_element_type=F32)
    owner = lax.broadcasted_iota(jnp.int32, (PER_GROUP, BLK), 1) // GROUP
    mine = owner == lax.broadcasted_iota(jnp.int32, (PER_GROUP, BLK), 0)
    mid_weights = jnp.where(mine, jnp.broadcast_to(tiled, (PER_GROUP, BLK)), 0.0)
    coarse_weights = jnp.broadcast_to(coarse_ref[...].astype(F32), (slot, BLK))
    row = lax.broadcasted_iota(jnp.int32, (slot, BLK), 0)
    total = jnp.zeros((slot, HEAD_DIM), F32)
    for which, source in enumerate((keys_ref, values_ref)):
        for block in range(block_count):
            here = source[block * BLK : (block + 1) * BLK, :]
            weights = jnp.concatenate(
                [
                    mid_weights,
                    jnp.where(row == which * block_count + block, coarse_weights, 0.0),
                ]
            ).astype(BF16)
            pooled = jnp.dot(weights, here, preferred_element_type=F32)
            total = total + pooled[PER_GROUP:]
            start = slot + which * rows + block * PER_GROUP
            mids = pooled[:PER_GROUP].astype(BF16)
            near_out[start : start + PER_GROUP, :] = mids
            nth = block - (block_count - last_blocks)
            if nth >= 0:
                start = slot + (which * last_blocks + nth) * PER_GROUP
                third_out[start : start + PER_GROUP, :] = mids
        edge = (block_count - 1) * BLK
        tails_out[which * BLK : (which + 1) * BLK, :] = source[edge : edge + BLK, :]
    near_out[:slot, :] = total.astype(BF16)
    third_out[:slot, :] = total.astype(BF16)
    for copy in copies[4:]:
        copy.wait()


def pool(flip, queries, keys, values, mid_pool, coarse_pool, block_count, last_blocks, slot):
    shapes = (
        (BLK, queries.shape[1] + 2 * HEAD_DIM),
        keys.shape,
        values.shape,
        (slot + 2 * block_count * PER_GROUP, HEAD_DIM),
        (slot + 2 * last_blocks * PER_GROUP, HEAD_DIM),
        (2 * BLK, HEAD_DIM),
    )
    return pl.pallas_call(
        functools.partial(pool_kernel, block_count, last_blocks, slot, flip),
        in_specs=[pl.BlockSpec(memory_space=pltpu.HBM)] * 5,
        out_specs=[pl.BlockSpec(memory_space=pltpu.VMEM) for _ in shapes],
        out_shape=[jax.ShapeDtypeStruct(shape, BF16) for shape in shapes],
        scratch_shapes=[
            pltpu.VMEM(mid_pool.shape, BF16),
            pltpu.VMEM(coarse_pool.shape, BF16),
            pltpu.SemaphoreType.DMA((7,)),
        ],
        cost_estimate=pl.CostEstimate(
            flops=4 * keys.size * (PER_GROUP + slot), bytes_accessed=6 * keys.size, transcendentals=0
        ),
        compiler_params=pltpu.CompilerParams(vmem_limit_bytes=VMEM_LIMIT),
        name="pool",
    )(*off_chip(queries, keys, values, mid_pool, coarse_pool))


def select_kernel(parts, *refs):
    out_ref, at = refs[-1], 0
    for index, start, size in parts:
        out_ref[at : at + size, :] = refs[index][start : start + size, :]
        at += size


def select(parts, *arrays):
    rows = sum(size for _, _, size in parts)
    return pl.pallas_call(
        functools.partial(select_kernel, parts),
        in_specs=[pl.BlockSpec(memory_space=pltpu.VMEM)] * len(arrays),
        out_specs=pl.BlockSpec(memory_space=pltpu.VMEM),
        out_shape=jax.ShapeDtypeStruct((rows, arrays[0].shape[1]), arrays[0].dtype),
        compiler_params=pltpu.CompilerParams(vmem_limit_bytes=VMEM_LIMIT),
        name="select",
    )(*arrays)


def load_kernel(*refs):
    count = len(refs) // 2
    copies = [
        pltpu.make_async_copy(refs[i], refs[count + i], refs[-1].at[i]) for i in range(count)
    ]
    for copy in copies:
        copy.start()
    for copy in copies:
        copy.wait()


def load(*arrays):
    return pl.pallas_call(
        load_kernel,
        in_specs=[pl.BlockSpec(memory_space=pltpu.HBM) for _ in arrays],
        out_specs=[pl.BlockSpec(memory_space=pltpu.VMEM) for _ in arrays],
        out_shape=[jax.ShapeDtypeStruct(a.shape, a.dtype) for a in arrays],
        scratch_shapes=[pltpu.SemaphoreType.DMA((len(arrays),))],
        compiler_params=pltpu.CompilerParams(vmem_limit_bytes=VMEM_LIMIT),
        cost_estimate=pl.CostEstimate(
            flops=2 * sum(a.size for a in arrays),
            bytes_accessed=4 * sum(a.size for a in arrays),
            transcendentals=0,
        ),
        name="load",
    )(*off_chip(*arrays))


def fill_mids(geometry, target, sources, mid_scratch, which, write):
    block_count, last_blocks, slot, _ = geometry
    near_ref, far_ref, third_ref, mine_ref = sources
    rows = block_count * PER_GROUP
    late = last_blocks * PER_GROUP
    at = 0
    for ref, start, size in (
        (third_ref, slot + which * late, late),
        (far_ref, slot + which * rows, rows),
        (near_ref, slot + which * rows, rows),
        (mine_ref, slot + which * rows, rows),
    ):
        mid_scratch[at : at + size, :] = ref[start : start + size, :]
        at += size
    window = pl.ds(pl.multiple_of(target * PER_GROUP, PER_GROUP), MIDS)
    write(0, mid_scratch[window, :])


def fill_previous(target, prev_at, source, tails_ref, which, write):
    before = pl.ds(pl.multiple_of(jnp.maximum(target - 1, 0) * BLK, BLK), BLK)
    tail = tails_ref[which * BLK : (which + 1) * BLK, :]
    write(prev_at, jnp.where(target == 0, tail, source[before, :]))


def fill_coarse(geometry, width, coarse, which, write):
    block_count, _, slot, reach = geometry
    wide = coarse.astype(F32)
    if which:
        wide = pltpu.roll(wide, reach * slot - block_count, 0)
    if width > reach * slot:
        wide = jnp.concatenate([wide, jnp.zeros((width - reach * slot, HEAD_DIM), F32)])
    write(MIDS, wide.astype(BF16))


def pack_mids_kernel(geometry, flip, *refs):
    sources, (out_ref, mid_scratch) = refs[:-2], refs[-2:]
    for which in range(2):

        def write(at, value):
            out_ref[at : at + value.shape[0], head_columns(which)] = value

        fill_mids(geometry, block_of(flip), sources, mid_scratch, which, write)


def pack_rest_kernel(flip, keys_ref, values_ref, tails_ref, coarse_ref, out_ref):
    half = coarse_ref.shape[0] // 2
    for which, source in enumerate((keys_ref, values_ref)):

        def write(at, value):
            out_ref[at : at + value.shape[0], head_columns(which)] = value

        fill_previous(block_of(flip), 0, source, tails_ref, which, write)
        write(BLK, coarse_ref[which * half : (which + 1) * half, :])


def whole_in_vmem(count):
    return [pl.BlockSpec(memory_space=pltpu.VMEM)] * count


def mid_rows(geometry):
    block_count, last_blocks = geometry[:2]
    return (3 * block_count + last_blocks) * PER_GROUP


def pack(kernel, rows, operands, scratch):
    return pl.pallas_call(
        kernel,
        in_specs=whole_in_vmem(len(operands)),
        out_specs=pl.BlockSpec(memory_space=pltpu.VMEM),
        out_shape=jax.ShapeDtypeStruct((rows, 2 * HEAD_DIM), BF16),
        scratch_shapes=scratch,
        compiler_params=pltpu.CompilerParams(vmem_limit_bytes=VMEM_LIMIT),
        cost_estimate=pl.CostEstimate(
            flops=rows * HEAD_DIM, bytes_accessed=8 * rows * HEAD_DIM, transcendentals=0
        ),
        name="pack",
    )(*operands)


def fill_bias(geometry, target, device, width, bias):
    block_count, _, slot, reach = geometry
    block = device * block_count + target
    coarse_at = MIDS
    prev_at = MIDS + width
    lane = lax.broadcasted_iota(jnp.int32, bias.shape, 1)
    mid_ok = lane >= (MIDB + 1 - block) * PER_GROUP
    far = (lane - coarse_at) // slot
    nth = (lane - coarse_at) % slot
    coarse_ok = (
        (nth < block_count)
        & (far < reach)
        & (far <= device)
        & (far * block_count - nth + target >= MIDB + 2)
    )
    mid_bias = jnp.where(mid_ok, 0.0, NEG)
    coarse_bias = jnp.where(coarse_ok, 0.0, NEG)
    prev_bias = jnp.where(block * (lane + 1) >= 1, 0.0, NEG)
    bias[...] = jnp.where(
        lane < coarse_at, mid_bias, jnp.where(lane < prev_at, coarse_bias, prev_bias)
    )


def attend_jobs(jobs, heads, scores, weights):
    group = max(1, heads // 2)
    units = [
        (job, first, half) for job in jobs for first in range(0, heads, group) for half in range(2)
    ]
    row = lax.broadcasted_iota(jnp.int32, (CHUNK, HALF), 0)
    column = lax.broadcasted_iota(jnp.int32, (CHUNK, HALF), 1)

    def score(unit):
        (q_ref, row_start, keys, _, bias, _), first, half = units[unit]
        seen = bias.shape[1] + (half + 1) * HALF
        rows_here = pl.ds(pl.multiple_of(row_start + half * HALF, HALF), HALF)
        stacked = jnp.concatenate([q_ref[rows_here, head_columns(first + i)] for i in range(group)])
        scores[unit % 2, :, :seen] = lax.dot_general(
            stacked, keys[:seen, :], (((1,), (1,)), ((), ())), preferred_element_type=F32
        )

    def weigh(unit):
        (_, _, _, _, bias, _), first, half = units[unit]
        own_at = bias.shape[1]
        seen = own_at + (half + 1) * HALF
        for at in range(0, group * HALF, CHUNK):
            here = slice(at, at + CHUNK)
            parts = [scores[unit % 2, here, :own_at] + bias[0:1, :]]
            if half:
                parts.append(scores[unit % 2, here, own_at : own_at + HALF])
            edge = scores[unit % 2, here, seen - HALF : seen]
            parts.append(jnp.where(row + at % HALF >= column, edge, NEG))
            chunk = jnp.concatenate(parts, axis=1)
            top = jnp.max(chunk, axis=-1, keepdims=True)
            weights[unit % 2, here, :seen] = jnp.exp2((chunk - top) * EXP_SCALE).astype(BF16)

    def mix(unit):
        (_, _, _, values, bias, emit), first, half = units[unit]
        seen = bias.shape[1] + (half + 1) * HALF
        mixed = jnp.dot(weights[unit % 2, :, :seen], values[:seen, :], preferred_element_type=F32)
        emit(first, group, half, (mixed[:, :HEAD_DIM] / mixed[:, HEAD_DIM:]).astype(BF16))

    for unit in range(len(units) + 2):
        if unit < len(units):
            score(unit)
        if 1 <= unit <= len(units):
            weigh(unit - 1)
        if unit >= 2:
            mix(unit - 2)


def head_columns(head):
    return slice(head * HEAD_DIM, (head + 1) * HEAD_DIM)


def store(ref, first_head, first, group, half, mixed):
    for i in range(group):
        ref[half * HALF : (half + 1) * HALF, head_columns(first_head + first + i)] = mixed[
            i * HALF : (i + 1) * HALF
        ]


def fill_local(geometry, width, target, sources, mid_scratch, scratch):
    own_at = MIDS + width + BLK
    for which in range(2):
        everything = scratch[which]

        def write(at, value):
            everything[at : at + value.shape[0], :HEAD_DIM] = value

        fill_mids(geometry, target, sources[3:7], mid_scratch, which, write)
        fill_previous(target, MIDS + width, sources[which], sources[2], which, write)
        fill_coarse(geometry, width, sources[-1][...], which, write)
        own = pl.ds(pl.multiple_of(target * BLK, BLK), BLK)
        write(own_at, sources[which][own, :])
    scratch[1][:, HEAD_DIM:] = jnp.ones((own_at + BLK, HEAD_DIM), BF16)
    fill_bias(geometry, target, lax.axis_index("seq"), width, scratch[2])


def fill_shipped(geometry, width, target, early_ref, mids_ref, rest_ref, scratch):
    own_at = MIDS + width + BLK
    for which in range(2):
        everything = scratch[which]
        columns = head_columns(which)

        def write(at, value):
            everything[at : at + value.shape[0], :HEAD_DIM] = value

        write(0, mids_ref[:, columns])
        coarse = jnp.concatenate([rest_ref[BLK:, head_columns(i)] for i in range(2)])
        fill_coarse(geometry, width, coarse, which, write)
        write(MIDS + width, rest_ref[:BLK, columns])
        at = early_ref.shape[1] - (2 - which) * HEAD_DIM
        write(own_at, early_ref[:, at : at + HEAD_DIM])
    scratch[1][:, HEAD_DIM:] = jnp.ones((own_at + BLK, HEAD_DIM), BF16)
    fill_bias(geometry, target, lax.axis_index("seq"), width, scratch[2])


def attend_kernel(flip, geometry, width, heads, q_ref, *rest):
    sources, (_, out_ref, mid_scratch) = rest[:SHARED], rest[SHARED : SHARED + 3]
    scratch, (scores, weights) = rest[SHARED + 3 : SHARED + 6], rest[SHARED + 6 :]
    target = block_of(flip)
    fill_local(geometry, width, target, sources, mid_scratch, scratch)
    emit = functools.partial(store, out_ref, 0)
    attend_jobs([(q_ref, target * BLK, *scratch, emit)], heads, scores, weights)


def finish_kernel(flip, geometry, width, heads, q_ref, *rest):
    sources, rest = rest[:SHARED], rest[SHARED:]
    early_ref, mids_ref, rest_ref, _, output, mid_scratch = rest[:6]
    rest = rest[3:]
    ours, theirs = rest[3:6], rest[6:9]
    scores, weights, results, sent = rest[9:]
    member = block_of(0)
    copies = []

    fill_local(geometry, width, member, sources, mid_scratch, ours)
    fill_shipped(geometry, width, member, early_ref, mids_ref, rest_ref, theirs)

    def emit(job, owner):
        def put(first, group, half, mixed):
            store(results, job * heads, first, group, half, mixed)
            if half:
                start = (job * heads + first) * HEAD_DIM
                size = group * HEAD_DIM
                at = pl.multiple_of((owner * heads + first) * HEAD_DIM, HEAD_DIM)
                copy = pltpu.make_async_copy(
                    results.at[:, start : start + size],
                    output.at[:, pl.ds(at, size)],
                    sent.at[len(copies)],
                )
                copies.append(copy)
                copy.start()

        return put

    attend_jobs(
        [
            (q_ref, member * BLK, *ours, emit(0, member)),
            (early_ref, 0, *theirs, emit(1, member ^ flip)),
        ],
        heads,
        scores,
        weights,
    )
    for copy in copies:
        copy.wait()


def context_scratch(total):
    return [
        pltpu.VMEM((total, HEAD_DIM), BF16),
        pltpu.VMEM((total, 2 * HEAD_DIM), BF16),
        pltpu.VMEM((8, total - BLK), F32),
    ]


def attend_call(kernel, operands, jobs, heads, geometry, out_columns, out_spec, extra):
    width = coarse_width(geometry)
    total = MIDS + width + 2 * BLK
    unit_rows = max(1, heads // 2) * HALF
    return pl.pallas_call(
        functools.partial(kernel, geometry, width, heads),
        in_specs=whole_in_vmem(len(operands) - 1)
        + [pl.BlockSpec(memory_space=pl.ANY)],
        out_specs=out_spec,
        scratch_shapes=[pltpu.VMEM((mid_rows(geometry), HEAD_DIM), BF16)]
        + context_scratch(total) * jobs
        + [
            pltpu.VMEM((2, unit_rows, total), F32),
            pltpu.VMEM((2, unit_rows, total), BF16),
        ]
        + extra,
        out_shape=jax.ShapeDtypeStruct((BLK, out_columns), BF16),
        compiler_params=pltpu.CompilerParams(vmem_limit_bytes=ATTEND_LIMIT),
        cost_estimate=pl.CostEstimate(
            flops=6 * jobs * BLK * heads * total * HEAD_DIM,
            bytes_accessed=4 * BLK * heads * HEAD_DIM + 1024 * 1024,
            transcendentals=jobs * BLK * heads * total,
        ),
        name="attend",
    )(*operands)


def coarse_width(geometry):
    return round_up(geometry[3] * geometry[2], LANES)


def attend(flip, queries, shared, after, heads, geometry):
    return attend_call(
        functools.partial(attend_kernel, flip),
        (queries, *shared, after),
        1,
        heads,
        geometry,
        heads * HEAD_DIM,
        pl.BlockSpec(memory_space=pltpu.VMEM),
        [],
    )


def finish(queries, shared, shipped, after, flip, heads, geometry, out_columns):
    kernel = functools.partial(finish_kernel, flip)
    groups = heads // max(1, heads // 2)
    return attend_call(
        kernel,
        (queries, *shared, *shipped, after),
        2,
        heads,
        geometry,
        out_columns,
        pl.BlockSpec(memory_space=pl.ANY),
        [
            pltpu.VMEM((BLK, 2 * heads * HEAD_DIM), BF16),
            pltpu.SemaphoreType.DMA((2 * groups,)),
        ],
    )


def place_kernel(spots, columns, *refs):
    pieces, out_ref, done = refs[: len(spots)], refs[-2], refs[-1]
    copies = []
    for i, (flip, at) in enumerate(spots):
        start = pl.multiple_of(block_of(flip) * columns + at, HEAD_DIM)
        target = out_ref.at[:, pl.ds(start, pieces[i].shape[1])]
        copies.append(pltpu.make_async_copy(pieces[i], target, done.at[i]))
    for copy in copies:
        copy.start()
    for copy in copies:
        copy.wait()


def place(output, pieces, columns):
    spots = [(flip, start * HEAD_DIM) for flip, start, _ in pieces]
    size = sum(piece.size for _, _, piece in pieces)
    return pl.pallas_call(
        functools.partial(place_kernel, spots, columns),
        in_specs=[pl.BlockSpec(memory_space=pltpu.VMEM)] * len(pieces)
        + [pl.BlockSpec(memory_space=pl.ANY)],
        out_specs=pl.BlockSpec(memory_space=pl.ANY),
        scratch_shapes=[pltpu.SemaphoreType.DMA((len(pieces),))],
        out_shape=jax.ShapeDtypeStruct(output.shape, output.dtype),
        input_output_aliases={len(pieces): 0},
        compiler_params=pltpu.CompilerParams(vmem_limit_bytes=VMEM_LIMIT),
        cost_estimate=pl.CostEstimate(flops=size, bytes_accessed=4 * size, transcendentals=0),
        name="place",
    )(*[piece for _, _, piece in pieces], output)


def body(queries, keys, values, mid_pool, coarse_pool):
    tokens_here, columns = queries.shape
    heads_here = columns // HEAD_DIM
    block_count = tokens_here // BLK
    members = lax.axis_size("head")
    length = lax.axis_size("seq")
    assert keys.shape[1] == HEAD_DIM and block_count == members
    assert block_count <= MIDB and members & (members - 1) == 0
    assert 2 * block_count <= MIDB < 3 * block_count
    last_blocks = MIDB + 1 - 2 * block_count
    slot = round_up(2 * block_count, 8)
    away = members // 2

    early, keys, values, mine, third, tails = pool(
        away, queries, keys, values, mid_pool, coarse_pool, block_count, last_blocks, slot
    )
    near = cyclic(mine, "seq", 1)
    early = exchange(early, "head", away)
    far = cyclic(mine, "seq", 2)
    third = cyclic(third, "seq", 3)
    tails = cyclic(tails, "seq", 1)
    (queries,) = load(queries)
    coarse = select([(i, 0, slot) for i in range(4)], mine, near, far, third)
    reach = 4
    while reach < length:
        arriving = cyclic(coarse, "seq", reach)
        size = coarse.shape[0]
        coarse = select([(0, 0, size), (1, 0, size)], coarse, arriving)
        reach *= 2
    geometry = (block_count, last_blocks, slot, reach)
    late = pack(
        functools.partial(pack_mids_kernel, geometry, away),
        MIDS,
        (near, far, third, mine),
        [pltpu.VMEM((mid_rows(geometry), HEAD_DIM), BF16)],
    )
    late = exchange(late, "head", away)
    rest = pack(
        functools.partial(pack_rest_kernel, away),
        BLK + reach * slot // 2,
        (keys, values, tails, coarse),
        [],
    )
    shipped = (early, late, exchange(rest, "head", away))

    shared = (keys, values, tails, near, far, third, mine, coarse)
    after = coarse
    arrived = []
    for flip in sent_flips(members):
        after = attend(flip, queries, shared, after, heads_here, geometry)
        arrived.append((flip, 0, exchange(after, "head", flip)))
    output = finish(queries, shared, shipped, after, away, heads_here, geometry, members * columns)
    return place(output, arrived, columns)


def sent_flips(members):
    return [*range(members // 2 + 1, members), *range(1, members // 2)]


def solution(mesh):
    return jax.shard_map(
        body,
        mesh=mesh,
        in_specs=(
            P("seq", "head"),
            P("seq", "head"),
            P("seq", "head"),
            P("head", None),
            P("head", None),
        ),
        out_specs=P(("seq", "head"), None),
        check_vma=False,
    )
```

```python
import functools
import math

import jax
import jax.numpy as jnp
from jax import lax
from jax.experimental import pallas as pl
from jax.experimental.pallas import tpu as pltpu
from jax.sharding import PartitionSpec as P


HEAD_DIM = 128
BLK = 256
GROUP = 8
MIDS = 256
MIDB = 8
PER_GROUP = BLK // GROUP
LANES = 128
NEG = -1e30
HALF = BLK // 2
CHUNK = 32
SHARED = 8
VMEM_LIMIT = 16 * 1024 * 1024
ATTEND_LIMIT = 28 * 1024 * 1024
EXP_SCALE = math.log2(math.e) / math.sqrt(HEAD_DIM)
BF16 = jnp.bfloat16
F32 = jnp.float32


def round_up(value, multiple):
    return -(-value // multiple) * multiple


def cyclic(array, axis, by):
    size = lax.axis_size(axis)
    return lax.ppermute(array, axis, [(i, (i + by) % size) for i in range(size)])


def off_chip(*arrays):
    return [pltpu.with_memory_space_constraint(a, pltpu.HBM) for a in arrays]


def exchange(array, axis, flip):
    size = lax.axis_size(axis)
    return lax.ppermute(array, axis, [(i, i ^ flip) for i in range(size)])


def block_of(flip):
    return lax.axis_index("head") ^ flip


def prepare_kernel(flip, *refs):
    sources, (early_out, *targets), arrived = refs[:5], refs[5:10], refs[10]
    wanted = pl.ds(pl.multiple_of(block_of(flip) * BLK, BLK), BLK)
    moves, at = [], 0
    for source in sources[:3]:
        columns = slice(at, at + source.shape[1])
        moves.append((source.at[wanted, :], early_out.at[:, columns]))
        at += source.shape[1]
    moves += list(zip(sources[1:], targets))
    copies = [
        pltpu.make_async_copy(source, target, arrived.at[i])
        for i, (source, target) in enumerate(moves)
    ]
    for copy in copies:
        copy.start()
    for copy in copies:
        copy.wait()


def prepare(flip, *arrays):
    early = jax.ShapeDtypeStruct((BLK, sum(a.shape[1] for a in arrays[:3])), BF16)
    shapes = [early] + [jax.ShapeDtypeStruct(a.shape, a.dtype) for a in arrays[1:]]
    return pl.pallas_call(
        functools.partial(prepare_kernel, flip),
        in_specs=[pl.BlockSpec(memory_space=pltpu.HBM) for _ in arrays],
        out_specs=[pl.BlockSpec(memory_space=pltpu.VMEM) for _ in shapes],
        out_shape=shapes,
        scratch_shapes=[pltpu.SemaphoreType.DMA((7,))],
        compiler_params=pltpu.CompilerParams(vmem_limit_bytes=VMEM_LIMIT),
        cost_estimate=pl.CostEstimate(
            flops=early.size, bytes_accessed=4 * early.size, transcendentals=0
        ),
        name="prepare",
    )(*off_chip(*arrays))


def pool_kernel(block_count, last_blocks, slot, keys_ref, values_ref, mid_ref, coarse_ref,
                near_out, third_out, tails_out):
    rows = block_count * PER_GROUP
    repeat = (
        lax.broadcasted_iota(jnp.int32, (GROUP, BLK), 1) % GROUP
        == lax.broadcasted_iota(jnp.int32, (GROUP, BLK), 0)
    ).astype(BF16)
    tiled = jnp.dot(mid_ref[...], repeat, preferred_element_type=F32)
    owner = lax.broadcasted_iota(jnp.int32, (PER_GROUP, BLK), 1) // GROUP
    mine = owner == lax.broadcasted_iota(jnp.int32, (PER_GROUP, BLK), 0)
    mid_weights = jnp.where(mine, jnp.broadcast_to(tiled, (PER_GROUP, BLK)), 0.0)
    coarse_weights = jnp.broadcast_to(coarse_ref[...].astype(F32), (slot, BLK))
    row = lax.broadcasted_iota(jnp.int32, (slot, BLK), 0)
    total = jnp.zeros((slot, HEAD_DIM), F32)
    for which, source in enumerate((keys_ref, values_ref)):
        for block in range(block_count):
            here = source[block * BLK : (block + 1) * BLK, :]
            weights = jnp.concatenate(
                [
                    mid_weights,
                    jnp.where(row == which * block_count + block, coarse_weights, 0.0),
                ]
            ).astype(BF16)
            pooled = jnp.dot(weights, here, preferred_element_type=F32)
            total = total + pooled[PER_GROUP:]
            start = slot + which * rows + block * PER_GROUP
            mids = pooled[:PER_GROUP].astype(BF16)
            near_out[start : start + PER_GROUP, :] = mids
            nth = block - (block_count - last_blocks)
            if nth >= 0:
                start = slot + (which * last_blocks + nth) * PER_GROUP
                third_out[start : start + PER_GROUP, :] = mids
        edge = (block_count - 1) * BLK
        tails_out[which * BLK : (which + 1) * BLK, :] = source[edge : edge + BLK, :]
    near_out[:slot, :] = total.astype(BF16)
    third_out[:slot, :] = total.astype(BF16)


def pool(keys, values, mid_pool, coarse_pool, block_count, last_blocks, slot):
    shapes = (
        (slot + 2 * block_count * PER_GROUP, HEAD_DIM),
        (slot + 2 * last_blocks * PER_GROUP, HEAD_DIM),
        (2 * BLK, HEAD_DIM),
    )
    return pl.pallas_call(
        functools.partial(pool_kernel, block_count, last_blocks, slot),
        in_specs=[pl.BlockSpec(memory_space=pltpu.VMEM)] * 4,
        out_specs=[pl.BlockSpec(memory_space=pltpu.VMEM) for _ in shapes],
        out_shape=[jax.ShapeDtypeStruct(shape, BF16) for shape in shapes],
        cost_estimate=pl.CostEstimate(
            flops=4 * keys.size * (PER_GROUP + slot), bytes_accessed=6 * keys.size, transcendentals=0
        ),
        compiler_params=pltpu.CompilerParams(vmem_limit_bytes=VMEM_LIMIT),
        name="pool",
    )(keys, values, mid_pool, coarse_pool)


def select_kernel(parts, *refs):
    out_ref, at = refs[-1], 0
    for index, start, size in parts:
        out_ref[at : at + size, :] = refs[index][start : start + size, :]
        at += size


def select(parts, *arrays):
    rows = sum(size for _, _, size in parts)
    return pl.pallas_call(
        functools.partial(select_kernel, parts),
        in_specs=[pl.BlockSpec(memory_space=pltpu.VMEM)] * len(arrays),
        out_specs=pl.BlockSpec(memory_space=pltpu.VMEM),
        out_shape=jax.ShapeDtypeStruct((rows, arrays[0].shape[1]), arrays[0].dtype),
        compiler_params=pltpu.CompilerParams(vmem_limit_bytes=VMEM_LIMIT),
        name="select",
    )(*arrays)


def load_kernel(*refs):
    count = len(refs) // 2
    copies = [
        pltpu.make_async_copy(refs[i], refs[count + i], refs[-1].at[i]) for i in range(count)
    ]
    for copy in copies:
        copy.start()
    for copy in copies:
        copy.wait()


def load(*arrays):
    return pl.pallas_call(
        load_kernel,
        in_specs=[pl.BlockSpec(memory_space=pltpu.HBM) for _ in arrays],
        out_specs=[pl.BlockSpec(memory_space=pltpu.VMEM) for _ in arrays],
        out_shape=[jax.ShapeDtypeStruct(a.shape, a.dtype) for a in arrays],
        scratch_shapes=[pltpu.SemaphoreType.DMA((len(arrays),))],
        compiler_params=pltpu.CompilerParams(vmem_limit_bytes=VMEM_LIMIT),
        cost_estimate=pl.CostEstimate(
            flops=2 * sum(a.size for a in arrays),
            bytes_accessed=4 * sum(a.size for a in arrays),
            transcendentals=0,
        ),
        name="load",
    )(*off_chip(*arrays))


def fill_mids(geometry, target, sources, mid_scratch, which, write):
    block_count, last_blocks, slot, _ = geometry
    near_ref, far_ref, third_ref, mine_ref = sources
    rows = block_count * PER_GROUP
    late = last_blocks * PER_GROUP
    at = 0
    for ref, start, size in (
        (third_ref, slot + which * late, late),
        (far_ref, slot + which * rows, rows),
        (near_ref, slot + which * rows, rows),
        (mine_ref, slot + which * rows, rows),
    ):
        mid_scratch[at : at + size, :] = ref[start : start + size, :]
        at += size
    window = pl.ds(pl.multiple_of(target * PER_GROUP, PER_GROUP), MIDS)
    write(0, mid_scratch[window, :])


def fill_previous(target, prev_at, source, tails_ref, which, write):
    before = pl.ds(pl.multiple_of(jnp.maximum(target - 1, 0) * BLK, BLK), BLK)
    tail = tails_ref[which * BLK : (which + 1) * BLK, :]
    write(prev_at, jnp.where(target == 0, tail, source[before, :]))


def fill_coarse(geometry, width, coarse, which, write):
    block_count, _, slot, reach = geometry
    wide = coarse.astype(F32)
    if which:
        wide = pltpu.roll(wide, reach * slot - block_count, 0)
    if width > reach * slot:
        wide = jnp.concatenate([wide, jnp.zeros((width - reach * slot, HEAD_DIM), F32)])
    write(MIDS, wide.astype(BF16))


def pack_mids_kernel(geometry, flip, *refs):
    sources, (out_ref, mid_scratch) = refs[:-2], refs[-2:]
    for which in range(2):

        def write(at, value):
            out_ref[at : at + value.shape[0], head_columns(which)] = value

        fill_mids(geometry, block_of(flip), sources, mid_scratch, which, write)


def pack_rest_kernel(flip, keys_ref, values_ref, tails_ref, coarse_ref, out_ref):
    half = coarse_ref.shape[0] // 2
    for which, source in enumerate((keys_ref, values_ref)):

        def write(at, value):
            out_ref[at : at + value.shape[0], head_columns(which)] = value

        fill_previous(block_of(flip), 0, source, tails_ref, which, write)
        write(BLK, coarse_ref[which * half : (which + 1) * half, :])


def whole_in_vmem(count):
    return [pl.BlockSpec(memory_space=pltpu.VMEM)] * count


def mid_rows(geometry):
    block_count, last_blocks = geometry[:2]
    return (3 * block_count + last_blocks) * PER_GROUP


def pack(kernel, rows, operands, scratch):
    return pl.pallas_call(
        kernel,
        in_specs=whole_in_vmem(len(operands)),
        out_specs=pl.BlockSpec(memory_space=pltpu.VMEM),
        out_shape=jax.ShapeDtypeStruct((rows, 2 * HEAD_DIM), BF16),
        scratch_shapes=scratch,
        compiler_params=pltpu.CompilerParams(vmem_limit_bytes=VMEM_LIMIT),
        cost_estimate=pl.CostEstimate(
            flops=rows * HEAD_DIM, bytes_accessed=8 * rows * HEAD_DIM, transcendentals=0
        ),
        name="pack",
    )(*operands)


def fill_bias(geometry, target, device, width, bias):
    block_count, _, slot, reach = geometry
    block = device * block_count + target
    coarse_at = MIDS
    prev_at = MIDS + width
    lane = lax.broadcasted_iota(jnp.int32, bias.shape, 1)
    mid_ok = lane >= (MIDB + 1 - block) * PER_GROUP
    far = (lane - coarse_at) // slot
    nth = (lane - coarse_at) % slot
    coarse_ok = (
        (nth < block_count)
        & (far < reach)
        & (far <= device)
        & (far * block_count - nth + target >= MIDB + 2)
    )
    mid_bias = jnp.where(mid_ok, 0.0, NEG)
    coarse_bias = jnp.where(coarse_ok, 0.0, NEG)
    prev_bias = jnp.where(block * (lane + 1) >= 1, 0.0, NEG)
    bias[...] = jnp.where(
        lane < coarse_at, mid_bias, jnp.where(lane < prev_at, coarse_bias, prev_bias)
    )


def attend_jobs(jobs, heads, scores, weights):
    group = max(1, heads // 2)
    units = [
        (job, first, half) for job in jobs for first in range(0, heads, group) for half in range(2)
    ]
    row = lax.broadcasted_iota(jnp.int32, (CHUNK, HALF), 0)
    column = lax.broadcasted_iota(jnp.int32, (CHUNK, HALF), 1)

    def score(unit):
        (q_ref, row_start, keys, _, bias, _), first, half = units[unit]
        seen = bias.shape[1] + (half + 1) * HALF
        rows_here = pl.ds(pl.multiple_of(row_start + half * HALF, HALF), HALF)
        stacked = jnp.concatenate([q_ref[rows_here, head_columns(first + i)] for i in range(group)])
        scores[unit % 2, :, :seen] = lax.dot_general(
            stacked, keys[:seen, :], (((1,), (1,)), ((), ())), preferred_element_type=F32
        )

    def weigh(unit):
        (_, _, _, _, bias, _), first, half = units[unit]
        own_at = bias.shape[1]
        seen = own_at + (half + 1) * HALF
        for at in range(0, group * HALF, CHUNK):
            here = slice(at, at + CHUNK)
            parts = [scores[unit % 2, here, :own_at] + bias[0:1, :]]
            if half:
                parts.append(scores[unit % 2, here, own_at : own_at + HALF])
            edge = scores[unit % 2, here, seen - HALF : seen]
            parts.append(jnp.where(row + at % HALF >= column, edge, NEG))
            chunk = jnp.concatenate(parts, axis=1)
            top = jnp.max(chunk, axis=-1, keepdims=True)
            weights[unit % 2, here, :seen] = jnp.exp2((chunk - top) * EXP_SCALE).astype(BF16)

    def mix(unit):
        (_, _, _, values, bias, emit), first, half = units[unit]
        seen = bias.shape[1] + (half + 1) * HALF
        mixed = jnp.dot(weights[unit % 2, :, :seen], values[:seen, :], preferred_element_type=F32)
        emit(first, group, half, (mixed[:, :HEAD_DIM] / mixed[:, HEAD_DIM:]).astype(BF16))

    for unit in range(len(units) + 2):
        if unit < len(units):
            score(unit)
        if 1 <= unit <= len(units):
            weigh(unit - 1)
        if unit >= 2:
            mix(unit - 2)


def head_columns(head):
    return slice(head * HEAD_DIM, (head + 1) * HEAD_DIM)


def store(ref, first_head, first, group, half, mixed):
    for i in range(group):
        ref[half * HALF : (half + 1) * HALF, head_columns(first_head + first + i)] = mixed[
            i * HALF : (i + 1) * HALF
        ]


def fill_local(geometry, width, target, sources, mid_scratch, scratch):
    own_at = MIDS + width + BLK
    for which in range(2):
        everything = scratch[which]

        def write(at, value):
            everything[at : at + value.shape[0], :HEAD_DIM] = value

        fill_mids(geometry, target, sources[3:7], mid_scratch, which, write)
        fill_previous(target, MIDS + width, sources[which], sources[2], which, write)
        fill_coarse(geometry, width, sources[-1][...], which, write)
        own = pl.ds(pl.multiple_of(target * BLK, BLK), BLK)
        write(own_at, sources[which][own, :])
    scratch[1][:, HEAD_DIM:] = jnp.ones((own_at + BLK, HEAD_DIM), BF16)
    fill_bias(geometry, target, lax.axis_index("seq"), width, scratch[2])


def fill_shipped(geometry, width, target, early_ref, mids_ref, rest_ref, scratch):
    own_at = MIDS + width + BLK
    for which in range(2):
        everything = scratch[which]
        columns = head_columns(which)

        def write(at, value):
            everything[at : at + value.shape[0], :HEAD_DIM] = value

        write(0, mids_ref[:, columns])
        coarse = jnp.concatenate([rest_ref[BLK:, head_columns(i)] for i in range(2)])
        fill_coarse(geometry, width, coarse, which, write)
        write(MIDS + width, rest_ref[:BLK, columns])
        at = early_ref.shape[1] - (2 - which) * HEAD_DIM
        write(own_at, early_ref[:, at : at + HEAD_DIM])
    scratch[1][:, HEAD_DIM:] = jnp.ones((own_at + BLK, HEAD_DIM), BF16)
    fill_bias(geometry, target, lax.axis_index("seq"), width, scratch[2])


def attend_kernel(flip, geometry, width, heads, q_ref, *rest):
    sources, (_, out_ref, mid_scratch) = rest[:SHARED], rest[SHARED : SHARED + 3]
    scratch, (scores, weights) = rest[SHARED + 3 : SHARED + 6], rest[SHARED + 6 :]
    target = block_of(flip)
    fill_local(geometry, width, target, sources, mid_scratch, scratch)
    emit = functools.partial(store, out_ref, 0)
    attend_jobs([(q_ref, target * BLK, *scratch, emit)], heads, scores, weights)


def finish_kernel(flip, geometry, width, heads, q_ref, *rest):
    sources, rest = rest[:SHARED], rest[SHARED:]
    early_ref, mids_ref, rest_ref, _, output, mid_scratch = rest[:6]
    rest = rest[3:]
    ours, theirs = rest[3:6], rest[6:9]
    scores, weights, results, sent = rest[9:]
    member = block_of(0)
    copies = []

    fill_local(geometry, width, member, sources, mid_scratch, ours)
    fill_shipped(geometry, width, member, early_ref, mids_ref, rest_ref, theirs)

    def emit(job, owner):
        def put(first, group, half, mixed):
            store(results, job * heads, first, group, half, mixed)
            if half:
                start = (job * heads + first) * HEAD_DIM
                size = group * HEAD_DIM
                at = pl.multiple_of((owner * heads + first) * HEAD_DIM, HEAD_DIM)
                copy = pltpu.make_async_copy(
                    results.at[:, start : start + size],
                    output.at[:, pl.ds(at, size)],
                    sent.at[len(copies)],
                )
                copies.append(copy)
                copy.start()

        return put

    attend_jobs(
        [
            (q_ref, member * BLK, *ours, emit(0, member)),
            (early_ref, 0, *theirs, emit(1, member ^ flip)),
        ],
        heads,
        scores,
        weights,
    )
    for copy in copies:
        copy.wait()


def context_scratch(total):
    return [
        pltpu.VMEM((total, HEAD_DIM), BF16),
        pltpu.VMEM((total, 2 * HEAD_DIM), BF16),
        pltpu.VMEM((8, total - BLK), F32),
    ]


def attend_call(kernel, operands, jobs, heads, geometry, out_columns, out_spec, extra):
    width = coarse_width(geometry)
    total = MIDS + width + 2 * BLK
    unit_rows = max(1, heads // 2) * HALF
    return pl.pallas_call(
        functools.partial(kernel, geometry, width, heads),
        in_specs=whole_in_vmem(len(operands) - 1)
        + [pl.BlockSpec(memory_space=pl.ANY)],
        out_specs=out_spec,
        scratch_shapes=[pltpu.VMEM((mid_rows(geometry), HEAD_DIM), BF16)]
        + context_scratch(total) * jobs
        + [
            pltpu.VMEM((2, unit_rows, total), F32),
            pltpu.VMEM((2, unit_rows, total), BF16),
        ]
        + extra,
        out_shape=jax.ShapeDtypeStruct((BLK, out_columns), BF16),
        compiler_params=pltpu.CompilerParams(vmem_limit_bytes=ATTEND_LIMIT),
        cost_estimate=pl.CostEstimate(
            flops=6 * jobs * BLK * heads * total * HEAD_DIM,
            bytes_accessed=4 * BLK * heads * HEAD_DIM + 1024 * 1024,
            transcendentals=jobs * BLK * heads * total,
        ),
        name="attend",
    )(*operands)


def coarse_width(geometry):
    return round_up(geometry[3] * geometry[2], LANES)


def attend(flip, queries, shared, after, heads, geometry):
    return attend_call(
        functools.partial(attend_kernel, flip),
        (queries, *shared, after),
        1,
        heads,
        geometry,
        heads * HEAD_DIM,
        pl.BlockSpec(memory_space=pltpu.VMEM),
        [],
    )


def finish(queries, shared, shipped, after, flip, heads, geometry, out_columns):
    kernel = functools.partial(finish_kernel, flip)
    groups = heads // max(1, heads // 2)
    return attend_call(
        kernel,
        (queries, *shared, *shipped, after),
        2,
        heads,
        geometry,
        out_columns,
        pl.BlockSpec(memory_space=pl.ANY),
        [
            pltpu.VMEM((BLK, 2 * heads * HEAD_DIM), BF16),
            pltpu.SemaphoreType.DMA((2 * groups,)),
        ],
    )


def place_kernel(spots, columns, *refs):
    pieces, out_ref, done = refs[: len(spots)], refs[-2], refs[-1]
    copies = []
    for i, (flip, at) in enumerate(spots):
        start = pl.multiple_of(block_of(flip) * columns + at, HEAD_DIM)
        target = out_ref.at[:, pl.ds(start, pieces[i].shape[1])]
        copies.append(pltpu.make_async_copy(pieces[i], target, done.at[i]))
    for copy in copies:
        copy.start()
    for copy in copies:
        copy.wait()


def place(output, pieces, columns):
    spots = [(flip, start * HEAD_DIM) for flip, start, _ in pieces]
    size = sum(piece.size for _, _, piece in pieces)
    return pl.pallas_call(
        functools.partial(place_kernel, spots, columns),
        in_specs=[pl.BlockSpec(memory_space=pltpu.VMEM)] * len(pieces)
        + [pl.BlockSpec(memory_space=pl.ANY)],
        out_specs=pl.BlockSpec(memory_space=pl.ANY),
        scratch_shapes=[pltpu.SemaphoreType.DMA((len(pieces),))],
        out_shape=jax.ShapeDtypeStruct(output.shape, output.dtype),
        input_output_aliases={len(pieces): 0},
        compiler_params=pltpu.CompilerParams(vmem_limit_bytes=VMEM_LIMIT),
        cost_estimate=pl.CostEstimate(flops=size, bytes_accessed=4 * size, transcendentals=0),
        name="place",
    )(*[piece for _, _, piece in pieces], output)


def body(queries, keys, values, mid_pool, coarse_pool):
    tokens_here, columns = queries.shape
    heads_here = columns // HEAD_DIM
    block_count = tokens_here // BLK
    members = lax.axis_size("head")
    length = lax.axis_size("seq")
    assert keys.shape[1] == HEAD_DIM and block_count == members
    assert block_count <= MIDB and members & (members - 1) == 0
    assert 2 * block_count <= MIDB < 3 * block_count
    last_blocks = MIDB + 1 - 2 * block_count
    slot = round_up(2 * block_count, 8)
    away = members // 2

    early, keys, values, mid_pool, coarse_pool = prepare(
        away, queries, keys, values, mid_pool, coarse_pool
    )
    mine, third, tails = pool(keys, values, mid_pool, coarse_pool, block_count, last_blocks, slot)
    near = cyclic(mine, "seq", 1)
    early = exchange(early, "head", away)
    far = cyclic(mine, "seq", 2)
    third = cyclic(third, "seq", 3)
    tails = cyclic(tails, "seq", 1)
    (queries,) = load(queries)
    coarse = select([(i, 0, slot) for i in range(4)], mine, near, far, third)
    reach = 4
    while reach < length:
        arriving = cyclic(coarse, "seq", reach)
        size = coarse.shape[0]
        coarse = select([(0, 0, size), (1, 0, size)], coarse, arriving)
        reach *= 2
    geometry = (block_count, last_blocks, slot, reach)
    late = pack(
        functools.partial(pack_mids_kernel, geometry, away),
        MIDS,
        (near, far, third, mine),
        [pltpu.VMEM((mid_rows(geometry), HEAD_DIM), BF16)],
    )
    late = exchange(late, "head", away)
    rest = pack(
        functools.partial(pack_rest_kernel, away),
        BLK + reach * slot // 2,
        (keys, values, tails, coarse),
        [],
    )
    shipped = (early, late, exchange(rest, "head", away))

    shared = (keys, values, tails, near, far, third, mine, coarse)
    after = coarse
    arrived = []
    for flip in sent_flips(members):
        after = attend(flip, queries, shared, after, heads_here, geometry)
        arrived.append((flip, 0, exchange(after, "head", flip)))
    output = finish(queries, shared, shipped, after, away, heads_here, geometry, members * columns)
    output = place(output, [p for p in arrived if p[0] < away], columns)
    return place(output, [p for p in arrived if p[0] > away], columns)


def sent_flips(members):
    return [*range(members // 2 + 1, members), *range(1, members // 2)]


def solution(mesh):
    return jax.shard_map(
        body,
        mesh=mesh,
        in_specs=(
            P("seq", "head"),
            P("seq", "head"),
            P("seq", "head"),
            P("head", None),
            P("head", None),
        ),
        out_specs=P(("seq", "head"), None),
        check_vma=False,
    )
```
